32 devices in a mesh: gx: 4 (over z), gy: 4 (over y, x), gz: 2 (over core).
Axes of the slice: x: 2, y: 2, z: 4, core: 2. Of those that a mesh axis runs over, the one named last changes fastest.
Arguments:
- positions: float32 [3, 4096], P(None, ('gx', 'gy', 'gz')), may hold values from 0 to 4.5
- species: int32 [4096], P(('gx', 'gy', 'gz')), may hold values from 0 to 88
- cell_map: int32 [32, 128], P(('gx', 'gy', 'gz')), may hold values from 0 to 127, each once within a row
- neighbours: int32 [8, 4096], P(None, ('gx', 'gy', 'gz')), may hold values from 0 to 511
- struct_ids: int32 [4096], P(('gx', 'gy', 'gz')), may hold values from 0 to 15, as said below
- embed: float32 [89, 128], replicated, may hold values from -6 to 6
- w_up: float32 [2, 128, 128], replicated, may hold values from -0.5 to 0.5
- w_rad_in: float32 [2, 8, 64], replicated, may hold values from -2 to 2
- w_rad_out: float32 [2, 64, 256], replicated, may hold values from -0.75 to 0.75
- w_mix: float32 [2, 3, 128, 128], replicated, may hold values from -0.5 to 0.5
- read_first: float32 [128], replicated, may hold values from -0.5 to 0.5
- read_hidden: float32 [128, 16], replicated, may hold values from -0.5 to 0.5
- read_last: float32 [16], replicated, may hold values from -1.5 to 1.5
Outputs:
- energies: float32 [16], replicated
- virials: float32 [9, 16], replicated
- forces: float32 [3, 4096], P(None, ('gx', 'gy', 'gz'))
The draws below stay inside these ranges and needn't reach their ends.
Inputs may be any that keep to these rules, and one draw needn't show every extreme that they name: `cell_map`: each row is a permutation. `neighbours`: entries index the extended rows of the atom's own device. `struct_ids`: atoms of the devices with gx index a have ids from a * 4 to (a + 1) * 4 - 1.
All inputs are finite; a program needn't handle non-finite values.
Results may differ from the reference program's by a relative error of at most 0.0003.
Values sent between devices are 32-bit elements; how exact they have to be, the bound alone decides.
No kernel may reach another device: no remote copies, remote signals or barrier semaphores. Data moves between devices by JAX's collectives and lax.ppermute only.
A program may use at most 64 MiB of HBM per device.

```python
import math
import jax
import jax.numpy as jnp
from jax import lax

C = 128
NB = 8
H = 64
RH = 16
SPECIES = 89
NEIGH = 8
A_DEV = 128
SLAB_STRUCTS = 4
FACE_ATOMS = 64
EXTENDED = 512
ATOMS = 4096
SLAB_ATOMS = 1024
STRUCTS = 16
N_GX = 4
N_GY = 4
N_GZ = 2
DEVICES = 32


def draw_struct_ids(key, part):
    atom_index = jnp.arange(ATOMS, dtype=jnp.int32)
    slab_index = atom_index // SLAB_ATOMS
    within = jax.random.randint(key, (ATOMS,), 0, SLAB_STRUCTS, dtype=jnp.int32)
    return slab_index * SLAB_STRUCTS + within


def touch_ends(values, own_key, low, top_value):
    shape = values.shape
    spot = [jax.random.randint(jax.random.fold_in(own_key, axis), (), 0, shape[axis]) for axis in range(len(shape))]
    values = values.at[tuple(spot)].set(low)
    longest = shape.index(max(shape))
    spot[longest] = (spot[longest] + 1) % shape[longest]
    return values.at[tuple(spot)].set(top_value)


def block_levels(rng, extent, shards, least, high):
    def one(position, blocks):
        heights = jax.random.uniform(jax.random.fold_in(jax.random.fold_in(rng, 6), position), (blocks,), jnp.float32, least / len(shards), high / len(shards))
        return jnp.repeat(jnp.exp(heights), extent[position] // blocks).reshape((-1,) + (1,) * (len(extent) - position - 1))

    level = one(*shards[0])
    for cut in shards[1:]:
        level = level * one(*cut)
    return level


def gaussian(own_key, shape, width, limit, kind=jnp.bfloat16):
    values = jax.random.normal(own_key, shape, jnp.float32) * width
    return jnp.minimum(jnp.maximum(values, -limit), limit).astype(kind)


def setup_inputs(seed: int = 0) -> dict:
    splits = jax.random.split(jax.random.key(seed), 14)
    positions = jnp.clip(4.5 * jax.random.uniform(splits[0], (3, ATOMS), jnp.float32) ** block_levels(splits[0], (3, ATOMS), ((1, 32),), -0.2, 0.2), 0.0, 4.5)
    species = touch_ends(jax.random.randint(splits[1], (ATOMS,), 0, SPECIES), jax.random.fold_in(splits[1], 1), 0, SPECIES - 1).astype(jnp.int32)
    cell_map = jax.vmap(lambda own: jax.random.permutation(own, A_DEV))(jax.random.split(splits[2], DEVICES)).reshape((DEVICES, A_DEV)).astype(jnp.int32)
    neighbours = touch_ends(jax.random.randint(splits[3], (NEIGH, ATOMS), 0, EXTENDED), jax.random.fold_in(splits[3], 1), 0, EXTENDED - 1).astype(jnp.int32)
    struct_ids = draw_struct_ids(jax.random.fold_in(splits[13], 71), 0)
    embed = gaussian(splits[5], (SPECIES, C), 1.0, 6.0, jnp.float32)
    w_up = gaussian(splits[6], (2, C, C), C ** -0.5, 0.5, jnp.float32)
    w_rad_in = gaussian(splits[7], (2, NB, H), NB ** -0.5, 2.0, jnp.float32)
    w_rad_out = gaussian(splits[8], (2, H, 2 * C), H ** -0.5, 0.75, jnp.float32)
    w_mix = gaussian(splits[9], (2, 3, C, C), C ** -0.5, 0.5, jnp.float32)
    read_first = gaussian(splits[10], (C,), C ** -0.5, 0.5, jnp.float32)
    read_hidden = gaussian(splits[11], (C, RH), C ** -0.5, 0.5, jnp.float32)
    read_last = gaussian(splits[12], (RH,), RH ** -0.5, 1.5, jnp.float32)
    return dict(positions=positions, species=species, cell_map=cell_map, neighbours=neighbours, struct_ids=struct_ids, embed=embed, w_up=w_up, w_rad_in=w_rad_in, w_rad_out=w_rad_out, w_mix=w_mix, read_first=read_first, read_hidden=read_hidden, read_last=read_last)


precise = lax.Precision.HIGHEST
cutoff = 6.0
box_side = 4.5
soften = 0.25

def matmul(left, right):
    return jnp.dot(left, right, precision=precise, preferred_element_type=jnp.float32)

def edge_terms(edge_vec, bessels):
    radius = jnp.sqrt(lax.optimization_barrier(jnp.sum(edge_vec * edge_vec, axis=0)) + soften)
    envelope = jnp.square(jax.nn.relu(1.0 - radius * radius / (cutoff * cutoff)))
    harmonic = jnp.arange(1, bessels + 1).astype(jnp.float32)
    angles = harmonic[:, None, None] * (jnp.pi / cutoff) * radius[None]
    bessel = math.sqrt(2.0 / cutoff) * jnp.sin(angles) / radius[None] * envelope[None]
    return (bessel, edge_vec / radius[None])

def interact(edge_vec, feats_ext, nbr_slots, w_up, w_rad_in, w_rad_out, w_mix):
    bessel, direction = edge_terms(edge_vec, w_rad_in.shape[0])
    hidden = jax.nn.silu(jnp.einsum('nka,nh->kah', bessel, w_rad_in, precision=precise))
    radial = jnp.einsum('kah,hc->kac', hidden, w_rad_out, precision=precise)
    lifted = matmul(feats_ext, w_up)
    picked = lifted[nbr_slots]
    channels = lifted.shape[1]
    scaling = 1.0 / math.sqrt(nbr_slots.shape[0])
    scalar = lax.optimization_barrier(jnp.sum(radial[:, :, :channels] * picked, axis=0)) * scaling
    vector = jnp.einsum('mka,kac->mac', direction, radial[:, :, channels:] * picked, precision=precise) * scaling
    squares = lax.optimization_barrier(jnp.sum(vector * vector, axis=0))
    return matmul(scalar, w_mix[0]) + matmul(squares, w_mix[1]) + matmul(scalar * scalar, w_mix[2])

def atom_energy(layer_out, second, read_first, read_hidden, read_last):
    hidden = jax.nn.silu(matmul(second, read_hidden))
    return matmul(layer_out, read_first) + matmul(hidden, read_last)

def to_cells(grid_rows, cell_order):
    picked = jnp.take_along_axis(grid_rows, cell_order[..., None], axis=3)
    shape = grid_rows.shape
    return picked.reshape(shape[:3] + (2, 2, 2, shape[3] // 8, shape[4]))

def face_rows(cell_data):
    pieces = (jnp.roll(cell_data, 1, axis=0)[:, :, :, 1], jnp.roll(cell_data, -1, axis=0)[:, :, :, 0], jnp.roll(cell_data, 1, axis=1)[:, :, :, :, 1], jnp.roll(cell_data, -1, axis=1)[:, :, :, :, 0], jnp.roll(cell_data, 1, axis=2)[:, :, :, :, :, 1], jnp.roll(cell_data, -1, axis=2)[:, :, :, :, :, 0])
    return jnp.concatenate([piece.reshape(piece.shape[:3] + (-1, piece.shape[-1])) for piece in pieces], axis=3)

def scatter_rows(cell_order, values):
    return jnp.zeros_like(values).at[cell_order].add(values)

def return_rows(ghosts, cell_order):
    shape = ghosts.shape
    per_face = shape[3] // 6
    per_cell = per_face // 4
    channels = shape[4]
    pieces = ghosts.reshape(shape[:3] + (6, 2, 2, per_cell, channels))
    cell_sums = jnp.zeros(shape[:3] + (2, 2, 2, per_cell, channels), jnp.float32)
    cell_sums = cell_sums.at[:, :, :, 1].add(jnp.roll(pieces[:, :, :, 0], -1, axis=0))
    cell_sums = cell_sums.at[:, :, :, 0].add(jnp.roll(pieces[:, :, :, 1], 1, axis=0))
    cell_sums = cell_sums.at[:, :, :, :, 1].add(jnp.roll(pieces[:, :, :, 2], -1, axis=1))
    cell_sums = cell_sums.at[:, :, :, :, 0].add(jnp.roll(pieces[:, :, :, 3], 1, axis=1))
    cell_sums = cell_sums.at[:, :, :, :, :, 1].add(jnp.roll(pieces[:, :, :, 4], -1, axis=2))
    cell_sums = cell_sums.at[:, :, :, :, :, 0].add(jnp.roll(pieces[:, :, :, 5], 1, axis=2))
    devices = shape[0] * shape[1] * shape[2]
    flat_sums = cell_sums.reshape(devices, 8 * per_cell, channels)
    return jax.vmap(scatter_rows)(cell_order.reshape(devices, -1), flat_sums)

def pick_rows(table_rows, slots):
    return table_rows[slots]

def scatter_edges(slots, grads):
    flat_grad = grads.transpose(1, 2, 0).reshape(-1, 3)
    return jnp.zeros((EXTENDED, 3), jnp.float32).at[slots.reshape(-1)].add(flat_grad)

def reference(positions, species, cell_map, neighbours, struct_ids, embed, w_up, w_rad_in, w_rad_out, w_mix, read_first, read_hidden, read_last):
    dev_grid = (N_GX, N_GY, N_GZ)
    devices = N_GX * N_GY * N_GZ
    atom_count = A_DEV
    channels = embed.shape[1]
    cell_order = cell_map.reshape(dev_grid + (atom_count,))
    pos_rows = positions.reshape((3,) + dev_grid + (atom_count,)).transpose(1, 2, 3, 4, 0)
    shifts = jnp.array([[-box_side, 0.0, 0.0], [box_side, 0.0, 0.0], [0.0, -box_side, 0.0], [0.0, box_side, 0.0], [0.0, 0.0, -box_side], [0.0, 0.0, box_side]], jnp.float32)
    ghost_pos = face_rows(to_cells(pos_rows, cell_order)) + jnp.repeat(shifts, FACE_ATOMS, axis=0)
    ext_pos = jnp.concatenate([pos_rows, ghost_pos], axis=3).reshape(devices, EXTENDED, 3)
    nbr_slots = neighbours.reshape(NEIGH, devices, atom_count).transpose(1, 0, 2)
    far_rows = jax.vmap(pick_rows)(ext_pos, nbr_slots)
    edge_vec = (far_rows - pos_rows.reshape(devices, 1, atom_count, 3)).transpose(0, 3, 1, 2)
    one_hot = (species[:, None] == jnp.arange(embed.shape[0])[None]).astype(jnp.float32)
    initial = matmul(one_hot, embed).reshape(dev_grid + (atom_count, channels))
    initial_ext = jnp.concatenate([initial, face_rows(to_cells(initial, cell_order))], axis=3).reshape(devices, EXTENDED, channels)
    initial_flat = initial.reshape(devices, atom_count, channels)

    def layer_zero(packed):
        return interact(packed[0], packed[1], packed[2], w_up[0], w_rad_in[0], w_rad_out[0], w_mix[0])

    def layer_one(packed):
        return interact(packed[0], packed[1], packed[2], w_up[1], w_rad_in[1], w_rad_out[1], w_mix[1])
    step_zero = jax.checkpoint(layer_zero)
    step_one = jax.checkpoint(layer_one)

    def energies_of(edges):
        layer_out = initial_flat + lax.map(step_zero, (edges, initial_ext, nbr_slots))
        out_grid = layer_out.reshape(dev_grid + (atom_count, channels))
        out_ext = jnp.concatenate([out_grid, face_rows(to_cells(out_grid, cell_order))], axis=3).reshape(devices, EXTENDED, channels)
        second = layer_out + lax.map(step_one, (edges, out_ext, nbr_slots))
        return atom_energy(layer_out.reshape(-1, channels), second.reshape(-1, channels), read_first, read_hidden, read_last)
    atom_e, pullback = jax.vjp(energies_of, edge_vec)
    edge_grad, = pullback(jnp.ones_like(atom_e))
    scattered = jax.vmap(scatter_edges)(nbr_slots, edge_grad)
    own_grad = scattered[:, :atom_count] - lax.optimization_barrier(jnp.sum(edge_grad, axis=2)).transpose(0, 2, 1)
    returned = return_rows(scattered[:, atom_count:].reshape(dev_grid + (6 * FACE_ATOMS, 3)), cell_order)
    forces = -(own_grad + returned)
    forces = forces.transpose(2, 0, 1).reshape(3, ATOMS)
    outer_sums = -jnp.einsum('dakx,dbkx->abdx', edge_vec, edge_grad, precision=precise).reshape(9, ATOMS)
    member = (struct_ids[None] == jnp.arange(STRUCTS)[:, None]).astype(jnp.float32)
    energies = matmul(member, atom_e)
    virials = matmul(outer_sums, member.T)
    return (energies, virials, forces)
```

```python
import functools
import math

import jax
import jax.numpy as jnp
from jax import lax
from jax.experimental import pallas as pl
from jax.experimental.pallas import tpu as pltpu
from jax.sharding import PartitionSpec as P

AXES = ("gx", "gy", "gz")
SLAB_STRUCTS = 4
LANES = 128
EDGE_ROWS = 16

cutoff = 6.0
box_side = 4.5
soften = 0.25
amplitude = math.sqrt(2.0 / cutoff)

F32 = jnp.float32
BF16 = jnp.bfloat16
NN = (((1,), (0,)), ((), ()))
NT = (((1,), (1,)), ((), ()))
TN = (((0,), (0,)), ((), ()))


def dot(left, right, dims=NN):
    return lax.dot_general(left, right, dims, preferred_element_type=F32)


def split2(x):
    high = x.astype(BF16)
    return high, (x - high.astype(F32)).astype(BF16)


def split3(x):
    high = x.astype(BF16).astype(F32)
    rest = x - high
    middle = rest.astype(BF16).astype(F32)
    return high, middle, rest - middle


def left3(x):
    high, low = split2(x)
    return jnp.concatenate([high, high, low], axis=1)


def right3(x):
    high, low = split2(x)
    return jnp.concatenate([high, low, high], axis=0)


def iota(shape, axis):
    return lax.broadcasted_iota(jnp.int32, shape, axis)


def has_bit(lanes, group):
    per_cell = LANES // 8
    width = per_cell * 2 ** (3 - group)
    return (lanes & width) != 0


def pack_kernel(pos_ref, species_ref, cells_ref, nbr_ref, struct_ref, out_ref):
    atoms = pos_ref.shape[1]
    per_cell = atoms // 8
    place = (iota((atoms, atoms), 0) == cells_ref[...]).astype(F32).astype(BF16)
    lanes = iota((8, atoms), 1)
    inverse = dot(lanes.astype(F32).astype(BF16), place, NT)
    slots = nbr_ref[...]
    hits = jnp.concatenate(
        [(iota((atoms, atoms), 0) == slots[k : k + 1, :]).astype(F32).astype(BF16) for k in range(slots.shape[0])],
        axis=1,
    )
    found = dot(inverse.astype(BF16), hits)
    own = jnp.concatenate(
        [found[0:1, k * atoms : (k + 1) * atoms] for k in range(slots.shape[0])], axis=0
    )
    face_atoms = 4 * per_cell
    beyond = jnp.maximum(slots - atoms, 0)
    face = beyond // face_atoms
    spot = beyond - face * face_atoms
    upper = 1 - (face & 1)
    axis = face // 2
    along_x = upper * 4 * per_cell + spot
    along_y = (spot // (2 * per_cell)) * (4 * per_cell) + upper * 2 * per_cell + spot % (2 * per_cell)
    along_z = (spot // per_cell) * (2 * per_cell) + upper * per_cell + spot % per_cell
    cell = jnp.where(axis == 0, along_x, jnp.where(axis == 1, along_y, along_z))
    is_own = slots < atoms
    group = jnp.where(is_own, 0, axis + 1).astype(F32)
    cell = jnp.where(is_own, own, cell.astype(F32))
    high, middle, low = split3(pos_ref[...])
    blank = jnp.zeros((1, atoms), F32)
    rows = jnp.concatenate(
        [
            high,
            species_ref[...].astype(F32),
            struct_ref[...].astype(F32),
            middle,
            low,
            blank,
            blank,
            blank,
            blank,
            blank,
            cell,
            group,
        ],
        axis=0,
    )
    moved = dot(rows.astype(BF16), place)
    first = moved[0:8, :]
    shifted = jnp.concatenate([moved[5:11, :], jnp.zeros((2, atoms), F32)], axis=0)
    middle_rows = jnp.where(iota((8, atoms), 0) < 3, shifted, 0.0)
    low_rows = jnp.where(
        iota((8, atoms), 0) < 3, jnp.concatenate([moved[8:11, :], jnp.zeros((5, atoms), F32)], axis=0), 0.0
    )
    head = jnp.where(iota((8, atoms), 0) < 5, first, 0.0) + middle_rows + low_rows
    tail = moved[16:24, :] + float(atoms) * moved[24:32, :]
    chunk = jnp.concatenate([head, tail], axis=0)

    def store(device, carry):
        out_ref[device] = chunk
        return carry

    lax.fori_loop(0, out_ref.shape[0], store, 0)


def end_kernel(structs, got_ref, cells_ref, energy_ref, virial_ref, force_ref):
    devices, _, atoms = got_ref.shape
    step = 8

    def add(index, totals):
        return tuple(
            total + got_ref[index * step + j] for j, total in enumerate(totals)
        )

    totals = lax.fori_loop(
        0, devices // step, add, tuple(jnp.zeros((8, atoms), F32) for _ in range(step))
    )
    while len(totals) > 1:
        totals = tuple(totals[i] + totals[i + 1] for i in range(0, len(totals), 2))
    total = totals[0]
    place = (iota((atoms, atoms), 0) == cells_ref[...]).astype(F32).astype(BF16)
    parts = jnp.concatenate(split3(total), axis=0).astype(BF16)
    moved = dot(parts, place, NT)
    force_ref[...] = (moved[0:8] + moved[8:16] + moved[16:24])[0:3]
    per_row = LANES // structs
    for j in range(10):
        row, column = 3 + j // per_row, (j % per_row) * structs
        value = total[row : row + 1, column : column + structs]
        if j == 0:
            energy_ref[...] = value
        else:
            virial_ref[j - 1 : j, :] = value


def centre_offsets():
    units = [(1, 0, 0), (0, 1, 0), (0, 0, 1)]
    minus = [tuple(-v for v in unit) for unit in units]
    return units, minus


def plus(a, b):
    return tuple(x + y for x, y in zip(a, b))


def main_kernel(
    sizes,
    structs,
    elements,
    got_ref,
    embed_ref,
    up_ref,
    rad_in_ref,
    rad_out_ref,
    mix_ref,
    first_ref,
    hidden_ref,
    last_ref,
    out_ref,
    table_ref,
    radial_ref,
    picked_ref,
    spread_ref,
    grad_high_ref,
    grad_low_ref,
    slots_ref,
    full_ref,
    feats_ref,
):
    atoms = LANES
    neigh = got_ref.shape[1] - 8
    edges = neigh * atoms
    width = up_ref.shape[2]
    radial_hidden = rad_in_ref.shape[2]
    scaling = 1.0 / math.sqrt(neigh)
    lanes8 = iota((8, atoms), 1)
    rows8 = iota((8, atoms), 0)
    units, minus = centre_offsets()
    home = (0, 0, 0)
    here = [lax.axis_index(axis) for axis in AXES]

    def device(offset):
        index = 0
        for place, step, size in zip(here, offset, sizes):
            index = index * size + lax.rem(place + step + 2 * size, size)
        return index

    names = {}

    def device_of(offset):
        if offset not in names:
            names[offset] = device(offset)
        return names[offset]

    def head(offset):
        return got_ref[device_of(offset), 0:8, :]

    def table(centre):
        groups = [head(centre)]
        for q in (1, 2, 3):
            move = jnp.where(rows8 == q - 1, box_side, 0.0)
            groups.append(
                jnp.where(
                    has_bit(lanes8, q),
                    head(plus(centre, minus[q - 1])) - move,
                    head(plus(centre, units[q - 1])) + move,
                )
            )
        return [jnp.concatenate(split3(group), axis=0) for group in groups]

    def transposed(x):
        return jnp.transpose(x)

    padded = table_ref.shape[0]
    table_ref[...] = jnp.zeros_like(table_ref)
    table_ref[0:elements, :] = embed_ref[...]
    embed = table_ref[...]
    up_t = [left3(transposed(up_ref[l])) for l in (0, 1)]
    up_back = left3(up_ref[1])
    embed_t = transposed(embed)
    embed_left = jnp.concatenate(split2(embed_t), axis=1)
    lifted_left = jnp.concatenate(split2(dot(up_t[0], right3(embed_t))), axis=1)
    mix_t = [
        left3(jnp.concatenate([transposed(mix_ref[l, j]) for j in range(3)], axis=1)) for l in (0, 1)
    ]
    mix_back = [left3(mix_ref[l].reshape(3 * width, width)) for l in (0, 1)]
    out_t, out_back, out_high, in_left, in_back = [], [], [], [], []
    for l in (0, 1):
        w_out = rad_out_ref[l]
        out_t.append(left3(transposed(w_out)))
        high, low = split2(w_out)
        out_back.append(jnp.concatenate([high, low], axis=0))
        out_high.append(high)
        w_in = rad_in_ref[l]
        high, low = split3(w_in)[0], w_in - w_in.astype(BF16).astype(F32)
        in_left.append(jnp.concatenate([high, high, low], axis=0).astype(BF16))
        in_back.append(left3(w_in))

    def per_edge(row):
        return jnp.concatenate([row] * neigh, axis=1)

    def flat(rows):
        return jnp.concatenate([rows[k : k + 1, :] for k in range(neigh)], axis=1)

    def fold(x):
        total = x[:, 0:atoms]
        for k in range(1, neigh):
            total = total + x[:, k * atoms : (k + 1) * atoms]
        return total

    tall = iota((8, edges), 0)
    order = (tall + 1).astype(F32)
    tables = {}

    def table_of(centre):
        if centre not in tables:
            tables[centre] = table(centre)
        return tables[centre]

    blocks = []
    for block in range(4):
        if block == 0:
            centres = [home]
            slots = got_ref[device_of(home), 8 : 8 + neigh, :]
            base = head(home)
        else:
            centres = [units[block - 1], minus[block - 1]]
            bit = has_bit(lanes8, block)
            slots = jnp.where(
                bit,
                got_ref[device_of(centres[1]), 8 : 8 + neigh, :],
                got_ref[device_of(centres[0]), 8 : 8 + neigh, :],
            )
            base = jnp.where(bit, head(centres[1]), head(centres[0]))
        slots = flat(slots.astype(jnp.int32))
        cell, group = slots & (atoms - 1), slots // atoms
        hits = (iota((atoms, edges), 0) == cell).astype(F32).astype(BF16)
        slots_ref[block] = hits
        stack = []
        for centre in centres:
            stack += table_of(centre)
        found = dot(jnp.concatenate(stack, axis=0).astype(BF16), hits)
        combo = jnp.broadcast_to(group, (8, edges))
        if block:
            combo = combo + per_edge(jnp.where(bit, 4, 0))
        far = None
        for j in range(len(stack)):
            part = found[24 * j : 24 * j + 8] + found[24 * j + 8 : 24 * j + 16] + found[24 * j + 16 : 24 * j + 24]
            far = part if far is None else jnp.where(combo == j, part, far)
        vec = jnp.where(tall < 3, far - per_edge(base), 0.0)
        square = jnp.sum(vec * vec, axis=0, keepdims=True) + soften
        square = jnp.broadcast_to(square, (8, edges))
        radius = jnp.sqrt(square)
        inverse = 1.0 / radius
        turn = order * (jnp.minimum(radius, cutoff) * (1.0 / cutoff))
        whole = jnp.floor(turn + 0.5)
        part = (turn - whole) * math.pi
        sign = 1.0 - 2.0 * (whole - 2.0 * jnp.floor(whole * 0.5))
        p2 = part * part
        sine = part * (
            1.0
            + p2 * (-1.0 / 6 + p2 * (1.0 / 120 + p2 * (-1.0 / 5040 + p2 * (1.0 / 362880 - p2 * (1.0 / 39916800)))))
        )
        cosine = 1.0 + p2 * (
            -0.5
            + p2 * (1.0 / 24 + p2 * (-1.0 / 720 + p2 * (1.0 / 40320 + p2 * (-1.0 / 3628800 + p2 * (1.0 / 479001600)))))
        )
        sine, cosine = sine * sign * amplitude, cosine * sign * amplitude
        inside = jnp.maximum(1.0 - square * (1.0 / (cutoff * cutoff)), 0.0)
        envelope = inside * inside
        over = sine * inverse
        bessel = over * envelope
        slope = (
            (order * (math.pi / cutoff) * cosine - over) * inverse * envelope
            - sine * inside * (4.0 / (cutoff * cutoff))
        )
        high = bessel.astype(BF16).astype(F32)
        bessel_right = jnp.concatenate([high, bessel - high, high], axis=0).astype(BF16)
        direction = vec * inverse
        blocks.append(
            dict(
                base=base,
                combo=combo,
                far=far,
                vec=vec,
                inverse=inverse,
                slope=slope,
                bessel=bessel_right,
                direction=direction,
                struct=base[4:5, :],
            )
        )

    tile = 32

    def spread(block, m, k):
        row = blocks[block]["direction"][m : m + 1, k * atoms : (k + 1) * atoms]
        return jnp.broadcast_to(row, (8, atoms))

    for block in range(4):
        for m in range(3):
            for k in range(neigh):
                spread_ref[block, m * neigh + k] = spread(block, m, k)

    def wide(x):
        return jnp.concatenate([x] * (tile // 8), axis=0)

    def interact(layer, block, saved):
        pre = dot(in_left[layer], blocks[block]["bessel"], TN)
        sigma = 1.0 / (1.0 + jnp.exp(-pre))
        active = pre * sigma
        gain = sigma * (1.0 + pre * (1.0 - sigma))
        radial_ref[saved] = dot(out_t[layer], right3(active))
        scalars, squares = [], []
        vectors = [[], [], []]
        for start in range(0, width, tile):
            scalar = None
            vector = [None, None, None]
            for k in range(neigh):
                cut = pl.ds(k * atoms, atoms)
                rows = picked_ref[saved, pl.ds(start, tile), cut]
                zero = radial_ref[saved, pl.ds(start, tile), cut] * rows
                one = radial_ref[saved, pl.ds(width + start, tile), cut] * rows
                scalar = zero if scalar is None else scalar + zero
                for m in range(3):
                    term = wide(spread_ref[block, m * neigh + k]) * one
                    vector[m] = term if vector[m] is None else vector[m] + term
            scalars.append(scalar * scaling)
            for m in range(3):
                vectors[m].append(vector[m] * scaling)
        scalar = jnp.concatenate(scalars, axis=0)
        vector = [jnp.concatenate(v, axis=0) for v in vectors]
        square = vector[0] * vector[0] + vector[1] * vector[1] + vector[2] * vector[2]
        mixed = dot(mix_t[layer], right3(jnp.concatenate([scalar, square, scalar * scalar], axis=0)))
        return mixed, (gain, scalar, vector)

    def pull(layer, block, saved, kept, cotangent, want_picked):
        gain, scalar, vector = kept
        d = dot(mix_back[layer], right3(cotangent))
        d_scalar = (d[0:width] + 2.0 * scalar * d[2 * width : 3 * width]) * scaling
        factor = (2.0 * scaling) * d[width : 2 * width]
        d_vector = [v * factor for v in vector]
        toward = [[jnp.zeros((8, atoms), F32) for _ in range(neigh)] for _ in range(3)]
        for start in range(0, width, tile):
            part = slice(start, start + tile)
            for k in range(neigh):
                cut = pl.ds(k * atoms, atoms)
                rows = picked_ref[saved, pl.ds(start, tile), cut]
                one = radial_ref[saved, pl.ds(width + start, tile), cut]
                both = one * rows
                through = None
                for m in range(3):
                    term = wide(spread_ref[block, m * neigh + k]) * d_vector[m][part]
                    through = term if through is None else through + term
                    push = d_vector[m][part] * both
                    total = push[0:8]
                    for j in range(8, tile, 8):
                        total = total + push[j : j + 8]
                    toward[m][k] = toward[m][k] + total
                high, low = split2(d_scalar[part] * rows)
                grad_high_ref[pl.ds(start, tile), cut] = high
                grad_low_ref[pl.ds(start, tile), cut] = low
                high, low = split2(through * rows)
                grad_high_ref[pl.ds(width + start, tile), cut] = high
                grad_low_ref[pl.ds(width + start, tile), cut] = low
                if want_picked:
                    picked_ref[saved, pl.ds(start, tile), cut] = (
                        radial_ref[saved, pl.ds(start, tile), cut] * d_scalar[part] + one * through
                    )
        grad_high = grad_high_ref[...]
        both = dot(out_back[layer], grad_high)
        d_active = both[0:radial_hidden] + both[radial_hidden:] + dot(out_high[layer], grad_low_ref[...])
        d_bessel = dot(in_back[layer], right3(d_active * gain))
        own = blocks[block]
        d_radius = jnp.sum(d_bessel * own["slope"], axis=0, keepdims=True)
        lines = [
            jnp.concatenate([jnp.sum(toward[m][k], axis=0, keepdims=True) for k in range(neigh)], axis=1)
            for m in range(3)
        ]
        d_direction = jnp.concatenate(lines + [jnp.zeros((5, edges), F32)], axis=0)
        inverse, direction = own["inverse"], own["direction"]
        radial_part = d_radius - jnp.sum(d_direction * direction, axis=0, keepdims=True) * inverse
        return d_direction * inverse + radial_part * direction

    kept0 = []
    for block in range(4):
        far, base = blocks[block]["far"], blocks[block]["base"]
        kinds = far[3:4, :].astype(jnp.int32)
        hits = (iota((padded, edges), 0) == kinds).astype(F32).astype(BF16)
        picked_ref[block] = dot(lifted_left, jnp.concatenate([hits, hits], axis=0))
        mixed, kept = interact(0, block, block)
        kept0.append(kept)
        kinds = base[3:4, :].astype(jnp.int32)
        hits = (iota((padded, atoms), 0) == kinds).astype(F32).astype(BF16)
        feats_ref[:, pl.ds(block * atoms, atoms)] = (
            dot(embed_left, jnp.concatenate([hits, hits], axis=0)) + mixed
        )

    own_slots = flat(got_ref[device_of(home), 8 : 8 + neigh, :].astype(jnp.int32))
    full_ref[...] = (iota((4 * atoms, edges), 0) == own_slots).astype(F32).astype(BF16)
    feats = feats_ref[...]
    lifted = dot(up_t[1], right3(feats))
    high, low = split2(lifted)
    both = dot(jnp.concatenate([high, low], axis=0), full_ref[...])
    picked_ref[4] = both[0:width] + both[width:]
    mixed, kept1 = interact(1, 0, 4)
    layer_out = feats[:, 0:atoms]
    second = layer_out + mixed

    w_hidden = hidden_ref[...]
    pre = dot(left3(transposed(w_hidden)), right3(second))
    sigma = 1.0 / (1.0 + jnp.exp(-pre))
    gain = sigma * (1.0 + pre * (1.0 - sigma))
    first_row = jnp.broadcast_to(first_ref[...], (8, width))
    last_row = jnp.broadcast_to(last_ref[...], (8, last_ref.shape[1]))
    atom_energy = dot(left3(first_row), right3(layer_out)) + dot(left3(last_row), right3(pre * sigma))
    first_column = transposed(jnp.broadcast_to(first_ref[...], (atoms, width)))
    last_column = transposed(jnp.broadcast_to(last_ref[...], (atoms, last_ref.shape[1])))
    d_second = dot(left3(w_hidden), right3(last_column * gain))

    edge_grad_one = pull(1, 0, 4, kept1, d_second, True)
    high, low = split2(picked_ref[4])
    back = dot(jnp.concatenate([high, low], axis=0), full_ref[...], NT)
    d_feats = dot(up_back, right3(back[0:width] + back[width:]))

    forces = {}

    def push(offset, value):
        forces[offset] = forces[offset] + value if offset in forces else value

    sums = None
    for block in range(4):
        cotangent = d_feats[:, block * atoms : (block + 1) * atoms]
        if block == 0:
            cotangent = cotangent + d_second + first_column
        grad = pull(0, block, block, kept0[block], cotangent, False)
        if block == 0:
            grad = grad + edge_grad_one
        own = blocks[block]
        centres = [home] if block == 0 else [units[block - 1], minus[block - 1]]
        pulled = fold(grad)
        if block == 0:
            push(home, pulled)
        else:
            bit = has_bit(lanes8, block)
            push(centres[1], jnp.where(bit, pulled, 0.0))
            push(centres[0], jnp.where(bit, 0.0, pulled))
        high = grad.astype(BF16).astype(F32)
        pair = jnp.concatenate([high[0:4], (grad - high)[0:4]], axis=0)
        stack = [jnp.where(own["combo"] == j, pair, 0.0) for j in range(4 * len(centres))]
        landed = dot(jnp.concatenate(stack, axis=0).astype(BF16), slots_ref[block], NT)
        for c, centre in enumerate(centres):
            for q in range(4):
                j = 4 * c + q
                value = -landed[8 * j : 8 * j + 8]
                if q == 0:
                    push(centre, value)
                else:
                    bit = has_bit(lanes8, q)
                    push(plus(centre, minus[q - 1]), jnp.where(bit, value, 0.0))
                    push(plus(centre, units[q - 1]), jnp.where(bit, 0.0, value))
        rows = []
        for r in range(3):
            rows.append(-fold(jnp.broadcast_to(own["vec"][r : r + 1, :], (8, edges)) * grad))
        if block == 0:
            rows.append(atom_energy)
        rows = jnp.concatenate(rows, axis=0)
        member = (own["struct"].astype(jnp.int32) == (iota((atoms, atoms), 0) & (structs - 1))).astype(F32)
        high, low = split2(rows)
        got = dot(jnp.concatenate([high, low], axis=0), member.astype(BF16), NT)
        got = got[0 : rows.shape[0]] + got[rows.shape[0] :]
        if block == 0:
            energy_row = got[24:25]
            sums = got[0:24]
        else:
            sums = sums + got

    per_row = LANES // structs
    lane_row = iota((1, atoms), 1) // structs
    packed = []
    for row in range(-(-10 // per_row)):
        line = jnp.zeros((1, atoms), F32)
        for j in range(row * per_row, min(10, (row + 1) * per_row)):
            if j == 0:
                value = energy_row
            else:
                r, t = divmod(j - 1, 3)
                value = sums[8 * r + t : 8 * r + t + 1]
            line = line + jnp.where(lane_row == j - row * per_row, value, 0.0)
        packed.append(line)
    packed.append(jnp.zeros((5 - len(packed), atoms), F32)) if len(packed) < 5 else None
    common = jnp.concatenate([jnp.zeros((3, atoms), F32)] + packed, axis=0)

    def store(index, carry):
        out_ref[index] = common
        return carry

    lax.fori_loop(0, out_ref.shape[0], store, 0)
    for offset, value in forces.items():
        value = jnp.where(rows8 < 3, value + jnp.concatenate([value[4:8], value[0:4]], axis=0), 0.0)
        index = device_of(offset)
        out_ref[index] = out_ref[index] + value


def whole(memory_space=pltpu.VMEM):
    return pl.BlockSpec(memory_space=memory_space)


def shards(
    sizes,
    positions,
    species,
    cell_map,
    neighbours,
    struct_ids,
    embed,
    w_up,
    w_rad_in,
    w_rad_out,
    w_mix,
    read_first,
    read_hidden,
    read_last,
):
    devices = math.prod(sizes)
    atoms = positions.shape[1]
    neigh = neighbours.shape[0]
    width = w_up.shape[2]
    structs = SLAB_STRUCTS * sizes[0]
    elements = embed.shape[0]
    padded = -(-elements // LANES) * LANES
    edges = neigh * atoms
    params = pltpu.CompilerParams(vmem_limit_bytes=60 << 20)
    sent = pl.pallas_call(
        pack_kernel,
        out_shape=jax.ShapeDtypeStruct((devices, 8 + neigh, atoms), F32),
        in_specs=[whole()] * 5,
        out_specs=whole(),
        name="pack",
    )(positions, species.reshape(1, -1), cell_map, neighbours, struct_ids.reshape(1, -1))
    got = lax.all_to_all(sent, AXES, 0, 0, tiled=True)
    parts = pl.pallas_call(
        functools.partial(main_kernel, sizes, structs, elements),
        out_shape=jax.ShapeDtypeStruct((devices, 8, atoms), F32),
        in_specs=[whole()] * 9,
        out_specs=whole(),
        scratch_shapes=[
            pltpu.VMEM((padded, width), F32),
            pltpu.VMEM((5, 2 * width, edges), F32),
            pltpu.VMEM((5, width, edges), F32),
            pltpu.VMEM((4, 3 * neigh, 8, atoms), F32),
            pltpu.VMEM((2 * width, edges), BF16),
            pltpu.VMEM((2 * width, edges), BF16),
            pltpu.VMEM((4, atoms, edges), BF16),
            pltpu.VMEM((4 * atoms, edges), BF16),
            pltpu.VMEM((width, 4 * atoms), F32),
        ],
        compiler_params=params,
        name="forces",
    )(
        got,
        embed,
        w_up,
        w_rad_in,
        w_rad_out,
        w_mix,
        read_first.reshape(1, -1),
        read_hidden,
        read_last.reshape(1, -1),
    )
    back = lax.all_to_all(parts, AXES, 0, 0, tiled=True)
    energies, virials, forces = pl.pallas_call(
        functools.partial(end_kernel, structs),
        out_shape=(
            jax.ShapeDtypeStruct((1, structs), F32),
            jax.ShapeDtypeStruct((9, structs), F32),
            jax.ShapeDtypeStruct((3, atoms), F32),
        ),
        in_specs=[whole()] * 2,
        out_specs=(whole(),) * 3,
        name="finish",
    )(back, cell_map)
    return energies.reshape(-1), virials, forces


def solution(mesh):
    sizes = tuple(mesh.shape[axis] for axis in AXES)
    return jax.shard_map(
        functools.partial(shards, sizes),
        mesh=mesh,
        in_specs=(
            P(None, AXES),
            P(AXES),
            P(AXES, None),
            P(None, AXES),
            P(AXES),
            P(),
            P(),
            P(),
            P(),
            P(),
            P(),
            P(),
            P(),
        ),
        out_specs=(P(), P(), P(None, AXES)),
        check_vma=False,
    )
```

```python
import functools
import math

import jax
import jax.numpy as jnp
from jax import lax
from jax.experimental import pallas as pl
from jax.experimental.pallas import tpu as pltpu
from jax.sharding import PartitionSpec as P

AXES = ("gx", "gy", "gz")
SLAB_STRUCTS = 4
LANES = 128
HEAD_ROWS = 5
TAIL_ROWS = 3

cutoff = 6.0
box_side = 4.5
soften = 0.25
amplitude = math.sqrt(2.0 / cutoff)

F32 = jnp.float32
BF16 = jnp.bfloat16
NN = (((1,), (0,)), ((), ()))
NT = (((1,), (1,)), ((), ()))
TN = (((0,), (0,)), ((), ()))


def dot(left, right, dims=NN):
    return lax.dot_general(left, right, dims, preferred_element_type=F32)


def split2(x):
    high = x.astype(BF16)
    return high, (x - high.astype(F32)).astype(BF16)


def split3(x):
    high = x.astype(BF16).astype(F32)
    rest = x - high
    middle = rest.astype(BF16).astype(F32)
    return high, middle, rest - middle


def left3(x):
    high, low = split2(x)
    return jnp.concatenate([high, high, low], axis=1)


def right3(x):
    high, low = split2(x)
    return jnp.concatenate([high, low, high], axis=0)


def iota(shape, axis):
    return lax.broadcasted_iota(jnp.int32, shape, axis)


def has_bit(lanes, group):
    per_cell = LANES // 8
    width = per_cell * 2 ** (3 - group)
    return (lanes & width) != 0


def pack_kernel(pos_ref, species_ref, cells_ref, nbr_ref, struct_ref, out_ref):
    atoms = pos_ref.shape[1]
    per_cell = atoms // 8
    place = (iota((atoms, atoms), 0) == cells_ref[...]).astype(F32).astype(BF16)
    lanes = iota((8, atoms), 1)
    inverse = dot(lanes.astype(F32).astype(BF16), place, NT)
    slots = nbr_ref[...]
    hits = jnp.concatenate(
        [(iota((atoms, atoms), 0) == slots[k : k + 1, :]).astype(F32).astype(BF16) for k in range(slots.shape[0])],
        axis=1,
    )
    found = dot(inverse.astype(BF16), hits)
    own = jnp.concatenate(
        [found[0:1, k * atoms : (k + 1) * atoms] for k in range(slots.shape[0])], axis=0
    )
    face_atoms = 4 * per_cell
    beyond = jnp.maximum(slots - atoms, 0)
    face = beyond // face_atoms
    spot = beyond - face * face_atoms
    upper = 1 - (face & 1)
    axis = face // 2
    along_x = upper * 4 * per_cell + spot
    along_y = (spot // (2 * per_cell)) * (4 * per_cell) + upper * 2 * per_cell + spot % (2 * per_cell)
    along_z = (spot // per_cell) * (2 * per_cell) + upper * per_cell + spot % per_cell
    cell = jnp.where(axis == 0, along_x, jnp.where(axis == 1, along_y, along_z))
    is_own = slots < atoms
    group = jnp.where(is_own, 0, axis + 1).astype(F32)
    cell = jnp.where(is_own, own, cell.astype(F32))
    parts = jnp.concatenate(
        [*split3(pos_ref[...]), species_ref[...].astype(F32), struct_ref[...].astype(F32)], axis=0
    )
    blank = jnp.zeros((16 - parts.shape[0], atoms), F32)
    moved = dot(jnp.concatenate([parts, blank, cell, group], axis=0).astype(BF16), place)
    chunk = jnp.concatenate(
        [
            moved[0:3] + moved[3:6] + moved[6:9],
            moved[9:11],
            moved[16 : 16 + slots.shape[0]] + float(atoms) * moved[16 + slots.shape[0] :],
        ],
        axis=0,
    )
    rows = [chunk[j : j + 1, :] for j in range(chunk.shape[0])]

    def store(device, carry):
        for j, row in enumerate(rows):
            out_ref[device, j] = row
        return carry

    lax.fori_loop(0, out_ref.shape[0], store, 0)


def end_kernel(structs, got_ref, cells_ref, energy_ref, virial_ref, force_ref):
    devices, count, _, atoms = got_ref.shape
    step = 8

    def add(index, totals):
        return tuple(total + got_ref[index * step + j] for j, total in enumerate(totals))

    totals = lax.fori_loop(
        0, devices // step, add, tuple(jnp.zeros((count, 1, atoms), F32) for _ in range(step))
    )
    while len(totals) > 1:
        totals = tuple(totals[i] + totals[i + 1] for i in range(0, len(totals), 2))
    lines = [totals[0][j] for j in range(count)]
    total = jnp.concatenate(lines[0:3] + [jnp.zeros((5, atoms), F32)], axis=0)
    place = (iota((atoms, atoms), 0) == cells_ref[...]).astype(F32).astype(BF16)
    parts = jnp.concatenate(split3(total), axis=0).astype(BF16)
    moved = dot(parts, place, NT)
    force_ref[...] = (moved[0:8] + moved[8:16] + moved[16:24])[0:3]
    per_row = LANES // structs
    for j in range(10):
        row, column = 3 + j // per_row, (j % per_row) * structs
        value = lines[row][:, column : column + structs]
        if j == 0:
            energy_ref[...] = value
        else:
            virial_ref[j - 1 : j, :] = value


def centre_offsets():
    units = [(1, 0, 0), (0, 1, 0), (0, 0, 1)]
    minus = [tuple(-v for v in unit) for unit in units]
    return units, minus


def plus(a, b):
    return tuple(x + y for x, y in zip(a, b))


def prep_kernel(
    scaling,
    embed_ref,
    up_ref,
    rad_in_ref,
    rad_out_ref,
    mix_ref,
    first_ref,
    hidden_ref,
    last_ref,
    embed_left_ref,
    lifted_left_ref,
    up_left_ref,
    up_back_ref,
    mix_left_ref,
    mix_back_ref,
    out_left_ref,
    out_back_ref,
    in_left_ref,
    in_back_ref,
    read_left_ref,
    read_back_ref,
    row_left_ref,
    column_ref,
    table_ref,
):
    elements = embed_ref.shape[0]
    width = up_ref.shape[2]
    table_ref[...] = jnp.zeros_like(table_ref)
    table_ref[0:elements, :] = embed_ref[...]
    embed_t = jnp.transpose(table_ref[...])
    embed_left_ref[...] = jnp.concatenate(split2(embed_t), axis=1)
    lifted_left_ref[...] = jnp.concatenate(
        split2(dot(left3(jnp.transpose(up_ref[0])), right3(embed_t))), axis=1
    )
    up_left_ref[...] = left3(jnp.transpose(up_ref[1]))
    up_back_ref[...] = left3(up_ref[1])
    for l in (0, 1):
        mix_left_ref[l] = left3(jnp.concatenate([jnp.transpose(mix_ref[l, j]) for j in range(3)], axis=1))
        mix_back_ref[l] = left3(mix_ref[l].reshape(3 * width, width))
        w_out = rad_out_ref[l] * scaling
        out_left_ref[l] = left3(jnp.transpose(w_out))
        out_back_ref[l] = jnp.concatenate(split2(w_out), axis=0)
        w_in = rad_in_ref[l]
        high = w_in.astype(BF16).astype(F32)
        in_left_ref[l] = jnp.concatenate([high, high, w_in - high], axis=0).astype(BF16)
        in_back_ref[l] = left3(w_in)
    w_hidden = hidden_ref[...]
    read_left_ref[...] = left3(jnp.transpose(w_hidden))
    read_back_ref[...] = left3(w_hidden)
    first_row = jnp.broadcast_to(first_ref[...], (8, width))
    last_row = jnp.broadcast_to(last_ref[...], (8, last_ref.shape[1]))
    row_left_ref[...] = jnp.concatenate([left3(first_row), left3(last_row)], axis=1)
    column_ref[0:width, :] = jnp.transpose(jnp.broadcast_to(first_ref[...], (LANES, width)))
    column_ref[width:, :] = jnp.transpose(jnp.broadcast_to(last_ref[...], (LANES, last_ref.shape[1])))


def main_kernel(
    sizes,
    structs,
    got_ref,
    embed_left_ref,
    lifted_left_ref,
    up_left_ref,
    up_back_ref,
    mix_left_ref,
    mix_back_ref,
    out_left_ref,
    out_back_ref,
    in_left_ref,
    in_back_ref,
    read_left_ref,
    read_back_ref,
    row_left_ref,
    column_ref,
    out_ref,
    radial_ref,
    picked_ref,
    spread_ref,
    grad_high_ref,
    grad_low_ref,
    slots_ref,
    full_ref,
    feats_ref,
):
    atoms = LANES
    neigh = got_ref.shape[1] - HEAD_ROWS
    edges = neigh * atoms
    width = up_left_ref.shape[0]
    radial_hidden = in_left_ref.shape[2]
    padded = embed_left_ref.shape[1] // 2
    read_width = read_left_ref.shape[0]
    lanes8 = iota((8, atoms), 1)
    rows8 = iota((8, atoms), 0)
    units, minus = centre_offsets()
    home = (0, 0, 0)
    here = [lax.axis_index(axis) for axis in AXES]

    def device(offset):
        index = 0
        for place, step, size in zip(here, offset, sizes):
            index = index * size + lax.rem(place + step + 2 * size, size)
        return index

    names = {}

    def device_of(offset):
        if offset not in names:
            names[offset] = device(offset)
        return names[offset]

    def head(offset):
        index = device_of(offset)
        rows = [got_ref[index, j] for j in range(HEAD_ROWS)]
        return jnp.concatenate(rows + [jnp.zeros((8 - HEAD_ROWS, atoms), F32)], axis=0)

    heads = {}

    def head_of(offset):
        if offset not in heads:
            heads[offset] = head(offset)
        return heads[offset]

    def slots_of(offset):
        index = device_of(offset)
        rows = [got_ref[index, HEAD_ROWS + k] for k in range(neigh)]
        return jnp.concatenate(rows, axis=1)

    def table(centre):
        groups = [head_of(centre)]
        for q in (1, 2, 3):
            move = jnp.where(rows8 == q - 1, box_side, 0.0)
            groups.append(
                jnp.where(
                    has_bit(lanes8, q),
                    head_of(plus(centre, minus[q - 1])) - move,
                    head_of(plus(centre, units[q - 1])) + move,
                )
            )
        return [jnp.concatenate(split3(group), axis=0) for group in groups]

    def per_edge(row):
        return jnp.concatenate([row] * neigh, axis=1)

    def fold(x):
        total = x[:, 0:atoms]
        for k in range(1, neigh):
            total = total + x[:, k * atoms : (k + 1) * atoms]
        return total

    tall = iota((8, edges), 0)
    order = (tall + 1).astype(F32)
    tables = {}

    def table_of(centre):
        if centre not in tables:
            tables[centre] = table(centre)
        return tables[centre]

    blocks = []
    for block in range(4):
        if block == 0:
            centres = [home]
            slots = slots_of(home)
            base = head_of(home)
        else:
            centres = [units[block - 1], minus[block - 1]]
            bit = has_bit(lanes8, block)
            slots = jnp.where(per_edge(bit[0:1]), slots_of(centres[1]), slots_of(centres[0]))
            base = jnp.where(bit, head_of(centres[1]), head_of(centres[0]))
        slots = slots.astype(jnp.int32)
        if block == 0:
            own_slots = slots
        cell, group = slots & (atoms - 1), slots // atoms
        hits = (iota((atoms, edges), 0) == cell).astype(F32).astype(BF16)
        slots_ref[block] = hits
        stack = []
        for centre in centres:
            stack += table_of(centre)
        found = dot(jnp.concatenate(stack, axis=0).astype(BF16), hits)
        combo = jnp.broadcast_to(group, (8, edges))
        if block:
            combo = combo + per_edge(jnp.where(bit, 4, 0))
        far = None
        for j in range(len(stack)):
            part = found[24 * j : 24 * j + 8] + found[24 * j + 8 : 24 * j + 16] + found[24 * j + 16 : 24 * j + 24]
            far = part if far is None else jnp.where(combo == j, part, far)
        vec = jnp.where(tall < 3, far - per_edge(base), 0.0)
        square = jnp.sum(vec * vec, axis=0, keepdims=True) + soften
        square = jnp.broadcast_to(square, (8, edges))
        radius = jnp.sqrt(square)
        inverse = 1.0 / radius
        turn = order * (jnp.minimum(radius, cutoff) * (1.0 / cutoff))
        whole = jnp.floor(turn + 0.5)
        part = (turn - whole) * math.pi
        sign = 1.0 - 2.0 * (whole - 2.0 * jnp.floor(whole * 0.5))
        p2 = part * part
        sine = part * (
            1.0
            + p2 * (-1.0 / 6 + p2 * (1.0 / 120 + p2 * (-1.0 / 5040 + p2 * (1.0 / 362880 - p2 * (1.0 / 39916800)))))
        )
        cosine = 1.0 + p2 * (
            -0.5
            + p2 * (1.0 / 24 + p2 * (-1.0 / 720 + p2 * (1.0 / 40320 + p2 * (-1.0 / 3628800 + p2 * (1.0 / 479001600)))))
        )
        sine, cosine = sine * sign * amplitude, cosine * sign * amplitude
        inside = jnp.maximum(1.0 - square * (1.0 / (cutoff * cutoff)), 0.0)
        envelope = inside * inside
        over = sine * inverse
        bessel = over * envelope
        slope = (
            (order * (math.pi / cutoff) * cosine - over) * inverse * envelope
            - sine * inside * (4.0 / (cutoff * cutoff))
        )
        high = bessel.astype(BF16).astype(F32)
        bessel_right = jnp.concatenate([high, bessel - high, high], axis=0).astype(BF16)
        direction = vec * inverse
        blocks.append(
            dict(
                base=base,
                combo=combo,
                far=far,
                vec=vec,
                inverse=inverse,
                slope=slope,
                bessel=bessel_right,
                direction=direction,
                struct=base[4:5, :],
            )
        )

    tile = 32

    def spread(block, m, k):
        row = blocks[block]["direction"][m : m + 1, k * atoms : (k + 1) * atoms]
        return jnp.broadcast_to(row, (8, atoms))

    for block in range(4):
        for m in range(3):
            for k in range(neigh):
                spread_ref[block, m * neigh + k] = spread(block, m, k)

    def wide(x):
        return jnp.concatenate([x] * (tile // 8), axis=0)

    def interact(layer, block, saved):
        pre = dot(in_left_ref[layer], blocks[block]["bessel"], TN)
        sigma = 1.0 / (1.0 + jnp.exp(-pre))
        active = pre * sigma
        gain = sigma * (1.0 + pre * (1.0 - sigma))
        radial_ref[saved] = dot(out_left_ref[layer], right3(active))
        scalars, squares = [], []
        vectors = [[], [], []]
        for start in range(0, width, tile):
            scalar = None
            vector = [None, None, None]
            for k in range(neigh):
                cut = pl.ds(k * atoms, atoms)
                rows = picked_ref[saved, pl.ds(start, tile), cut]
                zero = radial_ref[saved, pl.ds(start, tile), cut] * rows
                one = radial_ref[saved, pl.ds(width + start, tile), cut] * rows
                scalar = zero if scalar is None else scalar + zero
                for m in range(3):
                    term = wide(spread_ref[block, m * neigh + k]) * one
                    vector[m] = term if vector[m] is None else vector[m] + term
            scalars.append(scalar)
            for m in range(3):
                vectors[m].append(vector[m])
        scalar = jnp.concatenate(scalars, axis=0)
        vector = [jnp.concatenate(v, axis=0) for v in vectors]
        square = vector[0] * vector[0] + vector[1] * vector[1] + vector[2] * vector[2]
        mixed = dot(mix_left_ref[layer], right3(jnp.concatenate([scalar, square, scalar * scalar], axis=0)))
        return mixed, (gain, scalar, vector)

    def pull(layer, block, saved, kept, cotangent, want_picked):
        gain, scalar, vector = kept
        d = dot(mix_back_ref[layer], right3(cotangent))
        d_scalar = d[0:width] + 2.0 * scalar * d[2 * width : 3 * width]
        factor = 2.0 * d[width : 2 * width]
        d_vector = [v * factor for v in vector]
        toward = [[jnp.zeros((8, atoms), F32) for _ in range(neigh)] for _ in range(3)]
        for start in range(0, width, tile):
            part = slice(start, start + tile)
            for k in range(neigh):
                cut = pl.ds(k * atoms, atoms)
                rows = picked_ref[saved, pl.ds(start, tile), cut]
                one = radial_ref[saved, pl.ds(width + start, tile), cut]
                both = one * rows
                through = None
                for m in range(3):
                    term = wide(spread_ref[block, m * neigh + k]) * d_vector[m][part]
                    through = term if through is None else through + term
                    push = d_vector[m][part] * both
                    total = push[0:8]
                    for j in range(8, tile, 8):
                        total = total + push[j : j + 8]
                    toward[m][k] = toward[m][k] + total
                high, low = split2(d_scalar[part] * rows)
                grad_high_ref[pl.ds(start, tile), cut] = high
                grad_low_ref[pl.ds(start, tile), cut] = low
                high, low = split2(through * rows)
                grad_high_ref[pl.ds(width + start, tile), cut] = high
                grad_low_ref[pl.ds(width + start, tile), cut] = low
                if want_picked:
                    picked_ref[saved, pl.ds(start, tile), cut] = (
                        radial_ref[saved, pl.ds(start, tile), cut] * d_scalar[part] + one * through
                    )
        grad_high = grad_high_ref[...]
        both = dot(out_back_ref[layer], grad_high)
        d_active = both[0:radial_hidden] + both[radial_hidden:] + dot(out_back_ref[layer, 0:radial_hidden], grad_low_ref[...])
        d_bessel = dot(in_back_ref[layer], right3(d_active * gain))
        own = blocks[block]
        d_radius = jnp.sum(d_bessel * own["slope"], axis=0, keepdims=True)
        lines = [
            jnp.concatenate([jnp.sum(toward[m][k], axis=0, keepdims=True) for k in range(neigh)], axis=1)
            for m in range(3)
        ]
        d_direction = jnp.concatenate(lines + [jnp.zeros((5, edges), F32)], axis=0)
        inverse, direction = own["inverse"], own["direction"]
        radial_part = d_radius - jnp.sum(d_direction * direction, axis=0, keepdims=True) * inverse
        return d_direction * inverse + radial_part * direction

    kept0 = []
    for block in range(4):
        far, base = blocks[block]["far"], blocks[block]["base"]
        kinds = far[3:4, :].astype(jnp.int32)
        hits = (iota((padded, edges), 0) == kinds).astype(F32).astype(BF16)
        picked_ref[block] = dot(lifted_left_ref[...], jnp.concatenate([hits, hits], axis=0))
        mixed, kept = interact(0, block, block)
        kept0.append(kept)
        kinds = base[3:4, :].astype(jnp.int32)
        hits = (iota((padded, atoms), 0) == kinds).astype(F32).astype(BF16)
        feats_ref[:, pl.ds(block * atoms, atoms)] = (
            dot(embed_left_ref[...], jnp.concatenate([hits, hits], axis=0)) + mixed
        )

    full_ref[...] = (iota((4 * atoms, edges), 0) == own_slots).astype(F32).astype(BF16)
    feats = feats_ref[...]
    lifted = dot(up_left_ref[...], right3(feats))
    high, low = split2(lifted)
    both = dot(jnp.concatenate([high, low], axis=0), full_ref[...])
    picked_ref[4] = both[0:width] + both[width:]
    mixed, kept1 = interact(1, 0, 4)
    layer_out = feats[:, 0:atoms]
    second = layer_out + mixed

    pre = dot(read_left_ref[...], right3(second))
    sigma = 1.0 / (1.0 + jnp.exp(-pre))
    gain = sigma * (1.0 + pre * (1.0 - sigma))
    atom_energy = dot(row_left_ref[:, 0 : 3 * width], right3(layer_out)) + dot(
        row_left_ref[:, 3 * width :], right3(pre * sigma)
    )
    first_column = column_ref[0:width, :]
    d_second = dot(read_back_ref[...], right3(column_ref[width : width + read_width, :] * gain))

    edge_grad_one = pull(1, 0, 4, kept1, d_second, True)
    high, low = split2(picked_ref[4])
    back = dot(jnp.concatenate([high, low], axis=0), full_ref[...], NT)
    d_feats = dot(up_back_ref[...], right3(back[0:width] + back[width:]))

    forces = {}

    def push(offset, value):
        forces[offset] = forces[offset] + value if offset in forces else value

    sums = None
    for block in range(4):
        cotangent = d_feats[:, block * atoms : (block + 1) * atoms]
        if block == 0:
            cotangent = cotangent + d_second + first_column
        grad = pull(0, block, block, kept0[block], cotangent, False)
        if block == 0:
            grad = grad + edge_grad_one
        own = blocks[block]
        centres = [home] if block == 0 else [units[block - 1], minus[block - 1]]
        pulled = fold(grad)
        if block == 0:
            push(home, pulled)
        else:
            bit = has_bit(lanes8, block)
            push(centres[1], jnp.where(bit, pulled, 0.0))
            push(centres[0], jnp.where(bit, 0.0, pulled))
        high = grad.astype(BF16).astype(F32)
        pair = jnp.concatenate([high[0:4], (grad - high)[0:4]], axis=0)
        stack = [jnp.where(own["combo"] == j, pair, 0.0) for j in range(4 * len(centres))]
        landed = dot(jnp.concatenate(stack, axis=0).astype(BF16), slots_ref[block], NT)
        for c, centre in enumerate(centres):
            for q in range(4):
                j = 4 * c + q
                value = -landed[8 * j : 8 * j + 8]
                if q == 0:
                    push(centre, value)
                else:
                    bit = has_bit(lanes8, q)
                    push(plus(centre, minus[q - 1]), jnp.where(bit, value, 0.0))
                    push(plus(centre, units[q - 1]), jnp.where(bit, 0.0, value))
        rows = []
        for r in range(3):
            rows.append(-fold(jnp.broadcast_to(own["vec"][r : r + 1, :], (8, edges)) * grad))
        if block == 0:
            rows.append(atom_energy)
        rows = jnp.concatenate(rows, axis=0)
        member = (own["struct"].astype(jnp.int32) == (iota((atoms, atoms), 0) & (structs - 1))).astype(F32)
        high, low = split2(rows)
        got = dot(jnp.concatenate([high, low], axis=0), member.astype(BF16), NT)
        got = got[0 : rows.shape[0]] + got[rows.shape[0] :]
        if block == 0:
            energy_row = got[24:25]
            sums = got[0:24]
        else:
            sums = sums + got

    per_row = LANES // structs
    lane_row = iota((1, atoms), 1) // structs
    packed = []
    for row in range(-(-10 // per_row)):
        line = jnp.zeros((1, atoms), F32)
        for j in range(row * per_row, min(10, (row + 1) * per_row)):
            if j == 0:
                value = energy_row
            else:
                r, t = divmod(j - 1, 3)
                value = sums[8 * r + t : 8 * r + t + 1]
            line = line + jnp.where(lane_row == j - row * per_row, value, 0.0)
        packed.append(line)

    def store(index, carry):
        for m in range(3):
            out_ref[index, m] = jnp.zeros((1, atoms), F32)
        for j, line in enumerate(packed):
            out_ref[index, 3 + j] = line
        return carry

    lax.fori_loop(0, out_ref.shape[0], store, 0)
    for offset, value in forces.items():
        value = value[0:3] + value[4:7]
        index = device_of(offset)
        for m in range(3):
            out_ref[index, m] = out_ref[index, m] + value[m : m + 1, :]


def whole(memory_space=pltpu.VMEM):
    return pl.BlockSpec(memory_space=memory_space)


def shards(
    sizes,
    positions,
    species,
    cell_map,
    neighbours,
    struct_ids,
    embed,
    w_up,
    w_rad_in,
    w_rad_out,
    w_mix,
    read_first,
    read_hidden,
    read_last,
):
    devices = math.prod(sizes)
    atoms = positions.shape[1]
    neigh = neighbours.shape[0]
    width = w_up.shape[2]
    structs = SLAB_STRUCTS * sizes[0]
    elements = embed.shape[0]
    padded = -(-elements // LANES) * LANES
    edges = neigh * atoms
    params = pltpu.CompilerParams(vmem_limit_bytes=24 << 20)
    small = pltpu.CompilerParams(vmem_limit_bytes=8 << 20)
    sent = pl.pallas_call(
        pack_kernel,
        out_shape=jax.ShapeDtypeStruct((devices, HEAD_ROWS + neigh, 1, atoms), F32),
        in_specs=[whole()] * 5,
        out_specs=whole(),
        compiler_params=pltpu.CompilerParams(vmem_limit_bytes=60 << 20),
        name="pack",
    )(positions, species.reshape(1, -1), cell_map, neighbours, struct_ids.reshape(1, -1))
    got = lax.all_to_all(sent, AXES, 0, 0, tiled=True)
    radial_hidden, read_width, bessels = w_rad_in.shape[2], read_hidden.shape[1], w_rad_in.shape[1]
    shapes = [
        ((width, 2 * padded), BF16),
        ((width, 2 * padded), BF16),
        ((width, 3 * width), BF16),
        ((width, 3 * width), BF16),
        ((2, width, 9 * width), BF16),
        ((2, 3 * width, 3 * width), BF16),
        ((2, 2 * width, 3 * radial_hidden), BF16),
        ((2, 2 * radial_hidden, 2 * width), BF16),
        ((2, 3 * bessels, radial_hidden), BF16),
        ((2, bessels, 3 * radial_hidden), BF16),
        ((read_width, 3 * width), BF16),
        ((width, 3 * read_width), BF16),
        ((8, 3 * width + 3 * read_width), BF16),
        ((width + read_width, atoms), F32),
    ]
    weights = pl.pallas_call(
        functools.partial(prep_kernel, 1.0 / math.sqrt(neigh)),
        out_shape=[jax.ShapeDtypeStruct(*shape) for shape in shapes],
        in_specs=[whole()] * 8,
        out_specs=[whole()] * len(shapes),
        scratch_shapes=[pltpu.VMEM((padded, width), F32)],
        compiler_params=small,
        cost_estimate=pl.CostEstimate(flops=4_000_000_000, bytes_accessed=2_000_000, transcendentals=0),
        name="weights",
    )(
        embed,
        w_up,
        w_rad_in,
        w_rad_out,
        w_mix,
        read_first.reshape(1, -1),
        read_hidden,
        read_last.reshape(1, -1),
    )
    count = TAIL_ROWS - (-10 // (LANES // structs))
    parts = pl.pallas_call(
        functools.partial(main_kernel, sizes, structs),
        out_shape=jax.ShapeDtypeStruct((devices, count, 1, atoms), F32),
        in_specs=[whole()] * (1 + len(shapes)),
        out_specs=whole(),
        scratch_shapes=[
            pltpu.VMEM((5, 2 * width, edges), F32),
            pltpu.VMEM((5, width, edges), F32),
            pltpu.VMEM((4, 3 * neigh, 8, atoms), F32),
            pltpu.VMEM((2 * width, edges), BF16),
            pltpu.VMEM((2 * width, edges), BF16),
            pltpu.VMEM((4, atoms, edges), BF16),
            pltpu.VMEM((4 * atoms, edges), BF16),
            pltpu.VMEM((width, 4 * atoms), F32),
        ],
        compiler_params=params,
        name="forces",
    )(got, *weights)
    back = lax.all_to_all(parts, AXES, 0, 0, tiled=True)
    energies, virials, forces = pl.pallas_call(
        functools.partial(end_kernel, structs),
        out_shape=(
            jax.ShapeDtypeStruct((1, structs), F32),
            jax.ShapeDtypeStruct((9, structs), F32),
            jax.ShapeDtypeStruct((3, atoms), F32),
        ),
        in_specs=[whole()] * 2,
        out_specs=(whole(),) * 3,
        compiler_params=small,
        name="finish",
    )(back, cell_map)
    return energies.reshape(-1), virials, forces


def solution(mesh):
    sizes = tuple(mesh.shape[axis] for axis in AXES)
    return jax.shard_map(
        functools.partial(shards, sizes),
        mesh=mesh,
        in_specs=(
            P(None, AXES),
            P(AXES),
            P(AXES, None),
            P(None, AXES),
            P(AXES),
            P(),
            P(),
            P(),
            P(),
            P(),
            P(),
            P(),
            P(),
        ),
        out_specs=(P(), P(), P(None, AXES)),
        check_vma=False,
    )
```

```python
import functools
import math

import jax
import jax.numpy as jnp
from jax import lax
from jax.experimental import pallas as pl
from jax.experimental.pallas import tpu as pltpu
from jax.sharding import PartitionSpec as P

AXES = ("gx", "gy", "gz")
SLAB_STRUCTS = 4
LANES = 128
HEAD_ROWS = 5
TAIL_ROWS = 3

cutoff = 6.0
box_side = 4.5
soften = 0.25
amplitude = math.sqrt(2.0 / cutoff)

F32 = jnp.float32
BF16 = jnp.bfloat16
NN = (((1,), (0,)), ((), ()))
NT = (((1,), (1,)), ((), ()))
TN = (((0,), (0,)), ((), ()))


def dot(left, right, dims=NN):
    return lax.dot_general(left, right, dims, preferred_element_type=F32)


def split2(x):
    high = x.astype(BF16)
    return high, (x - high.astype(F32)).astype(BF16)


def split3(x):
    high = x.astype(BF16).astype(F32)
    rest = x - high
    middle = rest.astype(BF16).astype(F32)
    return high, middle, rest - middle


def left3(x):
    high, low = split2(x)
    return jnp.concatenate([high, high, low], axis=1)


def right3(x):
    high, low = split2(x)
    return jnp.concatenate([high, low, high], axis=0)


def iota(shape, axis):
    return lax.broadcasted_iota(jnp.int32, shape, axis)


def marks(count, row):
    labels = iota((count, row.shape[1]), 0).astype(F32).astype(BF16)
    return jnp.where(labels == row.astype(BF16), jnp.bfloat16(1), jnp.bfloat16(0))


def silu(x):
    sigma = 0.5 + 0.5 * jnp.tanh(0.5 * x)
    value = x * sigma
    return value, sigma + value * (1.0 - sigma)


def has_bit(lanes, group):
    per_cell = LANES // 8
    width = per_cell * 2 ** (3 - group)
    return (lanes & width) != 0


def pack_kernel(pos_ref, species_ref, cells_ref, nbr_ref, struct_ref, out_ref):
    atoms = pos_ref.shape[1]
    per_cell = atoms // 8
    place = (iota((atoms, atoms), 0) == cells_ref[...]).astype(F32).astype(BF16)
    lanes = iota((8, atoms), 1)
    inverse = dot(lanes.astype(F32).astype(BF16), place, NT)
    slots = nbr_ref[...]
    hits = jnp.concatenate(
        [(iota((atoms, atoms), 0) == slots[k : k + 1, :]).astype(F32).astype(BF16) for k in range(slots.shape[0])],
        axis=1,
    )
    found = dot(inverse.astype(BF16), hits)
    own = jnp.concatenate(
        [found[0:1, k * atoms : (k + 1) * atoms] for k in range(slots.shape[0])], axis=0
    )
    face_atoms = 4 * per_cell
    beyond = jnp.maximum(slots - atoms, 0)
    face = beyond // face_atoms
    spot = beyond - face * face_atoms
    upper = 1 - (face & 1)
    axis = face // 2
    along_x = upper * 4 * per_cell + spot
    along_y = (spot // (2 * per_cell)) * (4 * per_cell) + upper * 2 * per_cell + spot % (2 * per_cell)
    along_z = (spot // per_cell) * (2 * per_cell) + upper * per_cell + spot % per_cell
    cell = jnp.where(axis == 0, along_x, jnp.where(axis == 1, along_y, along_z))
    is_own = slots < atoms
    group = jnp.where(is_own, 0, axis + 1).astype(F32)
    cell = jnp.where(is_own, own, cell.astype(F32))
    parts = jnp.concatenate(
        [*split3(pos_ref[...]), species_ref[...].astype(F32), struct_ref[...].astype(F32)], axis=0
    )
    blank = jnp.zeros((16 - parts.shape[0], atoms), F32)
    moved = dot(jnp.concatenate([parts, blank, cell, group], axis=0).astype(BF16), place)
    chunk = jnp.concatenate(
        [
            moved[0:3] + moved[3:6] + moved[6:9],
            moved[9:11],
            moved[16 : 16 + slots.shape[0]] + float(atoms) * moved[16 + slots.shape[0] :],
        ],
        axis=0,
    )
    rows = [chunk[j : j + 1, :] for j in range(chunk.shape[0])]

    def store(device, carry):
        for j, row in enumerate(rows):
            out_ref[device, j] = row
        return carry

    lax.fori_loop(0, out_ref.shape[0], store, 0)


def end_kernel(structs, got_ref, cells_ref, energy_ref, virial_ref, force_ref):
    devices, count, _, atoms = got_ref.shape
    step = 8

    def add(index, totals):
        return tuple(total + got_ref[index * step + j] for j, total in enumerate(totals))

    totals = lax.fori_loop(
        0, devices // step, add, tuple(jnp.zeros((count, 1, atoms), F32) for _ in range(step))
    )
    while len(totals) > 1:
        totals = tuple(totals[i] + totals[i + 1] for i in range(0, len(totals), 2))
    lines = [totals[0][j] for j in range(count)]
    total = jnp.concatenate(lines[0:3] + [jnp.zeros((5, atoms), F32)], axis=0)
    place = (iota((atoms, atoms), 0) == cells_ref[...]).astype(F32).astype(BF16)
    parts = jnp.concatenate(split3(total), axis=0).astype(BF16)
    moved = dot(parts, place, NT)
    force_ref[...] = (moved[0:8] + moved[8:16] + moved[16:24])[0:3]
    per_row = LANES // structs
    for j in range(10):
        row, column = 3 + j // per_row, (j % per_row) * structs
        value = lines[row][:, column : column + structs]
        if j == 0:
            energy_ref[...] = value
        else:
            virial_ref[j - 1 : j, :] = value


def centre_offsets():
    units = [(1, 0, 0), (0, 1, 0), (0, 0, 1)]
    minus = [tuple(-v for v in unit) for unit in units]
    return units, minus


def plus(a, b):
    return tuple(x + y for x, y in zip(a, b))


def prep_kernel(
    scaling,
    embed_ref,
    up_ref,
    rad_in_ref,
    rad_out_ref,
    mix_ref,
    first_ref,
    hidden_ref,
    last_ref,
    embed_left_ref,
    lifted_left_ref,
    up_left_ref,
    up_back_ref,
    mix_left_ref,
    mix_back_ref,
    out_left_ref,
    in_left_ref,
    read_left_ref,
    read_back_ref,
    row_left_ref,
    column_ref,
    table_ref,
):
    elements = embed_ref.shape[0]
    width = up_ref.shape[2]
    table_ref[...] = jnp.zeros_like(table_ref)
    table_ref[0:elements, :] = embed_ref[...]
    embed_t = jnp.transpose(table_ref[...])
    embed_left_ref[...] = jnp.concatenate(split2(embed_t), axis=1)
    lifted_left_ref[...] = jnp.concatenate(
        split2(dot(left3(jnp.transpose(up_ref[0])), right3(embed_t))), axis=1
    )
    up_left_ref[...] = left3(jnp.transpose(up_ref[1]))
    up_back_ref[...] = left3(up_ref[1])
    for l in (0, 1):
        mix_left_ref[l] = left3(jnp.concatenate([jnp.transpose(mix_ref[l, j]) for j in range(3)], axis=1))
        mix_back_ref[l] = left3(mix_ref[l].reshape(3 * width, width))
        w_out = rad_out_ref[l] * scaling
        out_left_ref[l] = left3(jnp.transpose(w_out))
        w_in = rad_in_ref[l]
        high = w_in.astype(BF16).astype(F32)
        in_left_ref[l] = jnp.concatenate([high, high, w_in - high], axis=0).astype(BF16)
    read_left_ref[...] = left3(hidden_ref[...])
    read_back_ref[...] = left3(jnp.transpose(hidden_ref[...]))
    first_row = jnp.broadcast_to(first_ref[...], (8, width))
    last_row = jnp.broadcast_to(last_ref[...], (8, last_ref.shape[1]))
    row_left_ref[...] = jnp.concatenate([left3(first_row), left3(last_row)], axis=1)
    column_ref[0:width, :] = jnp.transpose(jnp.broadcast_to(first_ref[...], (LANES, width)))
    column_ref[width:, :] = jnp.transpose(jnp.broadcast_to(last_ref[...], (LANES, last_ref.shape[1])))


def main_kernel(
    sizes,
    structs,
    got_ref,
    embed_left_ref,
    lifted_left_ref,
    up_left_ref,
    up_back_ref,
    mix_left_ref,
    mix_back_ref,
    out_left_ref,
    in_left_ref,
    read_left_ref,
    read_back_ref,
    row_left_ref,
    column_ref,
    out_ref,
    radial_ref,
    picked_ref,
    spread_ref,
    change_ref,
    slots_ref,
    full_ref,
    feats_ref,
):
    atoms = LANES
    neigh = got_ref.shape[1] - HEAD_ROWS
    edges = neigh * atoms
    width = up_left_ref.shape[0]
    radial_hidden = in_left_ref.shape[2]
    padded = embed_left_ref.shape[1] // 2
    read_width = read_left_ref.shape[0]
    lanes8 = iota((8, atoms), 1)
    rows8 = iota((8, atoms), 0)
    units, minus = centre_offsets()
    home = (0, 0, 0)
    here = [lax.axis_index(axis) for axis in AXES]

    def device(offset):
        index = 0
        for place, step, size in zip(here, offset, sizes):
            index = index * size + lax.rem(place + step + 2 * size, size)
        return index

    names = {}

    def device_of(offset):
        if offset not in names:
            names[offset] = device(offset)
        return names[offset]

    def head(offset):
        index = device_of(offset)
        rows = [got_ref[index, j] for j in range(HEAD_ROWS)]
        return jnp.concatenate(rows + [jnp.zeros((8 - HEAD_ROWS, atoms), F32)], axis=0)

    heads = {}

    def head_of(offset):
        if offset not in heads:
            heads[offset] = head(offset)
        return heads[offset]

    def slots_of(offset):
        index = device_of(offset)
        rows = [got_ref[index, HEAD_ROWS + k] for k in range(neigh)]
        return jnp.concatenate(rows, axis=1)

    def table(centre):
        groups = [head_of(centre)]
        for q in (1, 2, 3):
            move = jnp.where(rows8 == q - 1, box_side, 0.0)
            groups.append(
                jnp.where(
                    has_bit(lanes8, q),
                    head_of(plus(centre, minus[q - 1])) - move,
                    head_of(plus(centre, units[q - 1])) + move,
                )
            )
        return [jnp.concatenate([groups[j][0:4], groups[j + 1][0:4]], axis=0) for j in (0, 2)]

    def per_edge(row):
        return jnp.concatenate([row] * neigh, axis=1)

    def fold(x):
        total = x[:, 0:atoms]
        for k in range(1, neigh):
            total = total + x[:, k * atoms : (k + 1) * atoms]
        return total

    tall = iota((8, edges), 0)
    order = (tall + 1).astype(F32)
    blocks = []
    for block in range(4):
        if block == 0:
            centres = [home]
            slots = slots_of(home)
            base = head_of(home)
        else:
            centres = [units[block - 1], minus[block - 1]]
            bit = has_bit(lanes8, block)
            slots = jnp.where(per_edge(bit[0:1]), slots_of(centres[1]), slots_of(centres[0]))
            base = jnp.where(bit, head_of(centres[1]), head_of(centres[0]))
        slots = slots.astype(jnp.int32)

        cell, group = slots & (atoms - 1), slots // atoms
        hits = marks(atoms, cell.astype(F32))
        slots_ref[block] = hits
        pairs = [pair for centre in centres for pair in table(centre)]
        stack = jnp.concatenate([part for parts in zip(*map(split3, pairs)) for part in parts], axis=0)
        found = dot(stack.astype(BF16), hits)
        combo = jnp.broadcast_to(group, (8, edges))
        if block:
            combo = combo + per_edge(jnp.where(bit, 4, 0))
        far = None
        size = 8 * len(pairs)
        for j in range(len(pairs)):
            part = found[8 * j : 8 * j + 8] + found[size + 8 * j : size + 8 * j + 8]
            part = part + found[2 * size + 8 * j : 2 * size + 8 * j + 8]
            far = part if far is None else jnp.where(combo >= 2 * j, part, far)
        far = jnp.where((combo & 1) == 1, jnp.concatenate([far[4:8], far[0:4]], axis=0), far)
        vec = jnp.where(tall < 3, far - per_edge(base), 0.0)
        square = jnp.sum(vec * vec, axis=0, keepdims=True) + soften
        square = jnp.broadcast_to(square, (8, edges))
        radius = jnp.sqrt(square)
        inverse = 1.0 / radius
        turn = order * (jnp.minimum(radius, cutoff) * (1.0 / cutoff))
        whole = jnp.floor(turn + 0.5)
        part = (turn - whole) * math.pi
        sign = 1.0 - 2.0 * (whole - 2.0 * jnp.floor(whole * 0.5))
        p2 = part * part
        sine = part * (
            1.0
            + p2 * (-1.0 / 6 + p2 * (1.0 / 120 + p2 * (-1.0 / 5040 + p2 * (1.0 / 362880 - p2 * (1.0 / 39916800)))))
        )
        cosine = 1.0 + p2 * (
            -0.5
            + p2 * (1.0 / 24 + p2 * (-1.0 / 720 + p2 * (1.0 / 40320 + p2 * (-1.0 / 3628800 + p2 * (1.0 / 479001600)))))
        )
        sine, cosine = sine * sign * amplitude, cosine * sign * amplitude
        inside = jnp.maximum(1.0 - square * (1.0 / (cutoff * cutoff)), 0.0)
        envelope = inside * inside
        over = sine * inverse
        bessel = over * envelope
        slope = (
            (order * (math.pi / cutoff) * cosine - over) * inverse * envelope
            - sine * inside * (4.0 / (cutoff * cutoff))
        )
        both = jnp.concatenate([bessel, slope], axis=1)
        high = both.astype(BF16).astype(F32)
        bessel_right = jnp.concatenate([high, both - high, high], axis=0).astype(BF16)
        direction = vec * inverse
        blocks.append(
            dict(
                base=base,
                combo=combo,
                far=far,
                vec=vec,
                inverse=inverse,
                bessel=bessel_right,
                direction=direction,
                struct=base[4:5, :],
            )
        )

    tile = 32

    def spread(block, m, k):
        row = blocks[block]["direction"][m : m + 1, k * atoms : (k + 1) * atoms]
        return jnp.broadcast_to(row, (8, atoms))

    for block in range(4):
        for m in range(3):
            for k in range(neigh):
                spread_ref[block, m * neigh + k] = spread(block, m, k)

    def wide(x):
        return jnp.concatenate([x] * (tile // 8), axis=0)

    def interact(layer, block, saved):
        pre = dot(in_left_ref[layer], blocks[block]["bessel"], TN)
        active, gain = silu(pre[:, 0:edges])
        active, change = right3(active), right3(gain * pre[:, edges:])
        radial_ref[saved] = dot(out_left_ref[layer], active)
        change_ref[saved] = dot(out_left_ref[layer], change)
        scalars = []
        vectors = [[], [], []]
        for start in range(0, width, tile):
            scalar = None
            vector = [None, None, None]
            for k in range(neigh):
                cut = pl.ds(k * atoms, atoms)
                rows = picked_ref[saved, pl.ds(start, tile), cut]
                zero = radial_ref[saved, pl.ds(start, tile), cut] * rows
                one = radial_ref[saved, pl.ds(width + start, tile), cut] * rows
                if layer == 0:
                    radial_ref[saved, pl.ds(width + start, tile), cut] = one
                scalar = zero if scalar is None else scalar + zero
                for m in range(3):
                    term = wide(spread_ref[block, m * neigh + k]) * one
                    vector[m] = term if vector[m] is None else vector[m] + term
            scalars.append(scalar)
            for m in range(3):
                vectors[m].append(vector[m])
        return jnp.concatenate(scalars, axis=0), [jnp.concatenate(v, axis=0) for v in vectors]

    def mix(layer, kept):
        scalar = jnp.concatenate([k[0] for k in kept], axis=1)
        square = jnp.concatenate([k[1][0] * k[1][0] + k[1][1] * k[1][1] + k[1][2] * k[1][2] for k in kept], axis=1)
        return dot(mix_left_ref[layer], right3(jnp.concatenate([scalar, square, scalar * scalar], axis=0)))

    def pull(layer, block, saved, kept, d, want_picked):
        scalar, vector = kept
        d_scalar = d[0:width] + 2.0 * scalar * d[2 * width : 3 * width]
        factor = 2.0 * d[width : 2 * width]
        d_vector = [v * factor for v in vector]
        toward = [[None] * neigh for _ in range(4)]
        for start in range(0, width, tile):
            part = slice(start, start + tile)
            for k in range(neigh):
                cut = pl.ds(k * atoms, atoms)
                rows = picked_ref[saved, pl.ds(start, tile), cut]
                one = radial_ref[saved, pl.ds(width + start, tile), cut]
                both = one if layer == 0 else one * rows
                through = None
                sums = []
                for m in range(3):
                    term = wide(spread_ref[block, m * neigh + k]) * d_vector[m][part]
                    through = term if through is None else through + term
                    sums.append(d_vector[m][part] * both)
                sums.append(
                    rows
                    * (
                        change_ref[saved, pl.ds(start, tile), cut] * d_scalar[part]
                        + change_ref[saved, pl.ds(width + start, tile), cut] * through
                    )
                )
                for m, push in enumerate(sums):
                    total = push[0:8]
                    for j in range(8, tile, 8):
                        total = total + push[j : j + 8]
                    toward[m][k] = total if toward[m][k] is None else toward[m][k] + total
                if want_picked:
                    picked_ref[saved, pl.ds(start, tile), cut] = (
                        radial_ref[saved, pl.ds(start, tile), cut] * d_scalar[part] + one * through
                    )
        own = blocks[block]
        lines = [
            jnp.concatenate([jnp.sum(toward[m][k], axis=0, keepdims=True) for k in range(neigh)], axis=1)
            for m in range(4)
        ]
        d_direction = jnp.concatenate(lines[0:3] + [jnp.zeros((5, edges), F32)], axis=0)
        inverse, direction = own["inverse"], own["direction"]
        radial_part = lines[3] - jnp.sum(d_direction * direction, axis=0, keepdims=True) * inverse
        return d_direction * inverse + radial_part * direction

    kept0 = []
    kinds = jnp.concatenate([blocks[block]["base"][3:4, :] for block in range(4)], axis=1)
    hits = marks(padded, kinds)
    initial = dot(embed_left_ref[...], jnp.concatenate([hits, hits], axis=0))
    for block in range(4):
        hits = marks(padded, blocks[block]["far"][3:4, :])
        picked_ref[block] = dot(lifted_left_ref[...], jnp.concatenate([hits, hits], axis=0))
        kept0.append(interact(0, block, block))
        if block % 2:
            cut = slice((block - 1) * atoms, (block + 1) * atoms)
            feats_ref[:, cut] = initial[:, cut] + mix(0, kept0[block - 1 : block + 1])

    own_group = blocks[0]["combo"][0:1, :].astype(F32).astype(BF16)
    hits = slots_ref[0]
    for q in range(4):
        full_ref[q * atoms : (q + 1) * atoms, :] = jnp.where(
            own_group == jnp.bfloat16(q), hits, jnp.bfloat16(0)
        )
    feats = feats_ref[...]
    lifted = dot(up_left_ref[...], right3(feats))
    high, low = split2(lifted)
    both = dot(jnp.concatenate([high, low], axis=0), full_ref[...])
    picked_ref[4] = both[0:width] + both[width:]
    kept1 = interact(1, 0, 4)
    mixed = mix(1, [kept1])
    layer_out = feats[:, 0:atoms]
    second = layer_out + mixed

    pre = dot(read_left_ref[...], right3(second))
    active, gain = silu(pre)
    atom_energy = dot(row_left_ref[:, 0 : 3 * width], right3(layer_out)) + dot(
        row_left_ref[:, 3 * width :], right3(active)
    )
    first_column = column_ref[0:width, :]
    d_second = dot(read_back_ref[...], right3(column_ref[width : width + read_width, :] * gain))

    edge_grad_one = pull(1, 0, 4, kept1, dot(mix_back_ref[1], right3(d_second)), True)
    high, low = split2(picked_ref[4])
    back = dot(jnp.concatenate([high, low], axis=0), full_ref[...], NT)
    d_feats = dot(up_back_ref[...], right3(back[0:width] + back[width:]))

    forces = {}
    cotangent = jnp.concatenate([d_feats[:, 0:atoms] + d_second + first_column, d_feats[:, atoms:]], axis=1)
    d_mixed = dot(mix_back_ref[0], right3(cotangent))

    def push(offset, value):
        forces[offset] = forces[offset] + value if offset in forces else value

    sums = None
    for block in range(4):
        grad = pull(0, block, block, kept0[block], d_mixed[:, block * atoms : (block + 1) * atoms], False)
        if block == 0:
            grad = grad + edge_grad_one
        own = blocks[block]
        centres = [home] if block == 0 else [units[block - 1], minus[block - 1]]
        pulled = fold(grad)
        if block == 0:
            push(home, pulled)
        else:
            bit = has_bit(lanes8, block)
            push(centres[1], jnp.where(bit, pulled, 0.0))
            push(centres[0], jnp.where(bit, 0.0, pulled))
        high = grad.astype(BF16).astype(F32)
        pair = jnp.concatenate([high[0:4], (grad - high)[0:4]], axis=0)
        stack = [jnp.where(own["combo"] == j, pair, 0.0) for j in range(4 * len(centres))]
        landed = dot(jnp.concatenate(stack, axis=0).astype(BF16), slots_ref[block], NT)
        for c, centre in enumerate(centres):
            for q in range(4):
                j = 4 * c + q
                value = -landed[8 * j : 8 * j + 8]
                if q == 0:
                    push(centre, value)
                else:
                    bit = has_bit(lanes8, q)
                    push(plus(centre, minus[q - 1]), jnp.where(bit, value, 0.0))
                    push(plus(centre, units[q - 1]), jnp.where(bit, 0.0, value))
        rows = []
        for r in range(3):
            rows.append(-fold(jnp.broadcast_to(own["vec"][r : r + 1, :], (8, edges)) * grad))
        if block == 0:
            rows.append(atom_energy)
        rows = jnp.concatenate(rows, axis=0)
        member = (own["struct"].astype(jnp.int32) == (iota((atoms, atoms), 0) & (structs - 1))).astype(F32)
        high, low = split2(rows)
        got = dot(jnp.concatenate([high, low], axis=0), member.astype(BF16), NT)
        got = got[0 : rows.shape[0]] + got[rows.shape[0] :]
        if block == 0:
            energy_row = got[24:25]
            sums = got[0:24]
        else:
            sums = sums + got

    per_row = LANES // structs
    lane_row = iota((1, atoms), 1) // structs
    packed = []
    for row in range(-(-10 // per_row)):
        line = jnp.zeros((1, atoms), F32)
        for j in range(row * per_row, min(10, (row + 1) * per_row)):
            if j == 0:
                value = energy_row
            else:
                r, t = divmod(j - 1, 3)
                value = sums[8 * r + t : 8 * r + t + 1]
            line = line + jnp.where(lane_row == j - row * per_row, value, 0.0)
        packed.append(line)

    def store(index, carry):
        for m in range(3):
            out_ref[index, m] = jnp.zeros((1, atoms), F32)
        for j, line in enumerate(packed):
            out_ref[index, 3 + j] = line
        return carry

    lax.fori_loop(0, out_ref.shape[0], store, 0)
    for offset, value in forces.items():
        value = value[0:3] + value[4:7]
        index = device_of(offset)
        for m in range(3):
            out_ref[index, m] = out_ref[index, m] + value[m : m + 1, :]


def whole(memory_space=pltpu.VMEM):
    return pl.BlockSpec(memory_space=memory_space)


def shards(
    sizes,
    positions,
    species,
    cell_map,
    neighbours,
    struct_ids,
    embed,
    w_up,
    w_rad_in,
    w_rad_out,
    w_mix,
    read_first,
    read_hidden,
    read_last,
):
    devices = math.prod(sizes)
    atoms = positions.shape[1]
    neigh = neighbours.shape[0]
    width = w_up.shape[2]
    structs = SLAB_STRUCTS * sizes[0]
    elements = embed.shape[0]
    padded = -(-elements // LANES) * LANES
    edges = neigh * atoms
    params = pltpu.CompilerParams(vmem_limit_bytes=32 << 20)
    small = pltpu.CompilerParams(vmem_limit_bytes=8 << 20)
    sent = pl.pallas_call(
        pack_kernel,
        out_shape=jax.ShapeDtypeStruct((devices, HEAD_ROWS + neigh, 1, atoms), F32),
        in_specs=[whole()] * 5,
        out_specs=whole(),
        compiler_params=pltpu.CompilerParams(vmem_limit_bytes=60 << 20),
        name="pack",
    )(positions, species.reshape(1, -1), cell_map, neighbours, struct_ids.reshape(1, -1))
    got = lax.all_to_all(sent, AXES, 0, 0, tiled=True)
    radial_hidden, read_width, bessels = w_rad_in.shape[2], read_hidden.shape[1], w_rad_in.shape[1]
    shapes = [
        ((width, 2 * padded), BF16),
        ((width, 2 * padded), BF16),
        ((width, 3 * width), BF16),
        ((width, 3 * width), BF16),
        ((2, width, 9 * width), BF16),
        ((2, 3 * width, 3 * width), BF16),
        ((2, 2 * width, 3 * radial_hidden), BF16),
        ((2, 3 * bessels, radial_hidden), BF16),
        ((read_width, 3 * width), BF16),
        ((width, 3 * read_width), BF16),
        ((8, 3 * width + 3 * read_width), BF16),
        ((width + read_width, atoms), F32),
    ]
    weights = pl.pallas_call(
        functools.partial(prep_kernel, 1.0 / math.sqrt(neigh)),
        out_shape=[jax.ShapeDtypeStruct(*shape) for shape in shapes],
        in_specs=[whole()] * 8,
        out_specs=[whole()] * len(shapes),
        scratch_shapes=[pltpu.VMEM((padded, width), F32)],
        compiler_params=small,
        cost_estimate=pl.CostEstimate(flops=4_000_000_000, bytes_accessed=2_000_000, transcendentals=0),
        name="weights",
    )(
        embed,
        w_up,
        w_rad_in,
        w_rad_out,
        w_mix,
        read_first.reshape(1, -1),
        read_hidden.T,
        read_last.reshape(1, -1),
    )
    count = TAIL_ROWS - (-10 // (LANES // structs))
    parts = pl.pallas_call(
        functools.partial(main_kernel, sizes, structs),
        out_shape=jax.ShapeDtypeStruct((devices, count, 1, atoms), F32),
        in_specs=[whole()] * (1 + len(shapes)),
        out_specs=whole(),
        scratch_shapes=[
            pltpu.VMEM((5, 2 * width, edges), F32),
            pltpu.VMEM((5, width, edges), F32),
            pltpu.VMEM((4, 3 * neigh, 8, atoms), F32),
            pltpu.VMEM((5, 2 * width, edges), F32),
            pltpu.VMEM((4, atoms, edges), BF16),
            pltpu.VMEM((4 * atoms, edges), BF16),
            pltpu.VMEM((width, 4 * atoms), F32),
        ],
        compiler_params=params,
        name="forces",
    )(got, *weights)
    back = lax.all_to_all(parts, AXES, 0, 0, tiled=True)
    energies, virials, forces = pl.pallas_call(
        functools.partial(end_kernel, structs),
        out_shape=(
            jax.ShapeDtypeStruct((1, structs), F32),
            jax.ShapeDtypeStruct((9, structs), F32),
            jax.ShapeDtypeStruct((3, atoms), F32),
        ),
        in_specs=[whole()] * 2,
        out_specs=(whole(),) * 3,
        compiler_params=small,
        name="finish",
    )(back, cell_map)
    return energies.reshape(-1), virials, forces


def solution(mesh):
    sizes = tuple(mesh.shape[axis] for axis in AXES)
    return jax.shard_map(
        functools.partial(shards, sizes),
        mesh=mesh,
        in_specs=(
            P(None, AXES),
            P(AXES),
            P(AXES, None),
            P(None, AXES),
            P(AXES),
            P(),
            P(),
            P(),
            P(),
            P(),
            P(),
            P(),
            P(),
        ),
        out_specs=(P(), P(), P(None, AXES)),
        check_vma=False,
    )
```

```python
import functools
import math

import jax
import jax.numpy as jnp
from jax import lax
from jax.experimental import pallas as pl
from jax.experimental.pallas import tpu as pltpu
from jax.sharding import PartitionSpec as P

AXES = ("gx", "gy", "gz")
SLAB_STRUCTS = 4
LANES = 128
HEAD_ROWS = 5
TAIL_ROWS = 3

cutoff = 6.0
box_side = 4.5
soften = 0.25
amplitude = math.sqrt(2.0 / cutoff)

F32 = jnp.float32
BF16 = jnp.bfloat16
NN = (((1,), (0,)), ((), ()))
NT = (((1,), (1,)), ((), ()))
TN = (((0,), (0,)), ((), ()))


def dot(left, right, dims=NN):
    return lax.dot_general(left, right, dims, preferred_element_type=F32)


def split2(x):
    high = x.astype(BF16)
    return high, (x - high.astype(F32)).astype(BF16)


def split3(x):
    high = x.astype(BF16).astype(F32)
    rest = x - high
    middle = rest.astype(BF16).astype(F32)
    return high, middle, rest - middle


def left3(x):
    high, low = split2(x)
    return jnp.concatenate([high, high, low], axis=1)


def right3(x):
    high, low = split2(x)
    return jnp.concatenate([high, low, high], axis=0)


def iota(shape, axis):
    return lax.broadcasted_iota(jnp.int32, shape, axis)


def marks(count, row):
    labels = iota((count, row.shape[1]), 0).astype(F32).astype(BF16)
    return jnp.where(labels == row.astype(BF16), jnp.bfloat16(1), jnp.bfloat16(0))


def silu(x):
    sigma = 0.5 + 0.5 * jnp.tanh(0.5 * x)
    value = x * sigma
    return value, sigma + value * (1.0 - sigma)


def has_bit(lanes, group):
    per_cell = LANES // 8
    width = per_cell * 2 ** (3 - group)
    return (lanes & width) != 0


def pack_kernel(pos_ref, species_ref, cells_ref, nbr_ref, struct_ref, out_ref):
    atoms = pos_ref.shape[1]
    per_cell = atoms // 8
    place = (iota((atoms, atoms), 0) == cells_ref[...]).astype(F32).astype(BF16)
    neigh = nbr_ref.shape[0]
    lanes = iota((8, atoms), 1)
    inverse = dot(lanes.astype(F32).astype(BF16), place, NT)
    high = nbr_ref[...] // atoms
    parts = jnp.concatenate(
        [*split3(pos_ref[...]), species_ref[...].astype(F32), struct_ref[...].astype(F32)], axis=0
    )
    blank = jnp.zeros((16 - parts.shape[0], atoms), F32)
    low = (nbr_ref[...] - high * atoms).astype(F32)
    moved = dot(jnp.concatenate([parts, blank, low, high.astype(F32)], axis=0).astype(BF16), place)
    low, high = moved[16 : 16 + neigh], moved[16 + neigh :]
    slots = (low + float(atoms) * high).astype(jnp.int32)
    hits = jnp.concatenate([marks(atoms, low[k : k + 1, :]) for k in range(neigh)], axis=1)
    found = dot(inverse.astype(BF16), hits)
    own = jnp.concatenate([found[0:1, k * atoms : (k + 1) * atoms] for k in range(neigh)], axis=0)
    face_atoms = 4 * per_cell
    beyond = jnp.maximum(slots - atoms, 0)
    face = beyond // face_atoms
    spot = beyond - face * face_atoms
    upper = 1 - (face & 1)
    axis = face // 2
    along_x = upper * 4 * per_cell + spot
    along_y = (spot // (2 * per_cell)) * (4 * per_cell) + upper * 2 * per_cell + spot % (2 * per_cell)
    along_z = (spot // per_cell) * (2 * per_cell) + upper * per_cell + spot % per_cell
    cell = jnp.where(axis == 0, along_x, jnp.where(axis == 1, along_y, along_z))
    is_own = slots < atoms
    group = jnp.where(is_own, 0, axis + 1).astype(F32)
    cell = jnp.where(is_own, own, cell.astype(F32))
    rows = [moved[j : j + 1] + moved[j + 3 : j + 4] + moved[j + 6 : j + 7] for j in range(3)]
    rows += [moved[9:10], moved[10:11]]
    slots = cell + float(atoms) * group
    rows += [slots[k : k + 1] for k in range(neigh)]

    def store(device, carry):
        for j, row in enumerate(rows):
            out_ref[device, j] = row
        return carry

    lax.fori_loop(0, out_ref.shape[0], store, 0)


def end_kernel(structs, got_ref, cells_ref, energy_ref, virial_ref, force_ref):
    devices, count, _, atoms = got_ref.shape
    step = 8

    def add(index, totals):
        return tuple(total + got_ref[index * step + j] for j, total in enumerate(totals))

    totals = lax.fori_loop(
        0, devices // step, add, tuple(jnp.zeros((count, 1, atoms), F32) for _ in range(step))
    )
    while len(totals) > 1:
        totals = tuple(totals[i] + totals[i + 1] for i in range(0, len(totals), 2))
    lines = [totals[0][j] for j in range(count)]
    total = jnp.concatenate(lines[0:3] + [jnp.zeros((5, atoms), F32)], axis=0)
    place = (iota((atoms, atoms), 0) == cells_ref[...]).astype(F32).astype(BF16)
    parts = jnp.concatenate(split3(total), axis=0).astype(BF16)
    moved = dot(parts, place, NT)
    force_ref[...] = (moved[0:8] + moved[8:16] + moved[16:24])[0:3]
    per_row = LANES // structs
    for j in range(10):
        row, column = 3 + j // per_row, (j % per_row) * structs
        value = lines[row][:, column : column + structs]
        if j == 0:
            energy_ref[...] = value
        else:
            virial_ref[j - 1 : j, :] = value


def centre_offsets():
    units = [(1, 0, 0), (0, 1, 0), (0, 0, 1)]
    minus = [tuple(-v for v in unit) for unit in units]
    return units, minus


def plus(a, b):
    return tuple(x + y for x, y in zip(a, b))


def prep_kernel(
    scaling,
    embed_ref,
    up_ref,
    rad_in_ref,
    rad_out_ref,
    mix_ref,
    first_ref,
    hidden_ref,
    last_ref,
    embed_left_ref,
    lifted_left_ref,
    up_left_ref,
    up_back_ref,
    mix_left_ref,
    mix_back_ref,
    out_left_ref,
    in_left_ref,
    read_left_ref,
    read_back_ref,
    row_left_ref,
    column_ref,
    table_ref,
):
    elements = embed_ref.shape[0]
    width = up_ref.shape[2]
    table_ref[...] = jnp.zeros_like(table_ref)
    table_ref[0:elements, :] = embed_ref[...]
    embed_t = jnp.transpose(table_ref[...])
    embed_left_ref[...] = jnp.concatenate(split2(embed_t), axis=1)
    lifted_left_ref[...] = jnp.concatenate(
        split2(dot(left3(jnp.transpose(up_ref[0])), right3(embed_t))), axis=1
    )
    up_left_ref[...] = left3(jnp.transpose(up_ref[1]))
    up_back_ref[...] = left3(up_ref[1])
    for l in (0, 1):
        mix_left_ref[l] = left3(jnp.concatenate([jnp.transpose(mix_ref[l, j]) for j in range(3)], axis=1))
        mix_back_ref[l] = left3(mix_ref[l].reshape(3 * width, width))
        w_out = rad_out_ref[l] * scaling
        out_left_ref[l] = left3(jnp.transpose(w_out))
        w_in = rad_in_ref[l]
        high = w_in.astype(BF16).astype(F32)
        in_left_ref[l] = jnp.concatenate([high, high, w_in - high], axis=0).astype(BF16)
    read_left_ref[...] = left3(hidden_ref[...])
    read_back_ref[...] = left3(jnp.transpose(hidden_ref[...]))
    first_row = jnp.broadcast_to(first_ref[...], (8, width))
    last_row = jnp.broadcast_to(last_ref[...], (8, last_ref.shape[1]))
    row_left_ref[...] = jnp.concatenate([left3(first_row), left3(last_row)], axis=1)
    column_ref[0:width, :] = jnp.transpose(jnp.broadcast_to(first_ref[...], (LANES, width)))
    column_ref[width:, :] = jnp.transpose(jnp.broadcast_to(last_ref[...], (LANES, last_ref.shape[1])))


def main_kernel(
    sizes,
    structs,
    got_ref,
    embed_left_ref,
    lifted_left_ref,
    up_left_ref,
    up_back_ref,
    mix_left_ref,
    mix_back_ref,
    out_left_ref,
    in_left_ref,
    read_left_ref,
    read_back_ref,
    row_left_ref,
    column_ref,
    out_ref,
    radial_ref,
    picked_ref,
    spread_ref,
    change_ref,
    turned_ref,
    slots_ref,
    full_ref,
    feats_ref,
):
    atoms = LANES
    neigh = got_ref.shape[1] - HEAD_ROWS
    edges = neigh * atoms
    width = up_left_ref.shape[0]
    radial_hidden = in_left_ref.shape[2]
    padded = embed_left_ref.shape[1] // 2
    read_width = read_left_ref.shape[0]
    lanes8 = iota((8, atoms), 1)
    rows8 = iota((8, atoms), 0)
    units, minus = centre_offsets()
    home = (0, 0, 0)
    here = [lax.axis_index(axis) for axis in AXES]

    def device(offset):
        index = 0
        for place, step, size in zip(here, offset, sizes):
            index = index * size + lax.rem(place + step + 2 * size, size)
        return index

    names = {}

    def device_of(offset):
        if offset not in names:
            names[offset] = device(offset)
        return names[offset]

    def head(offset):
        index = device_of(offset)
        rows = [got_ref[index, j] for j in range(HEAD_ROWS)]
        return jnp.concatenate(rows + [jnp.zeros((8 - HEAD_ROWS, atoms), F32)], axis=0)

    heads = {}

    def head_of(offset):
        if offset not in heads:
            heads[offset] = head(offset)
        return heads[offset]

    def slots_of(offset):
        index = device_of(offset)
        rows = [got_ref[index, HEAD_ROWS + k] for k in range(neigh)]
        return jnp.concatenate(rows, axis=1)

    def table(centre):
        groups = [head_of(centre)]
        for q in (1, 2, 3):
            move = jnp.where(rows8 == q - 1, box_side, 0.0)
            groups.append(
                jnp.where(
                    has_bit(lanes8, q),
                    head_of(plus(centre, minus[q - 1])) - move,
                    head_of(plus(centre, units[q - 1])) + move,
                )
            )
        return [jnp.concatenate([groups[j][0:4], groups[j + 1][0:4]], axis=0) for j in (0, 2)]

    def per_edge(row):
        return jnp.concatenate([row] * neigh, axis=1)

    def fold(x):
        total = x[:, 0:atoms]
        for k in range(1, neigh):
            total = total + x[:, k * atoms : (k + 1) * atoms]
        return total

    tall = iota((8, edges), 0)
    order = (tall + 1).astype(F32)
    blocks = []
    for block in range(4):
        if block == 0:
            centres = [home]
            slots = slots_of(home)
            base = head_of(home)
        else:
            centres = [units[block - 1], minus[block - 1]]
            bit = has_bit(lanes8, block)
            slots = jnp.where(per_edge(bit[0:1]), slots_of(centres[1]), slots_of(centres[0]))
            base = jnp.where(bit, head_of(centres[1]), head_of(centres[0]))
        slots = slots.astype(jnp.int32)

        cell, group = slots & (atoms - 1), slots // atoms
        hits = marks(atoms, cell.astype(F32))
        slots_ref[block] = hits
        pairs = [pair for centre in centres for pair in table(centre)]
        stack = jnp.concatenate([part for parts in zip(*map(split3, pairs)) for part in parts], axis=0)
        found = dot(stack.astype(BF16), hits)
        combo = jnp.broadcast_to(group, (8, edges))
        if block:
            combo = combo + per_edge(jnp.where(bit, 4, 0))
        far = None
        size = 8 * len(pairs)
        for j in range(len(pairs)):
            part = found[8 * j : 8 * j + 8] + found[size + 8 * j : size + 8 * j + 8]
            part = part + found[2 * size + 8 * j : 2 * size + 8 * j + 8]
            far = part if far is None else jnp.where(combo >= 2 * j, part, far)
        far = jnp.where((combo & 1) == 1, jnp.concatenate([far[4:8], far[0:4]], axis=0), far)
        vec = jnp.where(tall < 3, far - per_edge(base), 0.0)
        square = jnp.sum(vec * vec, axis=0, keepdims=True) + soften
        square = jnp.broadcast_to(square, (8, edges))
        radius = jnp.sqrt(square)
        inverse = 1.0 / radius
        turn = order * (jnp.minimum(radius, cutoff) * (1.0 / cutoff))
        whole = jnp.floor(turn + 0.5)
        part = (turn - whole) * math.pi
        sign = 1.0 - 2.0 * (whole - 2.0 * jnp.floor(whole * 0.5))
        p2 = part * part
        sine = part * (
            1.0
            + p2 * (-1.0 / 6 + p2 * (1.0 / 120 + p2 * (-1.0 / 5040 + p2 * (1.0 / 362880 - p2 * (1.0 / 39916800)))))
        )
        cosine = 1.0 + p2 * (
            -0.5
            + p2 * (1.0 / 24 + p2 * (-1.0 / 720 + p2 * (1.0 / 40320 + p2 * (-1.0 / 3628800 + p2 * (1.0 / 479001600)))))
        )
        sine, cosine = sine * sign * amplitude, cosine * sign * amplitude
        inside = jnp.maximum(1.0 - square * (1.0 / (cutoff * cutoff)), 0.0)
        envelope = inside * inside
        over = sine * inverse
        bessel = over * envelope
        slope = (
            (order * (math.pi / cutoff) * cosine - over) * inverse * envelope
            - sine * inside * (4.0 / (cutoff * cutoff))
        )
        both = jnp.concatenate([bessel, slope], axis=1)
        high = both.astype(BF16).astype(F32)
        bessel_right = jnp.concatenate([high, both - high, high], axis=0).astype(BF16)
        direction = vec * inverse
        blocks.append(
            dict(
                base=base,
                combo=combo,
                far=far,
                vec=vec,
                inverse=inverse,
                bessel=bessel_right,
                direction=direction,
                struct=base[4:5, :],
            )
        )

    tile = 32

    def spread(block, m, k):
        row = blocks[block]["direction"][m : m + 1, k * atoms : (k + 1) * atoms]
        return jnp.broadcast_to(row, (8, atoms))

    for block in range(4):
        for m in range(3):
            for k in range(neigh):
                spread_ref[block, m * neigh + k] = spread(block, m, k)

    def wide(x):
        return jnp.concatenate([x] * (tile // 8), axis=0)

    def radial(layer, block, saved):
        pre = dot(in_left_ref[layer], blocks[block]["bessel"], TN)
        active, gain = silu(pre[:, 0:edges])
        radial_ref[saved] = dot(out_left_ref[layer], right3(active))
        turned_ref[saved] = right3(gain * pre[:, edges:])

    def change(layer, saved):
        change_ref[saved] = dot(out_left_ref[layer], turned_ref[saved])

    def interact(layer, block, saved):
        scalars = []
        vectors = [[], [], []]
        for start in range(0, width, tile):
            scalar = None
            vector = [None, None, None]
            for k in range(neigh):
                cut = pl.ds(k * atoms, atoms)
                rows = picked_ref[saved, pl.ds(start, tile), cut]
                zero = radial_ref[saved, pl.ds(start, tile), cut] * rows
                one = radial_ref[saved, pl.ds(width + start, tile), cut] * rows
                if layer == 0:
                    radial_ref[saved, pl.ds(width + start, tile), cut] = one
                scalar = zero if scalar is None else scalar + zero
                for m in range(3):
                    term = wide(spread_ref[block, m * neigh + k]) * one
                    vector[m] = term if vector[m] is None else vector[m] + term
            scalars.append(scalar)
            for m in range(3):
                vectors[m].append(vector[m])
        return jnp.concatenate(scalars, axis=0), [jnp.concatenate(v, axis=0) for v in vectors]

    def mix(layer, kept):
        scalar = jnp.concatenate([k[0] for k in kept], axis=1)
        square = jnp.concatenate([k[1][0] * k[1][0] + k[1][1] * k[1][1] + k[1][2] * k[1][2] for k in kept], axis=1)
        return dot(mix_left_ref[layer], right3(jnp.concatenate([scalar, square, scalar * scalar], axis=0)))

    def add_up(value, total):
        part = value[0:8]
        for j in range(8, tile, 8):
            part = part + value[j : j + 8]
        return part if total is None else total + part

    odd, upper = (rows8 & 1) == 1, (rows8 & 2) == 2

    def gather_rows(values):
        a, b, c, d = values
        low = jnp.where(odd, b, a) + pltpu.roll(jnp.where(odd, a, b), 7, 0)
        high = jnp.where(odd, d, c) + pltpu.roll(jnp.where(odd, c, d), 7, 0)
        both = jnp.where(upper, high, low) + pltpu.roll(jnp.where(upper, low, high), 6, 0)
        return both + pltpu.roll(both, 4, 0)

    def pull(layer, block, saved, kept, d):
        scalar, vector = kept
        d_scalar = d[0:width] + 2.0 * scalar * d[2 * width : 3 * width]
        factor = 2.0 * d[width : 2 * width]
        toward = [[None] * neigh for _ in range(4)]
        d_vector = [v * factor for v in vector]
        for start in range(0, width, tile):
            part = slice(start, start + tile)
            for k in range(neigh):
                cut = pl.ds(k * atoms, atoms)
                rows = picked_ref[saved, pl.ds(start, tile), cut]
                one = radial_ref[saved, pl.ds(width + start, tile), cut]
                both = one * rows if layer else one
                through = None
                for m in range(3):
                    term = wide(spread_ref[block, m * neigh + k]) * d_vector[m][part]
                    through = term if through is None else through + term
                    toward[m][k] = add_up(d_vector[m][part] * both, toward[m][k])
                turned = rows * (
                    change_ref[saved, pl.ds(start, tile), cut] * d_scalar[part]
                    + change_ref[saved, pl.ds(width + start, tile), cut] * through
                )
                toward[3][k] = add_up(turned, toward[3][k])
                if layer:
                    picked_ref[saved, pl.ds(start, tile), cut] = (
                        radial_ref[saved, pl.ds(start, tile), cut] * d_scalar[part] + one * through
                    )
        own = blocks[block]
        lines = jnp.concatenate([gather_rows([toward[m][k] for m in range(4)]) for k in range(neigh)], axis=1)
        d_direction = jnp.where(tall < 3, lines, 0.0)
        inverse, direction = own["inverse"], own["direction"]
        radial_part = lines[3:4] - jnp.sum(d_direction * direction, axis=0, keepdims=True) * inverse
        return d_direction * inverse + radial_part * direction

    kept0 = []
    kinds = jnp.concatenate([blocks[block]["base"][3:4, :] for block in range(4)], axis=1)
    hits = marks(padded, kinds)
    initial = dot(embed_left_ref[...], jnp.concatenate([hits, hits], axis=0))

    def ready(block):
        hits = marks(padded, blocks[block]["far"][3:4, :])
        picked_ref[block] = dot(lifted_left_ref[...], jnp.concatenate([hits, hits], axis=0))
        radial(0, block, block)

    ready(0)
    for block in range(4):
        if block < 3:
            ready(block + 1)
        else:
            radial(1, 0, 4)
        kept0.append(interact(0, block, block))
        if block % 2:
            cut = slice((block - 1) * atoms, (block + 1) * atoms)
            feats_ref[:, cut] = initial[:, cut] + mix(0, kept0[block - 1 : block + 1])

    own_group = blocks[0]["combo"][0:1, :].astype(F32).astype(BF16)
    hits = slots_ref[0]
    for q in range(4):
        full_ref[q * atoms : (q + 1) * atoms, :] = jnp.where(
            own_group == jnp.bfloat16(q), hits, jnp.bfloat16(0)
        )
    feats = feats_ref[...]
    lifted = dot(up_left_ref[...], right3(feats))
    high, low = split2(lifted)
    both = dot(jnp.concatenate([high, low], axis=0), full_ref[...])
    picked_ref[4] = both[0:width] + both[width:]
    change(1, 4)
    kept1 = interact(1, 0, 4)
    mixed = mix(1, [kept1])
    layer_out = feats[:, 0:atoms]
    second = layer_out + mixed

    pre = dot(read_left_ref[...], right3(second))
    active, gain = silu(pre)
    atom_energy = dot(row_left_ref[:, 0 : 3 * width], right3(layer_out)) + dot(
        row_left_ref[:, 3 * width :], right3(active)
    )
    first_column = column_ref[0:width, :]
    d_second = dot(read_back_ref[...], right3(column_ref[width : width + read_width, :] * gain))

    d_mixed = dot(mix_back_ref[1], right3(d_second))
    change(0, 0)
    edge_grad_one = pull(1, 0, 4, kept1, d_mixed)
    high, low = split2(picked_ref[4])
    back = dot(jnp.concatenate([high, low], axis=0), full_ref[...], NT)
    d_feats = dot(up_back_ref[...], right3(back[0:width] + back[width:]))

    forces = {}
    cotangent = jnp.concatenate([d_feats[:, 0:atoms] + d_second + first_column, d_feats[:, atoms:]], axis=1)
    d_mixed = dot(mix_back_ref[0], right3(cotangent))

    def push(offset, value):
        forces[offset] = forces[offset] + value if offset in forces else value

    sums = None
    for block in range(4):
        if block < 3:
            change(0, block + 1)
        grad = pull(0, block, block, kept0[block], d_mixed[:, block * atoms : (block + 1) * atoms])
        if block == 0:
            grad = grad + edge_grad_one
        own = blocks[block]
        centres = [home] if block == 0 else [units[block - 1], minus[block - 1]]
        pulled = fold(grad)
        if block == 0:
            push(home, pulled)
        else:
            bit = has_bit(lanes8, block)
            push(centres[1], jnp.where(bit, pulled, 0.0))
            push(centres[0], jnp.where(bit, 0.0, pulled))
        high = grad.astype(BF16).astype(F32)
        pair = jnp.concatenate([high[0:4], (grad - high)[0:4]], axis=0)
        stack = [jnp.where(own["combo"] == j, pair, 0.0) for j in range(4 * len(centres))]
        landed = dot(jnp.concatenate(stack, axis=0).astype(BF16), slots_ref[block], NT)
        for c, centre in enumerate(centres):
            for q in range(4):
                j = 4 * c + q
                value = -landed[8 * j : 8 * j + 8]
                if q == 0:
                    push(centre, value)
                else:
                    bit = has_bit(lanes8, q)
                    push(plus(centre, minus[q - 1]), jnp.where(bit, value, 0.0))
                    push(plus(centre, units[q - 1]), jnp.where(bit, 0.0, value))
        rows = []
        for r in range(3):
            rows.append(-fold(jnp.broadcast_to(own["vec"][r : r + 1, :], (8, edges)) * grad))
        if block == 0:
            rows.append(atom_energy)
        rows = jnp.concatenate(rows, axis=0)
        member = (own["struct"].astype(jnp.int32) == (iota((atoms, atoms), 0) & (structs - 1))).astype(F32)
        high, low = split2(rows)
        got = dot(jnp.concatenate([high, low], axis=0), member.astype(BF16), NT)
        got = got[0 : rows.shape[0]] + got[rows.shape[0] :]
        if block == 0:
            energy_row = got[24:25]
            sums = got[0:24]
        else:
            sums = sums + got

    per_row = LANES // structs
    lane_row = iota((1, atoms), 1) // structs
    packed = []
    for row in range(-(-10 // per_row)):
        line = jnp.zeros((1, atoms), F32)
        for j in range(row * per_row, min(10, (row + 1) * per_row)):
            if j == 0:
                value = energy_row
            else:
                r, t = divmod(j - 1, 3)
                value = sums[8 * r + t : 8 * r + t + 1]
            line = line + jnp.where(lane_row == j - row * per_row, value, 0.0)
        packed.append(line)

    def store(index, carry):
        for m in range(3):
            out_ref[index, m] = jnp.zeros((1, atoms), F32)
        for j, line in enumerate(packed):
            out_ref[index, 3 + j] = line
        return carry

    lax.fori_loop(0, out_ref.shape[0], store, 0)
    for offset, value in forces.items():
        value = value[0:3] + value[4:7]
        index = device_of(offset)
        for m in range(3):
            out_ref[index, m] = out_ref[index, m] + value[m : m + 1, :]


def whole(memory_space=pltpu.VMEM):
    return pl.BlockSpec(memory_space=memory_space)


def shards(
    sizes,
    positions,
    species,
    cell_map,
    neighbours,
    struct_ids,
    embed,
    w_up,
    w_rad_in,
    w_rad_out,
    w_mix,
    read_first,
    read_hidden,
    read_last,
):
    devices = math.prod(sizes)
    atoms = positions.shape[1]
    neigh = neighbours.shape[0]
    width = w_up.shape[2]
    structs = SLAB_STRUCTS * sizes[0]
    elements = embed.shape[0]
    padded = -(-elements // LANES) * LANES
    edges = neigh * atoms
    params = pltpu.CompilerParams(vmem_limit_bytes=32 << 20)
    small = pltpu.CompilerParams(vmem_limit_bytes=8 << 20)
    sent = pl.pallas_call(
        pack_kernel,
        out_shape=jax.ShapeDtypeStruct((devices, HEAD_ROWS + neigh, 1, atoms), F32),
        in_specs=[whole()] * 5,
        out_specs=whole(),
        compiler_params=pltpu.CompilerParams(vmem_limit_bytes=60 << 20),
        name="pack",
    )(positions, species.reshape(1, -1), cell_map, neighbours, struct_ids.reshape(1, -1))
    got = lax.all_to_all(sent, AXES, 0, 0, tiled=True)
    radial_hidden, read_width, bessels = w_rad_in.shape[2], read_hidden.shape[1], w_rad_in.shape[1]
    shapes = [
        ((width, 2 * padded), BF16),
        ((width, 2 * padded), BF16),
        ((width, 3 * width), BF16),
        ((width, 3 * width), BF16),
        ((2, width, 9 * width), BF16),
        ((2, 3 * width, 3 * width), BF16),
        ((2, 2 * width, 3 * radial_hidden), BF16),
        ((2, 3 * bessels, radial_hidden), BF16),
        ((read_width, 3 * width), BF16),
        ((width, 3 * read_width), BF16),
        ((8, 3 * width + 3 * read_width), BF16),
        ((width + read_width, atoms), F32),
    ]
    weights = pl.pallas_call(
        functools.partial(prep_kernel, 1.0 / math.sqrt(neigh)),
        out_shape=[jax.ShapeDtypeStruct(*shape) for shape in shapes],
        in_specs=[whole()] * 8,
        out_specs=[whole()] * len(shapes),
        scratch_shapes=[pltpu.VMEM((padded, width), F32)],
        compiler_params=small,
        cost_estimate=pl.CostEstimate(flops=4_000_000_000, bytes_accessed=2_000_000, transcendentals=0),
        name="weights",
    )(
        embed,
        w_up,
        w_rad_in,
        w_rad_out,
        w_mix,
        read_first.reshape(1, -1),
        read_hidden.T,
        read_last.reshape(1, -1),
    )
    count = TAIL_ROWS - (-10 // (LANES // structs))
    parts = pl.pallas_call(
        functools.partial(main_kernel, sizes, structs),
        out_shape=jax.ShapeDtypeStruct((devices, count, 1, atoms), F32),
        in_specs=[whole()] * (1 + len(shapes)),
        out_specs=whole(),
        scratch_shapes=[
            pltpu.VMEM((5, 2 * width, edges), F32),
            pltpu.VMEM((5, width, edges), F32),
            pltpu.VMEM((4, 3 * neigh, 8, atoms), F32),
            pltpu.VMEM((5, 2 * width, edges), F32),
            pltpu.VMEM((5, 3 * radial_hidden, edges), BF16),
            pltpu.VMEM((4, atoms, edges), BF16),
            pltpu.VMEM((4 * atoms, edges), BF16),
            pltpu.VMEM((width, 4 * atoms), F32),
        ],
        compiler_params=params,
        name="forces",
    )(got, *weights)
    back = lax.all_to_all(parts, AXES, 0, 0, tiled=True)
    energies, virials, forces = pl.pallas_call(
        functools.partial(end_kernel, structs),
        out_shape=(
            jax.ShapeDtypeStruct((1, structs), F32),
            jax.ShapeDtypeStruct((9, structs), F32),
            jax.ShapeDtypeStruct((3, atoms), F32),
        ),
        in_specs=[whole()] * 2,
        out_specs=(whole(),) * 3,
        compiler_params=small,
        name="finish",
    )(back, cell_map)
    return energies.reshape(-1), virials, forces


def solution(mesh):
    sizes = tuple(mesh.shape[axis] for axis in AXES)
    return jax.shard_map(
        functools.partial(shards, sizes),
        mesh=mesh,
        in_specs=(
            P(None, AXES),
            P(AXES),
            P(AXES, None),
            P(None, AXES),
            P(AXES),
            P(),
            P(),
            P(),
            P(),
            P(),
            P(),
            P(),
            P(),
        ),
        out_specs=(P(), P(), P(None, AXES)),
        check_vma=False,
    )
```

```python
import functools
import math

import jax
import jax.numpy as jnp
from jax import lax
from jax.experimental import pallas as pl
from jax.experimental.pallas import tpu as pltpu
from jax.sharding import PartitionSpec as P

AXES = ("gx", "gy", "gz")
SLAB_STRUCTS = 4
LANES = 128
HEAD_ROWS = 5
TAIL_ROWS = 3

cutoff = 6.0
box_side = 4.5
soften = 0.25
amplitude = math.sqrt(2.0 / cutoff)

F32 = jnp.float32
BF16 = jnp.bfloat16
NN = (((1,), (0,)), ((), ()))
NT = (((1,), (1,)), ((), ()))
TN = (((0,), (0,)), ((), ()))


def dot(left, right, dims=NN):
    return lax.dot_general(left, right, dims, preferred_element_type=F32)


def split2(x):
    high = x.astype(BF16)
    return high, (x - high.astype(F32)).astype(BF16)


def split3(x):
    high = x.astype(BF16).astype(F32)
    rest = x - high
    middle = rest.astype(BF16).astype(F32)
    return high, middle, rest - middle


def left3(x):
    high, low = split2(x)
    return jnp.concatenate([high, high, low], axis=1)


def right3(x):
    high, low = split2(x)
    return jnp.concatenate([high, low, high], axis=0)


def iota(shape, axis):
    return lax.broadcasted_iota(jnp.int32, shape, axis)


def marks(count, row):
    labels = iota((count, row.shape[1]), 0).astype(F32).astype(BF16)
    return jnp.where(labels == row.astype(BF16), jnp.bfloat16(1), jnp.bfloat16(0))


def silu(x):
    sigma = 0.5 + 0.5 * jnp.tanh(0.5 * x)
    value = x * sigma
    return value, sigma + value * (1.0 - sigma)


def has_bit(lanes, group):
    per_cell = LANES // 8
    width = per_cell * 2 ** (3 - group)
    return (lanes & width) != 0


def pack_kernel(pos_ref, species_ref, cells_ref, nbr_ref, struct_ref, out_ref):
    atoms = pos_ref.shape[1]
    per_cell = atoms // 8
    place = (iota((atoms, atoms), 0) == cells_ref[...]).astype(F32).astype(BF16)
    neigh = nbr_ref.shape[0]
    lanes = iota((8, atoms), 1)
    inverse = dot(lanes.astype(F32).astype(BF16), place, NT)
    high = nbr_ref[...] // atoms
    parts = jnp.concatenate(
        [*split3(pos_ref[...]), species_ref[...].astype(F32), struct_ref[...].astype(F32)], axis=0
    )
    blank = jnp.zeros((16 - parts.shape[0], atoms), F32)
    low = (nbr_ref[...] - high * atoms).astype(F32)
    moved = dot(jnp.concatenate([parts, blank, low, high.astype(F32)], axis=0).astype(BF16), place)
    low, high = moved[16 : 16 + neigh], moved[16 + neigh :]
    slots = (low + float(atoms) * high).astype(jnp.int32)
    hits = jnp.concatenate([marks(atoms, low[k : k + 1, :]) for k in range(neigh)], axis=1)
    found = dot(inverse.astype(BF16), hits)
    own = jnp.concatenate([found[0:1, k * atoms : (k + 1) * atoms] for k in range(neigh)], axis=0)
    face_atoms = 4 * per_cell
    beyond = jnp.maximum(slots - atoms, 0)
    face = beyond // face_atoms
    spot = beyond - face * face_atoms
    upper = 1 - (face & 1)
    axis = face // 2
    along_x = upper * 4 * per_cell + spot
    along_y = (spot // (2 * per_cell)) * (4 * per_cell) + upper * 2 * per_cell + spot % (2 * per_cell)
    along_z = (spot // per_cell) * (2 * per_cell) + upper * per_cell + spot % per_cell
    cell = jnp.where(axis == 0, along_x, jnp.where(axis == 1, along_y, along_z))
    is_own = slots < atoms
    group = jnp.where(is_own, 0, axis + 1).astype(F32)
    cell = jnp.where(is_own, own, cell.astype(F32))
    rows = [moved[j : j + 1] + moved[j + 3 : j + 4] + moved[j + 6 : j + 7] for j in range(3)]
    rows += [moved[9:10], moved[10:11]]
    slots = cell + float(atoms) * group
    rows += [slots[k : k + 1] for k in range(neigh)]

    def store(device, carry):
        for j, row in enumerate(rows):
            out_ref[device, j] = row
        return carry

    lax.fori_loop(0, out_ref.shape[0], store, 0)


def end_kernel(structs, got_ref, cells_ref, energy_ref, virial_ref, force_ref):
    devices, count, _, atoms = got_ref.shape
    step = 8

    def add(index, totals):
        return tuple(total + got_ref[index * step + j] for j, total in enumerate(totals))

    totals = lax.fori_loop(
        0, devices // step, add, tuple(jnp.zeros((count, 1, atoms), F32) for _ in range(step))
    )
    while len(totals) > 1:
        totals = tuple(totals[i] + totals[i + 1] for i in range(0, len(totals), 2))
    lines = [totals[0][j] for j in range(count)]
    total = jnp.concatenate(lines[0:3] + [jnp.zeros((5, atoms), F32)], axis=0)
    place = (iota((atoms, atoms), 0) == cells_ref[...]).astype(F32).astype(BF16)
    parts = jnp.concatenate(split3(total), axis=0).astype(BF16)
    moved = dot(parts, place, NT)
    force_ref[...] = (moved[0:8] + moved[8:16] + moved[16:24])[0:3]
    per_row = LANES // structs
    for j in range(10):
        row, column = 3 + j // per_row, (j % per_row) * structs
        value = lines[row][:, column : column + structs]
        if j == 0:
            energy_ref[...] = value
        else:
            virial_ref[j - 1 : j, :] = value


def centre_offsets():
    units = [(1, 0, 0), (0, 1, 0), (0, 0, 1)]
    minus = [tuple(-v for v in unit) for unit in units]
    return units, minus


def plus(a, b):
    return tuple(x + y for x, y in zip(a, b))


def prep_kernel(
    scaling,
    embed_ref,
    up_ref,
    rad_in_ref,
    rad_out_ref,
    mix_ref,
    first_ref,
    hidden_ref,
    last_ref,
    embed_left_ref,
    embed_lift_ref,
    lifted_left_ref,
    mix_left_ref,
    mix_lift_ref,
    mix_read_ref,
    mix_back_ref,
    mix_up_back_ref,
    mix_read_back_ref,
    out_left_ref,
    in_left_ref,
    read_left_ref,
    read_back_ref,
    row_left_ref,
    column_ref,
    table_ref,
):
    elements = embed_ref.shape[0]
    width = up_ref.shape[2]
    table_ref[...] = jnp.zeros_like(table_ref)
    table_ref[0:elements, :] = embed_ref[...]
    embed_t = jnp.transpose(table_ref[...])
    embed_left_ref[...] = jnp.concatenate(split2(embed_t), axis=1)
    lifted_left_ref[...] = jnp.concatenate(
        split2(dot(left3(jnp.transpose(up_ref[0])), right3(embed_t))), axis=1
    )
    up_t = left3(jnp.transpose(up_ref[1]))
    embed_lift_ref[...] = jnp.concatenate(split2(dot(up_t, right3(embed_t))), axis=1)
    mix_t = [jnp.concatenate([jnp.transpose(mix_ref[l, j]) for j in range(3)], axis=1) for l in (0, 1)]
    mix_back = [left3(mix_ref[l].reshape(3 * width, width)) for l in (0, 1)]
    hidden_t = hidden_ref[...]
    hidden = jnp.transpose(hidden_t)
    mix_left_ref[...] = left3(mix_t[0])
    mix_lift_ref[...] = left3(dot(up_t, right3(mix_t[0])))
    mix_read_ref[...] = left3(dot(left3(hidden_t), right3(mix_t[1])))
    mix_back_ref[...] = mix_back[0]
    mix_up_back_ref[...] = left3(dot(mix_back[0], right3(up_ref[1])))
    mix_read_back_ref[...] = left3(dot(mix_back[1], right3(hidden)))
    for l in (0, 1):
        w_out = rad_out_ref[l] * scaling
        out_left_ref[l] = left3(jnp.transpose(w_out))
        w_in = rad_in_ref[l]
        high = w_in.astype(BF16).astype(F32)
        in_left_ref[l] = jnp.concatenate([high, high, w_in - high], axis=0).astype(BF16)
    read_left_ref[...] = left3(hidden_t)
    read_back_ref[...] = left3(hidden)
    first_row = jnp.broadcast_to(first_ref[...], (8, width))
    last_row = jnp.broadcast_to(last_ref[...], (8, last_ref.shape[1]))
    row_left_ref[...] = jnp.concatenate([left3(first_row), left3(last_row)], axis=1)
    column_ref[0:width, :] = jnp.transpose(jnp.broadcast_to(first_ref[...], (LANES, width)))
    column_ref[width:, :] = jnp.transpose(jnp.broadcast_to(last_ref[...], (LANES, last_ref.shape[1])))


def main_kernel(
    sizes,
    structs,
    got_ref,
    embed_left_ref,
    embed_lift_ref,
    lifted_left_ref,
    mix_left_ref,
    mix_lift_ref,
    mix_read_ref,
    mix_back_ref,
    mix_up_back_ref,
    mix_read_back_ref,
    out_left_ref,
    in_left_ref,
    read_left_ref,
    read_back_ref,
    row_left_ref,
    column_ref,
    out_ref,
    radial_ref,
    picked_ref,
    spread_ref,
    change_ref,
    turned_ref,
    slots_ref,
    full_ref,
    feats_ref,
):
    atoms = LANES
    neigh = got_ref.shape[1] - HEAD_ROWS
    edges = neigh * atoms
    width = mix_left_ref.shape[0]
    radial_hidden = in_left_ref.shape[2]
    padded = embed_left_ref.shape[1] // 2
    read_width = read_left_ref.shape[0]
    lanes8 = iota((8, atoms), 1)
    rows8 = iota((8, atoms), 0)
    units, minus = centre_offsets()
    home = (0, 0, 0)
    here = [lax.axis_index(axis) for axis in AXES]

    def device(offset):
        index = 0
        for place, step, size in zip(here, offset, sizes):
            index = index * size + lax.rem(place + step + 2 * size, size)
        return index

    names = {}

    def device_of(offset):
        if offset not in names:
            names[offset] = device(offset)
        return names[offset]

    def head(offset):
        index = device_of(offset)
        rows = [got_ref[index, j] for j in range(HEAD_ROWS)]
        return jnp.concatenate(rows + [jnp.zeros((8 - HEAD_ROWS, atoms), F32)], axis=0)

    heads = {}

    def head_of(offset):
        if offset not in heads:
            heads[offset] = head(offset)
        return heads[offset]

    def slots_of(offset):
        index = device_of(offset)
        rows = [got_ref[index, HEAD_ROWS + k] for k in range(neigh)]
        return jnp.concatenate(rows, axis=1)

    def table(centre):
        groups = [head_of(centre)]
        for q in (1, 2, 3):
            move = jnp.where(rows8 == q - 1, box_side, 0.0)
            groups.append(
                jnp.where(
                    has_bit(lanes8, q),
                    head_of(plus(centre, minus[q - 1])) - move,
                    head_of(plus(centre, units[q - 1])) + move,
                )
            )
        return [jnp.concatenate([groups[j][0:4], groups[j + 1][0:4]], axis=0) for j in (0, 2)]

    def per_edge(row):
        return jnp.concatenate([row] * neigh, axis=1)

    def fold(x):
        total = x[:, 0:atoms]
        for k in range(1, neigh):
            total = total + x[:, k * atoms : (k + 1) * atoms]
        return total

    tall = iota((8, edges), 0)
    order = (tall + 1).astype(F32)
    blocks = []
    for block in range(4):
        if block == 0:
            centres = [home]
            slots = slots_of(home)
            base = head_of(home)
        else:
            centres = [units[block - 1], minus[block - 1]]
            bit = has_bit(lanes8, block)
            slots = jnp.where(per_edge(bit[0:1]), slots_of(centres[1]), slots_of(centres[0]))
            base = jnp.where(bit, head_of(centres[1]), head_of(centres[0]))
        slots = slots.astype(jnp.int32)

        cell, group = slots & (atoms - 1), slots // atoms
        hits = marks(atoms, cell.astype(F32))
        slots_ref[block] = hits
        pairs = [pair for centre in centres for pair in table(centre)]
        stack = jnp.concatenate([part for parts in zip(*map(split3, pairs)) for part in parts], axis=0)
        found = dot(stack.astype(BF16), hits)
        combo = jnp.broadcast_to(group, (8, edges))
        if block:
            combo = combo + per_edge(jnp.where(bit, 4, 0))
        far = None
        size = 8 * len(pairs)
        for j in range(len(pairs)):
            part = found[8 * j : 8 * j + 8] + found[size + 8 * j : size + 8 * j + 8]
            part = part + found[2 * size + 8 * j : 2 * size + 8 * j + 8]
            far = part if far is None else jnp.where(combo >= 2 * j, part, far)
        far = jnp.where((combo & 1) == 1, jnp.concatenate([far[4:8], far[0:4]], axis=0), far)
        vec = jnp.where(tall < 3, far - per_edge(base), 0.0)
        square = jnp.sum(vec * vec, axis=0, keepdims=True) + soften
        square = jnp.broadcast_to(square, (8, edges))
        radius = jnp.sqrt(square)
        inverse = 1.0 / radius
        turn = order * (jnp.minimum(radius, cutoff) * (1.0 / cutoff))
        whole = jnp.floor(turn + 0.5)
        part = (turn - whole) * math.pi
        sign = 1.0 - 2.0 * (whole - 2.0 * jnp.floor(whole * 0.5))
        p2 = part * part
        sine = part * (
            1.0
            + p2 * (-1.0 / 6 + p2 * (1.0 / 120 + p2 * (-1.0 / 5040 + p2 * (1.0 / 362880 - p2 * (1.0 / 39916800)))))
        )
        cosine = 1.0 + p2 * (
            -0.5
            + p2 * (1.0 / 24 + p2 * (-1.0 / 720 + p2 * (1.0 / 40320 + p2 * (-1.0 / 3628800 + p2 * (1.0 / 479001600)))))
        )
        sine, cosine = sine * sign * amplitude, cosine * sign * amplitude
        inside = jnp.maximum(1.0 - square * (1.0 / (cutoff * cutoff)), 0.0)
        envelope = inside * inside
        over = sine * inverse
        bessel = over * envelope
        slope = (
            (order * (math.pi / cutoff) * cosine - over) * inverse * envelope
            - sine * inside * (4.0 / (cutoff * cutoff))
        )
        both = jnp.concatenate([bessel, slope], axis=1)
        high = both.astype(BF16).astype(F32)
        bessel_right = jnp.concatenate([high, both - high, high], axis=0).astype(BF16)
        direction = vec * inverse
        blocks.append(
            dict(
                base=base,
                combo=combo,
                far=far,
                vec=vec,
                inverse=inverse,
                bessel=bessel_right,
                direction=direction,
                struct=base[4:5, :],
            )
        )

    tile = 32

    def spread(block, m, k):
        row = blocks[block]["direction"][m : m + 1, k * atoms : (k + 1) * atoms]
        return jnp.broadcast_to(row, (8, atoms))

    for block in range(4):
        for m in range(3):
            for k in range(neigh):
                spread_ref[block, m * neigh + k] = spread(block, m, k)

    def wide(x):
        return jnp.concatenate([x] * (tile // 8), axis=0)

    def radial(layer, block, saved):
        pre = dot(in_left_ref[layer], blocks[block]["bessel"], TN)
        active, gain = silu(pre[:, 0:edges])
        radial_ref[saved] = dot(out_left_ref[layer], right3(active))
        turned_ref[saved] = right3(gain * pre[:, edges:])

    def change(layer, saved):
        change_ref[saved] = dot(out_left_ref[layer], turned_ref[saved])

    def interact(layer, block, saved):
        scalars = []
        vectors = [[], [], []]
        for start in range(0, width, tile):
            scalar = None
            vector = [None, None, None]
            for k in range(neigh):
                cut = pl.ds(k * atoms, atoms)
                rows = picked_ref[saved, pl.ds(start, tile), cut]
                zero = radial_ref[saved, pl.ds(start, tile), cut] * rows
                one = radial_ref[saved, pl.ds(width + start, tile), cut] * rows
                if layer == 0:
                    radial_ref[saved, pl.ds(width + start, tile), cut] = one
                scalar = zero if scalar is None else scalar + zero
                for m in range(3):
                    term = wide(spread_ref[block, m * neigh + k]) * one
                    vector[m] = term if vector[m] is None else vector[m] + term
            scalars.append(scalar)
            for m in range(3):
                vectors[m].append(vector[m])
        return jnp.concatenate(scalars, axis=0), [jnp.concatenate(v, axis=0) for v in vectors]

    def invariants(kept):
        scalar = jnp.concatenate([k[0] for k in kept], axis=1)
        square = jnp.concatenate([k[1][0] * k[1][0] + k[1][1] * k[1][1] + k[1][2] * k[1][2] for k in kept], axis=1)
        return right3(jnp.concatenate([scalar, square, scalar * scalar], axis=0))

    def add_up(value, total):
        part = value[0:8]
        for j in range(8, tile, 8):
            part = part + value[j : j + 8]
        return part if total is None else total + part

    odd, upper = (rows8 & 1) == 1, (rows8 & 2) == 2

    def gather_rows(values):
        a, b, c, d = values
        low = jnp.where(odd, b, a) + pltpu.roll(jnp.where(odd, a, b), 7, 0)
        high = jnp.where(odd, d, c) + pltpu.roll(jnp.where(odd, c, d), 7, 0)
        both = jnp.where(upper, high, low) + pltpu.roll(jnp.where(upper, low, high), 6, 0)
        return both + pltpu.roll(both, 4, 0)

    def pull(layer, block, saved, kept, d):
        scalar, vector = kept
        d_scalar = d[0:width] + 2.0 * scalar * d[2 * width : 3 * width]
        factor = 2.0 * d[width : 2 * width]
        toward = [[None] * neigh for _ in range(4)]
        d_vector = [v * factor for v in vector]
        for start in range(0, width, tile):
            part = slice(start, start + tile)
            for k in range(neigh):
                cut = pl.ds(k * atoms, atoms)
                rows = picked_ref[saved, pl.ds(start, tile), cut]
                one = radial_ref[saved, pl.ds(width + start, tile), cut]
                both = one * rows if layer else one
                through = None
                for m in range(3):
                    term = wide(spread_ref[block, m * neigh + k]) * d_vector[m][part]
                    through = term if through is None else through + term
                    toward[m][k] = add_up(d_vector[m][part] * both, toward[m][k])
                turned = rows * (
                    change_ref[saved, pl.ds(start, tile), cut] * d_scalar[part]
                    + change_ref[saved, pl.ds(width + start, tile), cut] * through
                )
                toward[3][k] = add_up(turned, toward[3][k])
                if layer:
                    picked_ref[saved, pl.ds(start, tile), cut] = (
                        radial_ref[saved, pl.ds(start, tile), cut] * d_scalar[part] + one * through
                    )
        own = blocks[block]
        lines = jnp.concatenate([gather_rows([toward[m][k] for m in range(4)]) for k in range(neigh)], axis=1)
        d_direction = jnp.where(tall < 3, lines, 0.0)
        inverse, direction = own["inverse"], own["direction"]
        radial_part = lines[3:4] - jnp.sum(d_direction * direction, axis=0, keepdims=True) * inverse
        return d_direction * inverse + radial_part * direction

    kept0 = []
    kinds = jnp.concatenate([blocks[block]["base"][3:4, :] for block in range(4)], axis=1)
    hits = marks(padded, kinds)
    hits = jnp.concatenate([hits, hits], axis=0)
    feats_ref[...] = dot(embed_lift_ref[...], hits)
    initial = dot(embed_left_ref[...], hits[:, 0:atoms])

    def ready(block):
        hits = marks(padded, blocks[block]["far"][3:4, :])
        picked_ref[block] = dot(lifted_left_ref[...], jnp.concatenate([hits, hits], axis=0))
        radial(0, block, block)

    ready(0)
    for block in range(4):
        if block < 3:
            ready(block + 1)
        else:
            radial(1, 0, 4)
        kept0.append(interact(0, block, block))
        if block % 2:
            cut = slice((block - 1) * atoms, (block + 1) * atoms)
            mixing = invariants(kept0[block - 1 : block + 1])
            feats_ref[:, cut] = feats_ref[:, cut] + dot(mix_lift_ref[...], mixing)
            if block == 1:
                layer_out = initial + dot(mix_left_ref[...], mixing[:, 0:atoms])

    own_group = blocks[0]["combo"][0:1, :].astype(F32).astype(BF16)
    hits = slots_ref[0]
    for q in range(4):
        full_ref[q * atoms : (q + 1) * atoms, :] = jnp.where(
            own_group == jnp.bfloat16(q), hits, jnp.bfloat16(0)
        )
    high, low = split2(feats_ref[...])
    both = dot(jnp.concatenate([high, low], axis=0), full_ref[...])
    picked_ref[4] = both[0:width] + both[width:]
    change(1, 4)
    kept1 = interact(1, 0, 4)

    pre = dot(mix_read_ref[...], invariants([kept1])) + dot(read_left_ref[...], right3(layer_out))
    active, gain = silu(pre)
    atom_energy = dot(row_left_ref[:, 0 : 3 * width], right3(layer_out)) + dot(
        row_left_ref[:, 3 * width :], right3(active)
    )
    first_column = column_ref[0:width, :]
    turned = right3(column_ref[width : width + read_width, :] * gain)
    d_own = dot(read_back_ref[...], turned) + column_ref[0:width, :]

    d_mixed = dot(mix_read_back_ref[...], turned)
    d_mixed_own = dot(mix_back_ref[...], right3(d_own))
    change(0, 0)
    edge_grad_one = pull(1, 0, 4, kept1, d_mixed)
    high, low = split2(picked_ref[4])
    back = dot(jnp.concatenate([high, low], axis=0), full_ref[...], NT)

    forces = {}
    d_mixed = dot(mix_up_back_ref[...], right3(back[0:width] + back[width:]))
    d_mixed = [d_mixed[:, block * atoms : (block + 1) * atoms] for block in range(4)]
    d_mixed[0] = d_mixed[0] + d_mixed_own

    def push(offset, value):
        forces[offset] = forces[offset] + value if offset in forces else value

    sums = None
    for block in range(4):
        if block < 3:
            change(0, block + 1)
        grad = pull(0, block, block, kept0[block], d_mixed[block])
        if block == 0:
            grad = grad + edge_grad_one
        own = blocks[block]
        centres = [home] if block == 0 else [units[block - 1], minus[block - 1]]
        pulled = fold(grad)
        if block == 0:
            push(home, pulled)
        else:
            bit = has_bit(lanes8, block)
            push(centres[1], jnp.where(bit, pulled, 0.0))
            push(centres[0], jnp.where(bit, 0.0, pulled))
        high = grad.astype(BF16).astype(F32)
        pair = jnp.concatenate([high[0:4], (grad - high)[0:4]], axis=0)
        stack = [jnp.where(own["combo"] == j, pair, 0.0) for j in range(4 * len(centres))]
        landed = dot(jnp.concatenate(stack, axis=0).astype(BF16), slots_ref[block], NT)
        for c, centre in enumerate(centres):
            for q in range(4):
                j = 4 * c + q
                value = -landed[8 * j : 8 * j + 8]
                if q == 0:
                    push(centre, value)
                else:
                    bit = has_bit(lanes8, q)
                    push(plus(centre, minus[q - 1]), jnp.where(bit, value, 0.0))
                    push(plus(centre, units[q - 1]), jnp.where(bit, 0.0, value))
        rows = []
        for r in range(3):
            rows.append(-fold(jnp.broadcast_to(own["vec"][r : r + 1, :], (8, edges)) * grad))
        if block == 0:
            rows.append(atom_energy)
        rows = jnp.concatenate(rows, axis=0)
        member = (own["struct"].astype(jnp.int32) == (iota((atoms, atoms), 0) & (structs - 1))).astype(F32)
        high, low = split2(rows)
        got = dot(jnp.concatenate([high, low], axis=0), member.astype(BF16), NT)
        got = got[0 : rows.shape[0]] + got[rows.shape[0] :]
        if block == 0:
            energy_row = got[24:25]
            sums = got[0:24]
        else:
            sums = sums + got

    per_row = LANES // structs
    lane_row = iota((1, atoms), 1) // structs
    packed = []
    for row in range(-(-10 // per_row)):
        line = jnp.zeros((1, atoms), F32)
        for j in range(row * per_row, min(10, (row + 1) * per_row)):
            if j == 0:
                value = energy_row
            else:
                r, t = divmod(j - 1, 3)
                value = sums[8 * r + t : 8 * r + t + 1]
            line = line + jnp.where(lane_row == j - row * per_row, value, 0.0)
        packed.append(line)

    def store(index, carry):
        for m in range(3):
            out_ref[index, m] = jnp.zeros((1, atoms), F32)
        for j, line in enumerate(packed):
            out_ref[index, 3 + j] = line
        return carry

    lax.fori_loop(0, out_ref.shape[0], store, 0)
    for offset, value in forces.items():
        value = value[0:3] + value[4:7]
        index = device_of(offset)
        for m in range(3):
            out_ref[index, m] = out_ref[index, m] + value[m : m + 1, :]


def whole(memory_space=pltpu.VMEM):
    return pl.BlockSpec(memory_space=memory_space)


def shards(
    sizes,
    positions,
    species,
    cell_map,
    neighbours,
    struct_ids,
    embed,
    w_up,
    w_rad_in,
    w_rad_out,
    w_mix,
    read_first,
    read_hidden,
    read_last,
):
    devices = math.prod(sizes)
    atoms = positions.shape[1]
    neigh = neighbours.shape[0]
    width = w_up.shape[2]
    structs = SLAB_STRUCTS * sizes[0]
    elements = embed.shape[0]
    padded = -(-elements // LANES) * LANES
    edges = neigh * atoms
    params = pltpu.CompilerParams(vmem_limit_bytes=32 << 20)
    small = pltpu.CompilerParams(vmem_limit_bytes=8 << 20)
    sent = pl.pallas_call(
        pack_kernel,
        out_shape=jax.ShapeDtypeStruct((devices, HEAD_ROWS + neigh, 1, atoms), F32),
        in_specs=[whole()] * 5,
        out_specs=whole(),
        compiler_params=pltpu.CompilerParams(vmem_limit_bytes=60 << 20),
        name="pack",
    )(positions, species.reshape(1, -1), cell_map, neighbours, struct_ids.reshape(1, -1))
    got = lax.all_to_all(sent, AXES, 0, 0, tiled=True)
    radial_hidden, read_width, bessels = w_rad_in.shape[2], read_hidden.shape[1], w_rad_in.shape[1]
    shapes = [
        ((width, 2 * padded), BF16),
        ((width, 2 * padded), BF16),
        ((width, 2 * padded), BF16),
        ((width, 9 * width), BF16),
        ((width, 9 * width), BF16),
        ((read_width, 9 * width), BF16),
        ((3 * width, 3 * width), BF16),
        ((3 * width, 3 * width), BF16),
        ((3 * width, 3 * read_width), BF16),
        ((2, 2 * width, 3 * radial_hidden), BF16),
        ((2, 3 * bessels, radial_hidden), BF16),
        ((read_width, 3 * width), BF16),
        ((width, 3 * read_width), BF16),
        ((8, 3 * width + 3 * read_width), BF16),
        ((width + read_width, atoms), F32),
    ]
    weights = pl.pallas_call(
        functools.partial(prep_kernel, 1.0 / math.sqrt(neigh)),
        out_shape=[jax.ShapeDtypeStruct(*shape) for shape in shapes],
        in_specs=[whole()] * 8,
        out_specs=[whole()] * len(shapes),
        scratch_shapes=[pltpu.VMEM((padded, width), F32)],
        compiler_params=small,
        cost_estimate=pl.CostEstimate(flops=4_000_000_000, bytes_accessed=2_000_000, transcendentals=0),
        name="weights",
    )(
        embed,
        w_up,
        w_rad_in,
        w_rad_out,
        w_mix,
        read_first.reshape(1, -1),
        read_hidden.T,
        read_last.reshape(1, -1),
    )
    count = TAIL_ROWS - (-10 // (LANES // structs))
    parts = pl.pallas_call(
        functools.partial(main_kernel, sizes, structs),
        out_shape=jax.ShapeDtypeStruct((devices, count, 1, atoms), F32),
        in_specs=[whole()] * (1 + len(shapes)),
        out_specs=whole(),
        scratch_shapes=[
            pltpu.VMEM((5, 2 * width, edges), F32),
            pltpu.VMEM((5, width, edges), F32),
            pltpu.VMEM((4, 3 * neigh, 8, atoms), F32),
            pltpu.VMEM((5, 2 * width, edges), F32),
            pltpu.VMEM((5, 3 * radial_hidden, edges), BF16),
            pltpu.VMEM((4, atoms, edges), BF16),
            pltpu.VMEM((4 * atoms, edges), BF16),
            pltpu.VMEM((width, 4 * atoms), F32),
        ],
        compiler_params=params,
        name="forces",
    )(got, *weights)
    back = lax.all_to_all(parts, AXES, 0, 0, tiled=True)
    energies, virials, forces = pl.pallas_call(
        functools.partial(end_kernel, structs),
        out_shape=(
            jax.ShapeDtypeStruct((1, structs), F32),
            jax.ShapeDtypeStruct((9, structs), F32),
            jax.ShapeDtypeStruct((3, atoms), F32),
        ),
        in_specs=[whole()] * 2,
        out_specs=(whole(),) * 3,
        compiler_params=small,
        name="finish",
    )(back, cell_map)
    return energies.reshape(-1), virials, forces


def solution(mesh):
    sizes = tuple(mesh.shape[axis] for axis in AXES)
    return jax.shard_map(
        functools.partial(shards, sizes),
        mesh=mesh,
        in_specs=(
            P(None, AXES),
            P(AXES),
            P(AXES, None),
            P(None, AXES),
            P(AXES),
            P(),
            P(),
            P(),
            P(),
            P(),
            P(),
            P(),
            P(),
        ),
        out_specs=(P(), P(), P(None, AXES)),
        check_vma=False,
    )
```

```python
import functools
import math

import jax
import jax.numpy as jnp
from jax import lax
from jax.experimental import pallas as pl
from jax.experimental.pallas import tpu as pltpu
from jax.sharding import PartitionSpec as P

AXES = ("gx", "gy", "gz")
SLAB_STRUCTS = 4
LANES = 128
HEAD_ROWS = 5
TAIL_ROWS = 3

cutoff = 6.0
box_side = 4.5
soften = 0.25
amplitude = math.sqrt(2.0 / cutoff)

F32 = jnp.float32
BF16 = jnp.bfloat16
NN = (((1,), (0,)), ((), ()))
NT = (((1,), (1,)), ((), ()))
TN = (((0,), (0,)), ((), ()))


def dot(left, right, dims=NN):
    return lax.dot_general(left, right, dims, preferred_element_type=F32)


def split2(x):
    high = x.astype(BF16)
    return high, (x - high.astype(F32)).astype(BF16)


def split3(x):
    high = x.astype(BF16).astype(F32)
    rest = x - high
    middle = rest.astype(BF16).astype(F32)
    return high, middle, rest - middle


def left3(x):
    high, low = split2(x)
    return jnp.concatenate([high, high, low], axis=1)


def right3(x):
    high, low = split2(x)
    return jnp.concatenate([high, low, high], axis=0)


def iota(shape, axis):
    return lax.broadcasted_iota(jnp.int32, shape, axis)


def marks(count, row):
    labels = iota((count, row.shape[1]), 0).astype(F32).astype(BF16)
    return jnp.where(labels == row.astype(BF16), jnp.bfloat16(1), jnp.bfloat16(0))


def silu(x):
    sigma = 0.5 + 0.5 * jnp.tanh(0.5 * x)
    value = x * sigma
    return value, sigma + value * (1.0 - sigma)


def has_bit(lanes, group):
    per_cell = LANES // 8
    width = per_cell * 2 ** (3 - group)
    return (lanes & width) != 0


def pack_kernel(pos_ref, species_ref, cells_ref, nbr_ref, struct_ref, out_ref, own_ref):
    atoms = pos_ref.shape[1]
    per_cell = atoms // 8
    place = (iota((atoms, atoms), 0) == cells_ref[...]).astype(F32).astype(BF16)
    neigh = nbr_ref.shape[0]
    lanes = iota((8, atoms), 1)
    inverse = dot(lanes.astype(F32).astype(BF16), place, NT)
    high = nbr_ref[...] // atoms
    parts = jnp.concatenate(
        [*split3(pos_ref[...]), species_ref[...].astype(F32), struct_ref[...].astype(F32)], axis=0
    )
    blank = jnp.zeros((16 - parts.shape[0], atoms), F32)
    low = (nbr_ref[...] - high * atoms).astype(F32)
    moved = dot(jnp.concatenate([parts, blank, low, high.astype(F32)], axis=0).astype(BF16), place)
    low, high = moved[16 : 16 + neigh], moved[16 + neigh :]
    slots = (low + float(atoms) * high).astype(jnp.int32)
    hits = jnp.concatenate([marks(atoms, low[k : k + 1, :]) for k in range(neigh)], axis=1)
    found = dot(inverse.astype(BF16), hits)
    own = jnp.concatenate([found[0:1, k * atoms : (k + 1) * atoms] for k in range(neigh)], axis=0)
    face_atoms = 4 * per_cell
    beyond = jnp.maximum(slots - atoms, 0)
    face = beyond // face_atoms
    spot = beyond - face * face_atoms
    upper = 1 - (face & 1)
    axis = face // 2
    along_x = upper * 4 * per_cell + spot
    along_y = (spot // (2 * per_cell)) * (4 * per_cell) + upper * 2 * per_cell + spot % (2 * per_cell)
    along_z = (spot // per_cell) * (2 * per_cell) + upper * per_cell + spot % per_cell
    cell = jnp.where(axis == 0, along_x, jnp.where(axis == 1, along_y, along_z))
    is_own = slots < atoms
    group = jnp.where(is_own, 0, axis + 1).astype(F32)
    cell = jnp.where(is_own, own, cell.astype(F32))
    rows = [moved[j : j + 1] + moved[j + 3 : j + 4] + moved[j + 6 : j + 7] for j in range(3)]
    rows += [moved[9:10], moved[10:11]]
    slots = cell + float(atoms) * group
    rows += [slots[k : k + 1] for k in range(neigh)]

    for j, row in enumerate(rows):
        own_ref[0, j] = row

    def store(device, carry):
        for j, row in enumerate(rows):
            out_ref[device, j] = row
        return carry

    lax.fori_loop(0, out_ref.shape[0], store, 0)


def end_kernel(structs, got_ref, cells_ref, energy_ref, virial_ref, force_ref):
    devices, count, _, atoms = got_ref.shape
    step = 8

    def add(index, totals):
        return tuple(total + got_ref[index * step + j] for j, total in enumerate(totals))

    totals = lax.fori_loop(
        0, devices // step, add, tuple(jnp.zeros((count, 1, atoms), F32) for _ in range(step))
    )
    while len(totals) > 1:
        totals = tuple(totals[i] + totals[i + 1] for i in range(0, len(totals), 2))
    lines = [totals[0][j] for j in range(count)]
    total = jnp.concatenate(lines[0:3] + [jnp.zeros((5, atoms), F32)], axis=0)
    place = (iota((atoms, atoms), 0) == cells_ref[...]).astype(F32).astype(BF16)
    parts = jnp.concatenate(split3(total), axis=0).astype(BF16)
    moved = dot(parts, place, NT)
    force_ref[...] = (moved[0:8] + moved[8:16] + moved[16:24])[0:3]
    per_row = LANES // structs
    for j in range(10):
        row, column = 3 + j // per_row, (j % per_row) * structs
        value = lines[row][:, column : column + structs]
        if j == 0:
            energy_ref[...] = value
        else:
            virial_ref[j - 1 : j, :] = value


def centre_offsets():
    units = [(1, 0, 0), (0, 1, 0), (0, 0, 1)]
    minus = [tuple(-v for v in unit) for unit in units]
    return units, minus


def plus(a, b):
    return tuple(x + y for x, y in zip(a, b))


def prep_kernel(
    scaling,
    own_ref,
    embed_ref,
    up_ref,
    rad_in_ref,
    rad_out_ref,
    mix_ref,
    first_ref,
    hidden_ref,
    last_ref,
    embed_lift_ref,
    lifted_left_ref,
    mix_left_ref,
    mix_lift_ref,
    mix_read_ref,
    mix_back_ref,
    mix_up_back_ref,
    mix_read_back_ref,
    out_left_ref,
    in_left_ref,
    read_left_ref,
    read_back_ref,
    row_left_ref,
    column_ref,
    own_hits_ref,
    full_ref,
    initial_ref,
    table_ref,
):
    elements = embed_ref.shape[0]
    width = up_ref.shape[2]
    table_ref[...] = jnp.zeros_like(table_ref)
    table_ref[0:elements, :] = embed_ref[...]
    embed_t = jnp.transpose(table_ref[...])
    atoms = own_ref.shape[3]
    neigh = own_ref.shape[1] - HEAD_ROWS
    slots = jnp.concatenate([own_ref[0, HEAD_ROWS + k] for k in range(neigh)], axis=1)
    group = jnp.floor(slots * (1.0 / atoms))
    hits = marks(atoms, slots - group * atoms)
    own_hits_ref[...] = hits
    group = group.astype(BF16)
    for q in range(4):
        full_ref[q * atoms : (q + 1) * atoms, :] = jnp.where(group == jnp.bfloat16(q), hits, jnp.bfloat16(0))
    kinds = marks(table_ref.shape[0], own_ref[0, 3])
    initial_ref[...] = dot(
        jnp.concatenate(split2(embed_t), axis=1), jnp.concatenate([kinds, kinds], axis=0)
    )
    lifted_left_ref[...] = jnp.concatenate(
        split2(dot(left3(jnp.transpose(up_ref[0])), right3(embed_t))), axis=1
    )
    up_t = left3(jnp.transpose(up_ref[1]))
    embed_lift_ref[...] = jnp.concatenate(split2(dot(up_t, right3(embed_t))), axis=1)
    mix_t = [jnp.concatenate([jnp.transpose(mix_ref[l, j]) for j in range(3)], axis=1) for l in (0, 1)]
    mix_back = [left3(mix_ref[l].reshape(3 * width, width)) for l in (0, 1)]
    hidden_t = hidden_ref[...]
    hidden = jnp.transpose(hidden_t)
    mix_left_ref[...] = left3(mix_t[0])
    mix_lift_ref[...] = left3(dot(up_t, right3(mix_t[0])))
    mix_read_ref[...] = left3(dot(left3(hidden_t), right3(mix_t[1])))
    mix_back_ref[...] = mix_back[0]
    mix_up_back_ref[...] = left3(dot(mix_back[0], right3(up_ref[1])))
    mix_read_back_ref[...] = left3(dot(mix_back[1], right3(hidden)))
    for l in (0, 1):
        w_out = rad_out_ref[l] * scaling
        out_left_ref[l] = left3(jnp.transpose(w_out))
        w_in = 0.5 * rad_in_ref[l]
        high = w_in.astype(BF16).astype(F32)
        in_left_ref[l] = jnp.concatenate([high, high, w_in - high], axis=0).astype(BF16)
    read_left_ref[...] = left3(hidden_t)
    read_back_ref[...] = left3(hidden)
    first_row = jnp.broadcast_to(first_ref[...], (8, width))
    last_row = jnp.broadcast_to(last_ref[...], (8, last_ref.shape[1]))
    row_left_ref[...] = jnp.concatenate([left3(first_row), left3(last_row)], axis=1)
    column_ref[0:width, :] = jnp.transpose(jnp.broadcast_to(first_ref[...], (LANES, width)))
    column_ref[width:, :] = jnp.transpose(jnp.broadcast_to(last_ref[...], (LANES, last_ref.shape[1])))


def main_kernel(
    sizes,
    structs,
    got_ref,
    embed_lift_ref,
    lifted_left_ref,
    mix_left_ref,
    mix_lift_ref,
    mix_read_ref,
    mix_back_ref,
    mix_up_back_ref,
    mix_read_back_ref,
    out_left_ref,
    in_left_ref,
    read_left_ref,
    read_back_ref,
    row_left_ref,
    column_ref,
    own_hits_ref,
    full_ref,
    initial_ref,
    out_ref,
    radial_ref,
    picked_ref,
    spread_ref,
    change_ref,
    turned_ref,
    slots_ref,
    feats_ref,
):
    atoms = LANES
    neigh = got_ref.shape[1] - HEAD_ROWS
    edges = neigh * atoms
    width = mix_left_ref.shape[0]
    radial_hidden = in_left_ref.shape[2]
    padded = embed_lift_ref.shape[1] // 2
    read_width = read_left_ref.shape[0]
    lanes8 = iota((8, atoms), 1)
    rows8 = iota((8, atoms), 0)
    units, minus = centre_offsets()
    home = (0, 0, 0)
    here = [lax.axis_index(axis) for axis in AXES]

    def device(offset):
        index = 0
        for place, step, size in zip(here, offset, sizes):
            index = index * size + lax.rem(place + step + 2 * size, size)
        return index

    names = {}

    def device_of(offset):
        if offset not in names:
            names[offset] = device(offset)
        return names[offset]

    def head(offset):
        index = device_of(offset)
        rows = [got_ref[index, j] for j in range(HEAD_ROWS)]
        return jnp.concatenate(rows + [jnp.zeros((8 - HEAD_ROWS, atoms), F32)], axis=0)

    heads = {}

    def head_of(offset):
        if offset not in heads:
            heads[offset] = head(offset)
        return heads[offset]

    def slots_of(offset):
        index = device_of(offset)
        rows = [got_ref[index, HEAD_ROWS + k] for k in range(neigh)]
        return jnp.concatenate(rows, axis=1)

    def table(centre):
        groups = [head_of(centre)]
        for q in (1, 2, 3):
            move = jnp.where(rows8 == q - 1, box_side, 0.0)
            groups.append(
                jnp.where(
                    has_bit(lanes8, q),
                    head_of(plus(centre, minus[q - 1])) - move,
                    head_of(plus(centre, units[q - 1])) + move,
                )
            )
        return [jnp.concatenate([groups[j][0:4], groups[j + 1][0:4]], axis=0) for j in (0, 2)]

    def per_edge(row):
        return jnp.concatenate([row] * neigh, axis=1)

    def fold(x):
        total = x[:, 0:atoms]
        for k in range(1, neigh):
            total = total + x[:, k * atoms : (k + 1) * atoms]
        return total

    tall = iota((8, edges), 0)
    order = (tall + 1).astype(F32)
    blocks = []
    for block in range(4):
        if block == 0:
            centres = [home]
            slots = slots_of(home)
            base = head_of(home)
        else:
            centres = [units[block - 1], minus[block - 1]]
            bit = has_bit(lanes8, block)
            slots = jnp.where(per_edge(bit[0:1]), slots_of(centres[1]), slots_of(centres[0]))
            base = jnp.where(bit, head_of(centres[1]), head_of(centres[0]))
        slots = slots.astype(jnp.int32)

        cell, group = slots & (atoms - 1), slots // atoms
        if block == 0:
            hits = own_hits_ref[...]
        else:
            hits = marks(atoms, cell.astype(F32))
            slots_ref[block] = hits
        pairs = [pair for centre in centres for pair in table(centre)]
        stack = jnp.concatenate([part for parts in zip(*map(split3, pairs)) for part in parts], axis=0)
        found = dot(stack.astype(BF16), hits)
        combo = jnp.broadcast_to(group, (8, edges))
        if block:
            combo = combo + per_edge(jnp.where(bit, 4, 0))
        far = None
        size = 8 * len(pairs)
        for j in range(len(pairs)):
            part = found[8 * j : 8 * j + 8] + found[size + 8 * j : size + 8 * j + 8]
            part = part + found[2 * size + 8 * j : 2 * size + 8 * j + 8]
            far = part if far is None else jnp.where(combo >= 2 * j, part, far)
        far = jnp.where((combo & 1) == 1, jnp.concatenate([far[4:8], far[0:4]], axis=0), far)
        vec = jnp.where(tall < 3, far - per_edge(base), 0.0)
        square = jnp.sum(vec * vec, axis=0, keepdims=True) + soften
        square = jnp.broadcast_to(square, (8, edges))
        radius = jnp.sqrt(square)
        inverse = 1.0 / radius
        turn = order * (jnp.minimum(radius, cutoff) * (1.0 / cutoff))
        whole = jnp.floor(turn + 0.5)
        part = (turn - whole) * math.pi
        pairs = jnp.floor(whole * 0.5)
        sign = amplitude - (2.0 * amplitude) * whole + (4.0 * amplitude) * pairs
        p2 = part * part
        sine = part * (
            1.0
            + p2 * (-1.0 / 6 + p2 * (1.0 / 120 + p2 * (-1.0 / 5040 + p2 * (1.0 / 362880 - p2 * (1.0 / 39916800)))))
        )
        cosine = 1.0 + p2 * (
            -0.5
            + p2 * (1.0 / 24 + p2 * (-1.0 / 720 + p2 * (1.0 / 40320 + p2 * (-1.0 / 3628800 + p2 * (1.0 / 479001600)))))
        )
        sine, cosine = sine * sign, cosine * sign
        inside = jnp.maximum(1.0 - square * (1.0 / (cutoff * cutoff)), 0.0)
        envelope = inside * inside
        over = sine * inverse
        bessel = over * envelope
        slope = (
            (order * (math.pi / cutoff) * cosine - over) * inverse * envelope
            - sine * inside * (4.0 / (cutoff * cutoff))
        )
        both = jnp.concatenate([bessel, slope], axis=1)
        high = both.astype(BF16).astype(F32)
        bessel_right = jnp.concatenate([high, both - high, high], axis=0).astype(BF16)
        direction = vec * inverse
        blocks.append(
            dict(
                base=base,
                combo=combo,
                far=far,
                vec=vec,
                inverse=inverse,
                bessel=bessel_right,
                direction=direction,
                struct=base[4:5, :],
            )
        )

    tile = 32

    def spread(block, m, k):
        row = blocks[block]["direction"][m : m + 1, k * atoms : (k + 1) * atoms]
        return jnp.broadcast_to(row, (8, atoms))

    for block in range(4):
        for m in range(3):
            for k in range(neigh):
                spread_ref[block, m * neigh + k] = spread(block, m, k)

    def wide(x):
        return jnp.concatenate([x] * (tile // 8), axis=0)

    def radial(layer, block, saved):
        pre = dot(in_left_ref[layer], blocks[block]["bessel"], TN)
        turn = jnp.tanh(pre[:, 0:edges])
        more, less = 1.0 + turn, 1.0 - turn
        active = pre[:, 0:edges] * more
        radial_ref[saved] = dot(out_left_ref[layer], right3(active))
        turned_ref[saved] = right3((more + active * less) * pre[:, edges:])

    def change(layer, saved):
        change_ref[saved] = dot(out_left_ref[layer], turned_ref[saved])

    def interact(layer, block, saved):
        scalars = []
        vectors = [[], [], []]
        for start in range(0, width, tile):
            scalar = None
            vector = [None, None, None]
            for k in range(neigh):
                cut = pl.ds(k * atoms, atoms)
                rows = picked_ref[saved, pl.ds(start, tile), cut]
                zero = radial_ref[saved, pl.ds(start, tile), cut] * rows
                one = radial_ref[saved, pl.ds(width + start, tile), cut] * rows
                if layer == 0:
                    radial_ref[saved, pl.ds(width + start, tile), cut] = one
                scalar = zero if scalar is None else scalar + zero
                for m in range(3):
                    term = wide(spread_ref[block, m * neigh + k]) * one
                    vector[m] = term if vector[m] is None else vector[m] + term
            scalars.append(scalar)
            for m in range(3):
                vectors[m].append(vector[m])
        return jnp.concatenate(scalars, axis=0), [jnp.concatenate(v, axis=0) for v in vectors]

    def invariants(kept):
        scalar = jnp.concatenate([k[0] for k in kept], axis=1)
        square = jnp.concatenate([k[1][0] * k[1][0] + k[1][1] * k[1][1] + k[1][2] * k[1][2] for k in kept], axis=1)
        return right3(jnp.concatenate([scalar, square, scalar * scalar], axis=0))

    def add_up(value, total):
        part = value[0:8]
        for j in range(8, tile, 8):
            part = part + value[j : j + 8]
        return part if total is None else total + part

    odd, upper = (rows8 & 1) == 1, (rows8 & 2) == 2

    def gather_rows(values):
        a, b, c, d = values
        low = jnp.where(odd, b, a) + pltpu.roll(jnp.where(odd, a, b), 7, 0)
        high = jnp.where(odd, d, c) + pltpu.roll(jnp.where(odd, c, d), 7, 0)
        both = jnp.where(upper, high, low) + pltpu.roll(jnp.where(upper, low, high), 6, 0)
        return both + pltpu.roll(both, 4, 0)

    def pull(layer, block, saved, kept, d):
        scalar, vector = kept
        d_scalar = d[0:width] + 2.0 * scalar * d[2 * width : 3 * width]
        factor = 2.0 * d[width : 2 * width]
        toward = [[None] * neigh for _ in range(4)]
        d_vector = [v * factor for v in vector]
        for start in range(0, width, tile):
            part = slice(start, start + tile)
            for k in range(neigh):
                cut = pl.ds(k * atoms, atoms)
                rows = picked_ref[saved, pl.ds(start, tile), cut]
                one = radial_ref[saved, pl.ds(width + start, tile), cut]
                both = one * rows if layer else one
                through = None
                for m in range(3):
                    term = wide(spread_ref[block, m * neigh + k]) * d_vector[m][part]
                    through = term if through is None else through + term
                    toward[m][k] = add_up(d_vector[m][part] * both, toward[m][k])
                turned = rows * (
                    change_ref[saved, pl.ds(start, tile), cut] * d_scalar[part]
                    + change_ref[saved, pl.ds(width + start, tile), cut] * through
                )
                toward[3][k] = add_up(turned, toward[3][k])
                if layer:
                    picked_ref[saved, pl.ds(start, tile), cut] = (
                        radial_ref[saved, pl.ds(start, tile), cut] * d_scalar[part] + one * through
                    )
        own = blocks[block]
        lines = jnp.concatenate([gather_rows([toward[m][k] for m in range(4)]) for k in range(neigh)], axis=1)
        d_direction = jnp.where(tall < 3, lines, 0.0)
        inverse, direction = own["inverse"], own["direction"]
        radial_part = lines[3:4] - jnp.sum(d_direction * direction, axis=0, keepdims=True) * inverse
        return d_direction * inverse + radial_part * direction

    kept0 = []
    kinds = jnp.concatenate([blocks[block]["base"][3:4, :] for block in range(4)], axis=1)
    hits = marks(padded, kinds)
    hits = jnp.concatenate([hits, hits], axis=0)
    feats_ref[...] = dot(embed_lift_ref[...], hits)
    initial = initial_ref[...]

    def ready(block):
        hits = marks(padded, blocks[block]["far"][3:4, :])
        picked_ref[block] = dot(lifted_left_ref[...], jnp.concatenate([hits, hits], axis=0))
        radial(0, block, block)

    ready(0)
    for block in range(4):
        if block < 3:
            ready(block + 1)
        else:
            radial(1, 0, 4)
        kept0.append(interact(0, block, block))
        if block % 2:
            cut = slice((block - 1) * atoms, (block + 1) * atoms)
            mixing = invariants(kept0[block - 1 : block + 1])
            feats_ref[:, cut] = feats_ref[:, cut] + dot(mix_lift_ref[...], mixing)
            if block == 1:
                layer_out = initial + dot(mix_left_ref[...], mixing[:, 0:atoms])

    high, low = split2(feats_ref[...])
    both = dot(jnp.concatenate([high, low], axis=0), full_ref[...])
    picked_ref[4] = both[0:width] + both[width:]
    change(1, 4)
    kept1 = interact(1, 0, 4)

    pre = dot(mix_read_ref[...], invariants([kept1])) + dot(read_left_ref[...], right3(layer_out))
    active, gain = silu(pre)
    atom_energy = dot(row_left_ref[:, 0 : 3 * width], right3(layer_out)) + dot(
        row_left_ref[:, 3 * width :], right3(active)
    )
    first_column = column_ref[0:width, :]
    turned = right3(column_ref[width : width + read_width, :] * gain)
    d_own = dot(read_back_ref[...], turned) + column_ref[0:width, :]

    d_mixed = dot(mix_read_back_ref[...], turned)
    d_mixed_own = dot(mix_back_ref[...], right3(d_own))
    change(0, 0)
    edge_grad_one = pull(1, 0, 4, kept1, d_mixed)
    high, low = split2(picked_ref[4])
    back = dot(jnp.concatenate([high, low], axis=0), full_ref[...], NT)

    forces = {}
    d_mixed = dot(mix_up_back_ref[...], right3(back[0:width] + back[width:]))
    d_mixed = [d_mixed[:, block * atoms : (block + 1) * atoms] for block in range(4)]
    d_mixed[0] = d_mixed[0] + d_mixed_own

    def push(offset, value):
        forces[offset] = forces[offset] + value if offset in forces else value

    sums = None
    for block in range(4):
        if block < 3:
            change(0, block + 1)
        grad = pull(0, block, block, kept0[block], d_mixed[block])
        if block == 0:
            grad = grad + edge_grad_one
        own = blocks[block]
        centres = [home] if block == 0 else [units[block - 1], minus[block - 1]]
        pulled = fold(grad)
        if block == 0:
            push(home, pulled)
        else:
            bit = has_bit(lanes8, block)
            push(centres[1], jnp.where(bit, pulled, 0.0))
            push(centres[0], jnp.where(bit, 0.0, pulled))
        high = grad.astype(BF16).astype(F32)
        pair = jnp.concatenate([high[0:4], (grad - high)[0:4]], axis=0)
        stack = [jnp.where(own["combo"] == j, pair, 0.0) for j in range(4 * len(centres))]
        landed = dot(jnp.concatenate(stack, axis=0).astype(BF16), slots_ref[block] if block else own_hits_ref[...], NT)
        for c, centre in enumerate(centres):
            for q in range(4):
                j = 4 * c + q
                value = -landed[8 * j : 8 * j + 8]
                if q == 0:
                    push(centre, value)
                else:
                    bit = has_bit(lanes8, q)
                    push(plus(centre, minus[q - 1]), jnp.where(bit, value, 0.0))
                    push(plus(centre, units[q - 1]), jnp.where(bit, 0.0, value))
        rows = []
        for r in range(3):
            rows.append(-fold(jnp.broadcast_to(own["vec"][r : r + 1, :], (8, edges)) * grad))
        if block == 0:
            rows.append(atom_energy)
        rows = jnp.concatenate(rows, axis=0)
        member = (own["struct"].astype(jnp.int32) == (iota((atoms, atoms), 0) & (structs - 1))).astype(F32)
        high, low = split2(rows)
        got = dot(jnp.concatenate([high, low], axis=0), member.astype(BF16), NT)
        got = got[0 : rows.shape[0]] + got[rows.shape[0] :]
        if block == 0:
            energy_row = got[24:25]
            sums = got[0:24]
        else:
            sums = sums + got

    per_row = LANES // structs
    lane_row = iota((1, atoms), 1) // structs
    packed = []
    for row in range(-(-10 // per_row)):
        line = jnp.zeros((1, atoms), F32)
        for j in range(row * per_row, min(10, (row + 1) * per_row)):
            if j == 0:
                value = energy_row
            else:
                r, t = divmod(j - 1, 3)
                value = sums[8 * r + t : 8 * r + t + 1]
            line = line + jnp.where(lane_row == j - row * per_row, value, 0.0)
        packed.append(line)

    def store(index, carry):
        for m in range(3):
            out_ref[index, m] = jnp.zeros((1, atoms), F32)
        for j, line in enumerate(packed):
            out_ref[index, 3 + j] = line
        return carry

    lax.fori_loop(0, out_ref.shape[0], store, 0)
    for offset, value in forces.items():
        value = value[0:3] + value[4:7]
        index = device_of(offset)
        for m in range(3):
            out_ref[index, m] = out_ref[index, m] + value[m : m + 1, :]


def whole(memory_space=pltpu.VMEM):
    return pl.BlockSpec(memory_space=memory_space)


def shards(
    sizes,
    positions,
    species,
    cell_map,
    neighbours,
    struct_ids,
    embed,
    w_up,
    w_rad_in,
    w_rad_out,
    w_mix,
    read_first,
    read_hidden,
    read_last,
):
    devices = math.prod(sizes)
    atoms = positions.shape[1]
    neigh = neighbours.shape[0]
    width = w_up.shape[2]
    structs = SLAB_STRUCTS * sizes[0]
    elements = embed.shape[0]
    padded = -(-elements // LANES) * LANES
    edges = neigh * atoms
    params = pltpu.CompilerParams(vmem_limit_bytes=32 << 20)
    small = pltpu.CompilerParams(vmem_limit_bytes=8 << 20)
    sent, own = pl.pallas_call(
        pack_kernel,
        out_shape=[jax.ShapeDtypeStruct((count, HEAD_ROWS + neigh, 1, atoms), F32) for count in (devices, 1)],
        in_specs=[whole()] * 5,
        out_specs=[whole()] * 2,
        compiler_params=pltpu.CompilerParams(vmem_limit_bytes=60 << 20),
        name="pack",
    )(positions, species.reshape(1, -1), cell_map, neighbours, struct_ids.reshape(1, -1))
    got = lax.all_to_all(sent, AXES, 0, 0, tiled=True)
    radial_hidden, read_width, bessels = w_rad_in.shape[2], read_hidden.shape[1], w_rad_in.shape[1]
    shapes = [
        ((width, 2 * padded), BF16),
        ((width, 2 * padded), BF16),
        ((width, 9 * width), BF16),
        ((width, 9 * width), BF16),
        ((read_width, 9 * width), BF16),
        ((3 * width, 3 * width), BF16),
        ((3 * width, 3 * width), BF16),
        ((3 * width, 3 * read_width), BF16),
        ((2, 2 * width, 3 * radial_hidden), BF16),
        ((2, 3 * bessels, radial_hidden), BF16),
        ((read_width, 3 * width), BF16),
        ((width, 3 * read_width), BF16),
        ((8, 3 * width + 3 * read_width), BF16),
        ((width + read_width, atoms), F32),
        ((atoms, edges), BF16),
        ((4 * atoms, edges), BF16),
        ((width, atoms), F32),
    ]
    weights = pl.pallas_call(
        functools.partial(prep_kernel, 1.0 / math.sqrt(neigh)),
        out_shape=[jax.ShapeDtypeStruct(*shape) for shape in shapes],
        in_specs=[whole()] * 9,
        out_specs=[whole()] * len(shapes),
        scratch_shapes=[pltpu.VMEM((padded, width), F32)],
        compiler_params=small,
        cost_estimate=pl.CostEstimate(flops=4_000_000_000, bytes_accessed=2_000_000, transcendentals=0),
        name="weights",
    )(
        own,
        embed,
        w_up,
        w_rad_in,
        w_rad_out,
        w_mix,
        read_first.reshape(1, -1),
        read_hidden.T,
        read_last.reshape(1, -1),
    )
    count = TAIL_ROWS - (-10 // (LANES // structs))
    parts = pl.pallas_call(
        functools.partial(main_kernel, sizes, structs),
        out_shape=jax.ShapeDtypeStruct((devices, count, 1, atoms), F32),
        in_specs=[whole()] * (1 + len(shapes)),
        out_specs=whole(),
        scratch_shapes=[
            pltpu.VMEM((5, 2 * width, edges), F32),
            pltpu.VMEM((5, width, edges), F32),
            pltpu.VMEM((4, 3 * neigh, 8, atoms), F32),
            pltpu.VMEM((5, 2 * width, edges), F32),
            pltpu.VMEM((5, 3 * radial_hidden, edges), BF16),
            pltpu.VMEM((4, atoms, edges), BF16),
            pltpu.VMEM((width, 4 * atoms), F32),
        ],
        compiler_params=params,
        name="forces",
    )(got, *weights)
    back = lax.all_to_all(parts, AXES, 0, 0, tiled=True)
    energies, virials, forces = pl.pallas_call(
        functools.partial(end_kernel, structs),
        out_shape=(
            jax.ShapeDtypeStruct((1, structs), F32),
            jax.ShapeDtypeStruct((9, structs), F32),
            jax.ShapeDtypeStruct((3, atoms), F32),
        ),
        in_specs=[whole()] * 2,
        out_specs=(whole(),) * 3,
        compiler_params=small,
        name="finish",
    )(back, cell_map)
    return energies.reshape(-1), virials, forces


def solution(mesh):
    sizes = tuple(mesh.shape[axis] for axis in AXES)
    return jax.shard_map(
        functools.partial(shards, sizes),
        mesh=mesh,
        in_specs=(
            P(None, AXES),
            P(AXES),
            P(AXES, None),
            P(None, AXES),
            P(AXES),
            P(),
            P(),
            P(),
            P(),
            P(),
            P(),
            P(),
            P(),
        ),
        out_specs=(P(), P(), P(None, AXES)),
        check_vma=False,
    )
```

```python
import functools
import math

import jax
import jax.numpy as jnp
from jax import lax
from jax.experimental import pallas as pl
from jax.experimental.pallas import tpu as pltpu
from jax.sharding import PartitionSpec as P

AXES = ("gx", "gy", "gz")
SLAB_STRUCTS = 4
LANES = 128
HEAD_ROWS = 5
TAIL_ROWS = 3

cutoff = 6.0
box_side = 4.5
soften = 0.25
amplitude = math.sqrt(2.0 / cutoff)

F32 = jnp.float32
BF16 = jnp.bfloat16
NN = (((1,), (0,)), ((), ()))
NT = (((1,), (1,)), ((), ()))
TN = (((0,), (0,)), ((), ()))


def dot(left, right, dims=NN):
    return lax.dot_general(left, right, dims, preferred_element_type=F32)


def split2(x):
    high = x.astype(BF16)
    return high, (x - high.astype(F32)).astype(BF16)


def split3(x):
    high = x.astype(BF16).astype(F32)
    rest = x - high
    middle = rest.astype(BF16).astype(F32)
    return high, middle, rest - middle


def left3(x):
    high, low = split2(x)
    return jnp.concatenate([high, high, low], axis=1)


def right3(x):
    high, low = split2(x)
    return jnp.concatenate([high, low, high], axis=0)


def iota(shape, axis):
    return lax.broadcasted_iota(jnp.int32, shape, axis)


def marks(count, row):
    labels = iota((count, row.shape[1]), 0).astype(F32).astype(BF16)
    return jnp.where(labels == row.astype(BF16), jnp.bfloat16(1), jnp.bfloat16(0))


def silu(x):
    sigma = 0.5 + 0.5 * jnp.tanh(0.5 * x)
    value = x * sigma
    return value, sigma + value * (1.0 - sigma)


def has_bit(lanes, group):
    per_cell = LANES // 8
    width = per_cell * 2 ** (3 - group)
    return (lanes & width) != 0


def pack_kernel(pos_ref, species_ref, cells_ref, nbr_ref, struct_ref, out_ref, own_ref):
    atoms = pos_ref.shape[1]
    per_cell = atoms // 8
    place = (iota((atoms, atoms), 0) == cells_ref[...]).astype(F32).astype(BF16)
    neigh = nbr_ref.shape[0]
    lanes = iota((8, atoms), 1)
    inverse = dot(lanes.astype(F32).astype(BF16), place, NT)
    high = nbr_ref[...] // atoms
    parts = jnp.concatenate(
        [*split3(pos_ref[...]), species_ref[...].astype(F32), struct_ref[...].astype(F32)], axis=0
    )
    blank = jnp.zeros((16 - parts.shape[0], atoms), F32)
    low = (nbr_ref[...] - high * atoms).astype(F32)
    moved = dot(jnp.concatenate([parts, blank, low, high.astype(F32)], axis=0).astype(BF16), place)
    low, high = moved[16 : 16 + neigh], moved[16 + neigh :]
    slots = (low + float(atoms) * high).astype(jnp.int32)
    hits = jnp.concatenate([marks(atoms, low[k : k + 1, :]) for k in range(neigh)], axis=1)
    found = dot(inverse.astype(BF16), hits)
    own = jnp.concatenate([found[0:1, k * atoms : (k + 1) * atoms] for k in range(neigh)], axis=0)
    face_atoms = 4 * per_cell
    beyond = jnp.maximum(slots - atoms, 0)
    face = beyond // face_atoms
    spot = beyond - face * face_atoms
    upper = 1 - (face & 1)
    axis = face // 2
    along_x = upper * 4 * per_cell + spot
    along_y = (spot // (2 * per_cell)) * (4 * per_cell) + upper * 2 * per_cell + spot % (2 * per_cell)
    along_z = (spot // per_cell) * (2 * per_cell) + upper * per_cell + spot % per_cell
    cell = jnp.where(axis == 0, along_x, jnp.where(axis == 1, along_y, along_z))
    is_own = slots < atoms
    group = jnp.where(is_own, 0, axis + 1).astype(F32)
    cell = jnp.where(is_own, own, cell.astype(F32))
    rows = [moved[j : j + 1] + moved[j + 3 : j + 4] + moved[j + 6 : j + 7] for j in range(3)]
    rows += [moved[9:10], moved[10:11]]
    slots = cell + float(atoms) * group
    rows += [slots[k : k + 1] for k in range(neigh)]

    for j, row in enumerate(rows):
        own_ref[0, j] = row

    def store(device, carry):
        for step in range(8):
            for j, row in enumerate(rows):
                out_ref[device * 8 + step, j] = row
        return carry

    lax.fori_loop(0, out_ref.shape[0] // 8, store, 0)


def end_kernel(structs, got_ref, cells_ref, energy_ref, virial_ref, force_ref):
    devices, count, _, atoms = got_ref.shape
    step = 8

    def add(index, totals):
        return tuple(total + got_ref[index * step + j] for j, total in enumerate(totals))

    totals = lax.fori_loop(
        0, devices // step, add, tuple(jnp.zeros((count, 1, atoms), F32) for _ in range(step))
    )
    while len(totals) > 1:
        totals = tuple(totals[i] + totals[i + 1] for i in range(0, len(totals), 2))
    lines = [totals[0][j] for j in range(count)]
    total = jnp.concatenate(lines[0:3] + [jnp.zeros((5, atoms), F32)], axis=0)
    place = (iota((atoms, atoms), 0) == cells_ref[...]).astype(F32).astype(BF16)
    parts = jnp.concatenate(split3(total), axis=0).astype(BF16)
    moved = dot(parts, place, NT)
    force_ref[...] = (moved[0:8] + moved[8:16] + moved[16:24])[0:3]
    per_row = LANES // structs
    for j in range(10):
        row, column = 3 + j // per_row, (j % per_row) * structs
        value = lines[row][:, column : column + structs]
        if j == 0:
            energy_ref[...] = value
        else:
            virial_ref[j - 1 : j, :] = value


def centre_offsets():
    units = [(1, 0, 0), (0, 1, 0), (0, 0, 1)]
    minus = [tuple(-v for v in unit) for unit in units]
    return units, minus


def plus(a, b):
    return tuple(x + y for x, y in zip(a, b))


def prep_kernel(
    scaling,
    own_ref,
    embed_ref,
    up_ref,
    rad_in_ref,
    rad_out_ref,
    mix_ref,
    first_ref,
    hidden_ref,
    last_ref,
    embed_lift_ref,
    lifted_left_ref,
    mix_left_ref,
    mix_lift_ref,
    mix_read_ref,
    mix_back_ref,
    mix_up_back_ref,
    mix_read_back_ref,
    out_left_ref,
    in_left_ref,
    read_left_ref,
    read_back_ref,
    row_left_ref,
    column_ref,
    own_hits_ref,
    full_ref,
    initial_ref,
    table_ref,
):
    elements = embed_ref.shape[0]
    width = up_ref.shape[2]
    table_ref[...] = jnp.zeros_like(table_ref)
    table_ref[0:elements, :] = embed_ref[...]
    embed_t = jnp.transpose(table_ref[...])
    atoms = own_ref.shape[3]
    neigh = own_ref.shape[1] - HEAD_ROWS
    slots = jnp.concatenate([own_ref[0, HEAD_ROWS + k] for k in range(neigh)], axis=1)
    group = jnp.floor(slots * (1.0 / atoms))
    hits = marks(atoms, slots - group * atoms)
    own_hits_ref[...] = hits
    group = group.astype(BF16)
    for q in range(4):
        full_ref[q * atoms : (q + 1) * atoms, :] = jnp.where(group == jnp.bfloat16(q), hits, jnp.bfloat16(0))
    kinds = marks(table_ref.shape[0], own_ref[0, 3])
    initial_ref[...] = dot(
        jnp.concatenate(split2(embed_t), axis=1), jnp.concatenate([kinds, kinds], axis=0)
    )
    lifted_left_ref[...] = jnp.concatenate(
        split2(dot(left3(jnp.transpose(up_ref[0])), right3(embed_t))), axis=1
    )
    up_t = left3(jnp.transpose(up_ref[1]))
    embed_lift_ref[...] = jnp.concatenate(split2(dot(up_t, right3(embed_t))), axis=1)
    mix_t = [jnp.concatenate([jnp.transpose(mix_ref[l, j]) for j in range(3)], axis=1) for l in (0, 1)]
    mix_back = [left3(mix_ref[l].reshape(3 * width, width)) for l in (0, 1)]
    hidden_t = hidden_ref[...]
    hidden = jnp.transpose(hidden_t)
    mix_left_ref[...] = left3(mix_t[0])
    mix_lift_ref[...] = left3(dot(up_t, right3(mix_t[0])))
    mix_read_ref[...] = left3(dot(left3(hidden_t), right3(mix_t[1])))
    mix_back_ref[...] = mix_back[0]
    mix_up_back_ref[...] = left3(dot(mix_back[0], right3(up_ref[1])))
    mix_read_back_ref[...] = left3(dot(mix_back[1], right3(hidden)))
    for l in (0, 1):
        w_out = rad_out_ref[l] * scaling
        out_left_ref[l] = left3(jnp.transpose(w_out))
        w_in = 0.5 * rad_in_ref[l]
        high = w_in.astype(BF16).astype(F32)
        in_left_ref[l] = jnp.concatenate([high, high, w_in - high], axis=0).astype(BF16)
    read_left_ref[...] = left3(hidden_t)
    read_back_ref[...] = left3(hidden)
    first_row = jnp.broadcast_to(first_ref[...], (8, width))
    last_row = jnp.broadcast_to(last_ref[...], (8, last_ref.shape[1]))
    row_left_ref[...] = jnp.concatenate([left3(first_row), left3(last_row)], axis=1)
    column_ref[0:width, :] = jnp.transpose(jnp.broadcast_to(first_ref[...], (LANES, width)))
    column_ref[width:, :] = jnp.transpose(jnp.broadcast_to(last_ref[...], (LANES, last_ref.shape[1])))


def main_kernel(
    sizes,
    structs,
    got_ref,
    embed_lift_ref,
    lifted_left_ref,
    mix_left_ref,
    mix_lift_ref,
    mix_read_ref,
    mix_back_ref,
    mix_up_back_ref,
    mix_read_back_ref,
    out_left_ref,
    in_left_ref,
    read_left_ref,
    read_back_ref,
    row_left_ref,
    column_ref,
    own_hits_ref,
    full_ref,
    initial_ref,
    out_ref,
    radial_ref,
    picked_ref,
    spread_ref,
    change_ref,
    turned_ref,
    slots_ref,
    feats_ref,
):
    atoms = LANES
    neigh = got_ref.shape[1] - HEAD_ROWS
    edges = neigh * atoms
    width = mix_left_ref.shape[0]
    radial_hidden = in_left_ref.shape[2]
    padded = embed_lift_ref.shape[1] // 2
    read_width = read_left_ref.shape[0]
    lanes8 = iota((8, atoms), 1)
    rows8 = iota((8, atoms), 0)
    units, minus = centre_offsets()
    home = (0, 0, 0)
    here = [lax.axis_index(axis) for axis in AXES]

    def device(offset):
        index = 0
        for place, step, size in zip(here, offset, sizes):
            index = index * size + lax.rem(place + step + 2 * size, size)
        return index

    names = {}

    def device_of(offset):
        if offset not in names:
            names[offset] = device(offset)
        return names[offset]

    def head(offset):
        index = device_of(offset)
        rows = [got_ref[index, j] for j in range(HEAD_ROWS)]
        return jnp.concatenate(rows + [jnp.zeros((8 - HEAD_ROWS, atoms), F32)], axis=0)

    heads = {}

    def head_of(offset):
        if offset not in heads:
            heads[offset] = head(offset)
        return heads[offset]

    def slots_of(offset):
        index = device_of(offset)
        rows = [got_ref[index, HEAD_ROWS + k] for k in range(neigh)]
        return jnp.concatenate(rows, axis=1)

    def table(centre):
        groups = [head_of(centre)]
        for q in (1, 2, 3):
            move = jnp.where(rows8 == q - 1, box_side, 0.0)
            groups.append(
                jnp.where(
                    has_bit(lanes8, q),
                    head_of(plus(centre, minus[q - 1])) - move,
                    head_of(plus(centre, units[q - 1])) + move,
                )
            )
        return [jnp.concatenate([groups[j][0:4], groups[j + 1][0:4]], axis=0) for j in (0, 2)]

    def per_edge(row):
        return jnp.concatenate([row] * neigh, axis=1)

    def fold(x):
        total = x[:, 0:atoms]
        for k in range(1, neigh):
            total = total + x[:, k * atoms : (k + 1) * atoms]
        return total

    tall = iota((8, edges), 0)
    order = (tall + 1).astype(F32)
    blocks = []
    for block in range(4):
        if block == 0:
            centres = [home]
            slots = slots_of(home)
            base = head_of(home)
        else:
            centres = [units[block - 1], minus[block - 1]]
            bit = has_bit(lanes8, block)
            slots = jnp.where(per_edge(bit[0:1]), slots_of(centres[1]), slots_of(centres[0]))
            base = jnp.where(bit, head_of(centres[1]), head_of(centres[0]))
        slots = slots.astype(jnp.int32)

        cell, group = slots & (atoms - 1), slots // atoms
        if block == 0:
            hits = own_hits_ref[...]
        else:
            hits = marks(atoms, cell.astype(F32))
            slots_ref[block] = hits
        pairs = [pair for centre in centres for pair in table(centre)]
        stack = jnp.concatenate([part for parts in zip(*map(split3, pairs)) for part in parts], axis=0)
        found = dot(stack.astype(BF16), hits)
        combo = jnp.broadcast_to(group, (8, edges))
        if block:
            combo = combo + per_edge(jnp.where(bit, 4, 0))
        far = None
        size = 8 * len(pairs)
        for j in range(len(pairs)):
            part = found[8 * j : 8 * j + 8] + found[size + 8 * j : size + 8 * j + 8]
            part = part + found[2 * size + 8 * j : 2 * size + 8 * j + 8]
            far = part if far is None else jnp.where(combo >= 2 * j, part, far)
        far = jnp.where((combo & 1) == 1, jnp.concatenate([far[4:8], far[0:4]], axis=0), far)
        vec = jnp.where(tall < 3, far - per_edge(base), 0.0)
        square = jnp.sum(vec * vec, axis=0, keepdims=True) + soften
        square = jnp.broadcast_to(square, (8, edges))
        radius = jnp.sqrt(square)
        inverse = 1.0 / radius
        turn = order * (jnp.minimum(radius, cutoff) * (1.0 / cutoff))
        whole = jnp.floor(turn + 0.5)
        part = (turn - whole) * math.pi
        pairs = jnp.floor(whole * 0.5)
        sign = amplitude - (2.0 * amplitude) * whole + (4.0 * amplitude) * pairs
        p2 = part * part
        sine = part * (
            1.0
            + p2 * (-1.0 / 6 + p2 * (1.0 / 120 + p2 * (-1.0 / 5040 + p2 * (1.0 / 362880 - p2 * (1.0 / 39916800)))))
        )
        cosine = 1.0 + p2 * (
            -0.5
            + p2 * (1.0 / 24 + p2 * (-1.0 / 720 + p2 * (1.0 / 40320 + p2 * (-1.0 / 3628800 + p2 * (1.0 / 479001600)))))
        )
        sine, cosine = sine * sign, cosine * sign
        inside = jnp.maximum(1.0 - square * (1.0 / (cutoff * cutoff)), 0.0)
        envelope = inside * inside
        over = sine * inverse
        bessel = over * envelope
        slope = (
            (order * (math.pi / cutoff) * cosine - over) * inverse * envelope
            - sine * inside * (4.0 / (cutoff * cutoff))
        )
        both = jnp.concatenate([bessel, slope], axis=1)
        high = both.astype(BF16).astype(F32)
        bessel_right = jnp.concatenate([high, both - high, high], axis=0).astype(BF16)
        direction = vec * inverse
        blocks.append(
            dict(
                base=base,
                combo=combo,
                far=far,
                vec=vec,
                inverse=inverse,
                bessel=bessel_right,
                direction=direction,
                struct=base[4:5, :],
            )
        )

    tile = 32

    def spread(block, m, k):
        row = blocks[block]["direction"][m : m + 1, k * atoms : (k + 1) * atoms]
        return jnp.broadcast_to(row, (8, atoms))

    for block in range(4):
        for m in range(3):
            for k in range(neigh):
                spread_ref[block, m * neigh + k] = spread(block, m, k)

    def wide(x):
        return jnp.concatenate([x] * (tile // 8), axis=0)

    def radial(layer, block, saved):
        pre = dot(in_left_ref[layer], blocks[block]["bessel"], TN)
        turn = jnp.tanh(pre[:, 0:edges])
        more, less = 1.0 + turn, 1.0 - turn
        active = pre[:, 0:edges] * more
        radial_ref[saved] = dot(out_left_ref[layer], right3(active))
        turned_ref[saved] = right3((more + active * less) * pre[:, edges:])

    def change(layer, saved):
        change_ref[saved] = dot(out_left_ref[layer], turned_ref[saved])

    def interact(layer, block, saved):
        scalars = []
        vectors = [[], [], []]
        for start in range(0, width, tile):
            scalar = None
            vector = [None, None, None]
            for k in range(neigh):
                cut = pl.ds(k * atoms, atoms)
                rows = picked_ref[saved, pl.ds(start, tile), cut]
                zero = radial_ref[saved, pl.ds(start, tile), cut] * rows
                one = radial_ref[saved, pl.ds(width + start, tile), cut] * rows
                if layer == 0:
                    radial_ref[saved, pl.ds(width + start, tile), cut] = one
                scalar = zero if scalar is None else scalar + zero
                for m in range(3):
                    term = wide(spread_ref[block, m * neigh + k]) * one
                    vector[m] = term if vector[m] is None else vector[m] + term
            scalars.append(scalar)
            for m in range(3):
                vectors[m].append(vector[m])
        return jnp.concatenate(scalars, axis=0), [jnp.concatenate(v, axis=0) for v in vectors]

    def invariants(kept):
        scalar = jnp.concatenate([k[0] for k in kept], axis=1)
        square = jnp.concatenate([k[1][0] * k[1][0] + k[1][1] * k[1][1] + k[1][2] * k[1][2] for k in kept], axis=1)
        return right3(jnp.concatenate([scalar, square, scalar * scalar], axis=0))

    def add_up(value, total):
        part = value[0:8]
        for j in range(8, tile, 8):
            part = part + value[j : j + 8]
        return part if total is None else total + part

    odd, upper = (rows8 & 1) == 1, (rows8 & 2) == 2

    def gather_rows(values):
        a, b, c, d = values
        low = jnp.where(odd, b, a) + pltpu.roll(jnp.where(odd, a, b), 7, 0)
        high = jnp.where(odd, d, c) + pltpu.roll(jnp.where(odd, c, d), 7, 0)
        both = jnp.where(upper, high, low) + pltpu.roll(jnp.where(upper, low, high), 6, 0)
        return both + pltpu.roll(both, 4, 0)

    def pull(layer, block, saved, kept, d):
        scalar, vector = kept
        d_scalar = d[0:width] + 2.0 * scalar * d[2 * width : 3 * width]
        factor = 2.0 * d[width : 2 * width]
        toward = [[None] * neigh for _ in range(4)]
        d_vector = [v * factor for v in vector]
        for start in range(0, width, tile):
            part = slice(start, start + tile)
            for k in range(neigh):
                cut = pl.ds(k * atoms, atoms)
                rows = picked_ref[saved, pl.ds(start, tile), cut]
                one = radial_ref[saved, pl.ds(width + start, tile), cut]
                both = one * rows if layer else one
                through = None
                for m in range(3):
                    term = wide(spread_ref[block, m * neigh + k]) * d_vector[m][part]
                    through = term if through is None else through + term
                    toward[m][k] = add_up(d_vector[m][part] * both, toward[m][k])
                turned = rows * (
                    change_ref[saved, pl.ds(start, tile), cut] * d_scalar[part]
                    + change_ref[saved, pl.ds(width + start, tile), cut] * through
                )
                toward[3][k] = add_up(turned, toward[3][k])
                if layer:
                    picked_ref[saved, pl.ds(start, tile), cut] = (
                        radial_ref[saved, pl.ds(start, tile), cut] * d_scalar[part] + one * through
                    )
        own = blocks[block]
        lines = jnp.concatenate([gather_rows([toward[m][k] for m in range(4)]) for k in range(neigh)], axis=1)
        d_direction = jnp.where(tall < 3, lines, 0.0)
        inverse, direction = own["inverse"], own["direction"]
        radial_part = lines[3:4] - jnp.sum(d_direction * direction, axis=0, keepdims=True) * inverse
        return d_direction * inverse + radial_part * direction

    kept0 = []
    kinds = jnp.concatenate([blocks[block]["base"][3:4, :] for block in range(4)], axis=1)
    hits = marks(padded, kinds)
    hits = jnp.concatenate([hits, hits], axis=0)
    feats_ref[...] = dot(embed_lift_ref[...], hits)
    initial = initial_ref[...]

    def ready(block):
        hits = marks(padded, blocks[block]["far"][3:4, :])
        picked_ref[block] = dot(lifted_left_ref[...], jnp.concatenate([hits, hits], axis=0))
        radial(0, block, block)

    ready(0)
    for block in range(4):
        if block < 3:
            ready(block + 1)
        else:
            radial(1, 0, 4)
        kept0.append(interact(0, block, block))
        if block % 2:
            cut = slice((block - 1) * atoms, (block + 1) * atoms)
            mixing = invariants(kept0[block - 1 : block + 1])
            feats_ref[:, cut] = feats_ref[:, cut] + dot(mix_lift_ref[...], mixing)
            if block == 1:
                layer_out = initial + dot(mix_left_ref[...], mixing[:, 0:atoms])

    high, low = split2(feats_ref[...])
    both = dot(jnp.concatenate([high, low], axis=0), full_ref[...])
    picked_ref[4] = both[0:width] + both[width:]
    change(1, 4)
    kept1 = interact(1, 0, 4)

    pre = dot(mix_read_ref[...], invariants([kept1])) + dot(read_left_ref[...], right3(layer_out))
    active, gain = silu(pre)
    atom_energy = dot(row_left_ref[:, 0 : 3 * width], right3(layer_out)) + dot(
        row_left_ref[:, 3 * width :], right3(active)
    )
    first_column = column_ref[0:width, :]
    turned = right3(column_ref[width : width + read_width, :] * gain)
    d_own = dot(read_back_ref[...], turned) + column_ref[0:width, :]

    d_mixed = dot(mix_read_back_ref[...], turned)
    d_mixed_own = dot(mix_back_ref[...], right3(d_own))
    change(0, 0)
    edge_grad_one = pull(1, 0, 4, kept1, d_mixed)
    high, low = split2(picked_ref[4])
    back = dot(jnp.concatenate([high, low], axis=0), full_ref[...], NT)

    forces = {}
    d_mixed = dot(mix_up_back_ref[...], right3(back[0:width] + back[width:]))
    d_mixed = [d_mixed[:, block * atoms : (block + 1) * atoms] for block in range(4)]
    d_mixed[0] = d_mixed[0] + d_mixed_own

    def push(offset, value):
        forces[offset] = forces[offset] + value if offset in forces else value

    sums = None
    for block in range(4):
        if block < 3:
            change(0, block + 1)
        grad = pull(0, block, block, kept0[block], d_mixed[block])
        if block == 0:
            grad = grad + edge_grad_one
        own = blocks[block]
        centres = [home] if block == 0 else [units[block - 1], minus[block - 1]]
        pulled = fold(grad)
        if block == 0:
            push(home, pulled)
        else:
            bit = has_bit(lanes8, block)
            push(centres[1], jnp.where(bit, pulled, 0.0))
            push(centres[0], jnp.where(bit, 0.0, pulled))
        high = grad.astype(BF16).astype(F32)
        pair = jnp.concatenate([high[0:4], (grad - high)[0:4]], axis=0)
        stack = [jnp.where(own["combo"] == j, pair, 0.0) for j in range(4 * len(centres))]
        landed = dot(jnp.concatenate(stack, axis=0).astype(BF16), slots_ref[block] if block else own_hits_ref[...], NT)
        for c, centre in enumerate(centres):
            for q in range(4):
                j = 4 * c + q
                value = -landed[8 * j : 8 * j + 8]
                if q == 0:
                    push(centre, value)
                else:
                    bit = has_bit(lanes8, q)
                    push(plus(centre, minus[q - 1]), jnp.where(bit, value, 0.0))
                    push(plus(centre, units[q - 1]), jnp.where(bit, 0.0, value))
        rows = []
        for r in range(3):
            rows.append(-fold(jnp.broadcast_to(own["vec"][r : r + 1, :], (8, edges)) * grad))
        if block == 0:
            rows.append(atom_energy)
        rows = jnp.concatenate(rows, axis=0)
        member = (own["struct"].astype(jnp.int32) == (iota((atoms, atoms), 0) & (structs - 1))).astype(F32)
        high, low = split2(rows)
        got = dot(jnp.concatenate([high, low], axis=0), member.astype(BF16), NT)
        got = got[0 : rows.shape[0]] + got[rows.shape[0] :]
        if block == 0:
            energy_row = got[24:25]
            sums = got[0:24]
        else:
            sums = sums + got

    per_row = LANES // structs
    lane_row = iota((1, atoms), 1) // structs
    packed = []
    for row in range(-(-10 // per_row)):
        line = jnp.zeros((1, atoms), F32)
        for j in range(row * per_row, min(10, (row + 1) * per_row)):
            if j == 0:
                value = energy_row
            else:
                r, t = divmod(j - 1, 3)
                value = sums[8 * r + t : 8 * r + t + 1]
            line = line + jnp.where(lane_row == j - row * per_row, value, 0.0)
        packed.append(line)

    def store(index, carry):
        for step in range(8):
            for m in range(3):
                out_ref[index * 8 + step, m] = jnp.zeros((1, atoms), F32)
            for j, line in enumerate(packed):
                out_ref[index * 8 + step, 3 + j] = line
        return carry

    lax.fori_loop(0, out_ref.shape[0] // 8, store, 0)
    for offset, value in forces.items():
        value = value[0:3] + value[4:7]
        index = device_of(offset)
        for m in range(3):
            out_ref[index, m] = out_ref[index, m] + value[m : m + 1, :]


def whole(memory_space=pltpu.VMEM):
    return pl.BlockSpec(memory_space=memory_space)


def shards(
    sizes,
    positions,
    species,
    cell_map,
    neighbours,
    struct_ids,
    embed,
    w_up,
    w_rad_in,
    w_rad_out,
    w_mix,
    read_first,
    read_hidden,
    read_last,
):
    devices = math.prod(sizes)
    atoms = positions.shape[1]
    neigh = neighbours.shape[0]
    width = w_up.shape[2]
    structs = SLAB_STRUCTS * sizes[0]
    elements = embed.shape[0]
    padded = -(-elements // LANES) * LANES
    edges = neigh * atoms
    params = pltpu.CompilerParams(vmem_limit_bytes=32 << 20)
    small = pltpu.CompilerParams(vmem_limit_bytes=8 << 20)
    sent, own = pl.pallas_call(
        pack_kernel,
        out_shape=[jax.ShapeDtypeStruct((count, HEAD_ROWS + neigh, 1, atoms), F32) for count in (devices, 1)],
        in_specs=[whole()] * 5,
        out_specs=[whole()] * 2,
        compiler_params=pltpu.CompilerParams(vmem_limit_bytes=60 << 20),
        name="pack",
    )(positions, species.reshape(1, -1), cell_map, neighbours, struct_ids.reshape(1, -1))
    got = lax.all_to_all(sent, AXES, 0, 0, tiled=True)
    radial_hidden, read_width, bessels = w_rad_in.shape[2], read_hidden.shape[1], w_rad_in.shape[1]
    shapes = [
        ((width, 2 * padded), BF16),
        ((width, 2 * padded), BF16),
        ((width, 9 * width), BF16),
        ((width, 9 * width), BF16),
        ((read_width, 9 * width), BF16),
        ((3 * width, 3 * width), BF16),
        ((3 * width, 3 * width), BF16),
        ((3 * width, 3 * read_width), BF16),
        ((2, 2 * width, 3 * radial_hidden), BF16),
        ((2, 3 * bessels, radial_hidden), BF16),
        ((read_width, 3 * width), BF16),
        ((width, 3 * read_width), BF16),
        ((8, 3 * width + 3 * read_width), BF16),
        ((width + read_width, atoms), F32),
        ((atoms, edges), BF16),
        ((4 * atoms, edges), BF16),
        ((width, atoms), F32),
    ]
    weights = pl.pallas_call(
        functools.partial(prep_kernel, 1.0 / math.sqrt(neigh)),
        out_shape=[jax.ShapeDtypeStruct(*shape) for shape in shapes],
        in_specs=[whole()] * 9,
        out_specs=[whole()] * len(shapes),
        scratch_shapes=[pltpu.VMEM((padded, width), F32)],
        compiler_params=small,
        cost_estimate=pl.CostEstimate(flops=4_000_000_000, bytes_accessed=2_000_000, transcendentals=0),
        name="weights",
    )(
        own,
        embed,
        w_up,
        w_rad_in,
        w_rad_out,
        w_mix,
        read_first.reshape(1, -1),
        read_hidden.T,
        read_last.reshape(1, -1),
    )
    count = TAIL_ROWS - (-10 // (LANES // structs))
    parts = pl.pallas_call(
        functools.partial(main_kernel, sizes, structs),
        out_shape=jax.ShapeDtypeStruct((devices, count, 1, atoms), F32),
        in_specs=[whole()] * (1 + len(shapes)),
        out_specs=whole(),
        scratch_shapes=[
            pltpu.VMEM((5, 2 * width, edges), F32),
            pltpu.VMEM((5, width, edges), F32),
            pltpu.VMEM((4, 3 * neigh, 8, atoms), F32),
            pltpu.VMEM((5, 2 * width, edges), F32),
            pltpu.VMEM((5, 3 * radial_hidden, edges), BF16),
            pltpu.VMEM((4, atoms, edges), BF16),
            pltpu.VMEM((width, 4 * atoms), F32),
        ],
        compiler_params=params,
        name="forces",
    )(got, *weights)
    back = lax.all_to_all(parts, AXES, 0, 0, tiled=True)
    energies, virials, forces = pl.pallas_call(
        functools.partial(end_kernel, structs),
        out_shape=(
            jax.ShapeDtypeStruct((1, structs), F32),
            jax.ShapeDtypeStruct((9, structs), F32),
            jax.ShapeDtypeStruct((3, atoms), F32),
        ),
        in_specs=[whole()] * 2,
        out_specs=(whole(),) * 3,
        compiler_params=small,
        name="finish",
    )(back, cell_map)
    return energies.reshape(-1), virials, forces


def solution(mesh):
    sizes = tuple(mesh.shape[axis] for axis in AXES)
    return jax.shard_map(
        functools.partial(shards, sizes),
        mesh=mesh,
        in_specs=(
            P(None, AXES),
            P(AXES),
            P(AXES, None),
            P(None, AXES),
            P(AXES),
            P(),
            P(),
            P(),
            P(),
            P(),
            P(),
            P(),
            P(),
        ),
        out_specs=(P(), P(), P(None, AXES)),
        check_vma=False,
    )
```
